32 devices in a mesh: grid: 2 (over core), px: 4 (over y, x), py: 4 (over z).
Axes of the slice: x: 2, y: 2, z: 4, core: 2. Of those that a mesh axis runs over, the one named last changes fastest.
Arguments:
- residual: float32 [2, 32, 32, 5, 1024], P('grid', 'px', 'py'), may hold values from -3 to 3
- inverses: float32 [2, 32, 32, 25, 1024], P('grid', 'px', 'py'), may hold values from 0 to 1, as said below
- couplings: float32 [2, 32, 32, 4, 1024], P('grid', 'px', 'py'), may hold values from 0.22 to 0.735, as said below
- receptors: int32 [2, 4, 4, 512], P('grid', 'px', 'py'), may hold values from 0 to 65535, as said below
- owners: int32 [2, 4, 4, 512, 1], P('grid', 'px', 'py'), may hold values from 0 to 15; in each aligned block of 512 rows (0 to 511, 512 to 1023, ..., all dimensions but the last counted through in order) at most 64 rows name the same one
- donors: int32 [2, 4, 4, 512, 8], P('grid', 'px', 'py'), may hold values from 0 to 65535
- weights: float32 [2, 4, 4, 512, 8], P('grid', 'px', 'py'), may hold values from 0 to 1, as said below
Outputs:
- update: float32 [2, 32, 32, 5, 1024], P('grid', 'px', 'py')
The draws below stay inside these ranges and needn't reach their ends.
Inputs may be any that keep to these rules, and one draw needn't show every extreme that they name: `receptors`: receptor indices of one device are distinct. `owners`: among the receptors of one device no owner appears more than 64 times, and in every draw some device names one owner exactly 64 times. `weights`: nonnegative; the 8 weights of a receptor sum to 1. `inverses`: all entries nonnegative; off-diagonal entries 0.02 to 0.07; each row of a block sums to 0.94 to 1. `couplings`: a + b and e + f of each cell lie in 0.88 to 0.98, and each coupling is a quarter to three quarters of its pair's sum.
All inputs are finite; a program needn't handle non-finite values.
Results may differ from the reference program's by a relative error of at most 0.0001.
Values sent between devices are 32-bit elements; how exact they have to be, the bound alone decides.
A program may use at most 128 MiB of HBM per device.

```python
import math
import jax
import jax.numpy as jnp
import numpy as np
from jax import lax

COMPS = 5
DONORS = 8
CI = 8
CJ = 8
CK = 1024
R_DEV = 512
GRIDS = 2
BLOCKS_I = 4
BLOCKS_J = 4
NI = 32
NJ = 32
CELLS = 65536
OWNERS = 16
SLOTS = 64


def draw_residual(key, part):
    shape = (GRIDS, NI, NJ, COMPS, CK)
    return jnp.clip(0.5 * jax.random.normal(key, shape, jnp.float32), -3.0, 3.0)


def draw_inverses(key, part):
    first, second = jax.random.split(key)
    shape = (GRIDS, NI, NJ, COMPS, COMPS, CK)
    row_total = jax.random.uniform(first, (GRIDS, NI, NJ, COMPS, 1, CK), jnp.float32, 0.94, 1.0)
    identity = jnp.eye(COMPS, dtype=jnp.float32).reshape(1, 1, 1, COMPS, COMPS, 1)
    offdiag = jax.random.uniform(second, shape, jnp.float32, 0.02, 0.07) * (1.0 - identity)
    diagonal = row_total - jnp.sum(offdiag, axis=4, keepdims=True)
    blocks = offdiag + identity * diagonal
    return blocks.reshape(GRIDS, NI, NJ, COMPS * COMPS, CK)


def draw_couplings(key, part):
    keys = jax.random.split(key, 4)
    shape = (GRIDS, NI, NJ, 1, CK)
    low_total = 0.88
    lower_total = jax.random.uniform(keys[0], shape, jnp.float32, low_total, 0.98)
    upper_total = jax.random.uniform(keys[1], shape, jnp.float32, low_total, 0.98)
    lower_split = jax.random.uniform(keys[2], shape, jnp.float32, 0.25, 0.75)
    upper_split = jax.random.uniform(keys[3], shape, jnp.float32, 0.25, 0.75)
    return jnp.concatenate([lower_total * lower_split, lower_total * (1.0 - lower_split), upper_total * upper_split, upper_total * (1.0 - upper_split)], axis=3)


def draw_weights(key, part):
    shape = (GRIDS, NI // CI, NJ // CJ, R_DEV, DONORS)
    raw_weight = jax.random.uniform(key, shape, jnp.float32, 0.05, 1.0)
    return raw_weight / jnp.sum(raw_weight, axis=-1, keepdims=True)


def draw_receptors(key, part):
    stride = CELLS // R_DEV
    shape = (GRIDS, NI // CI, NJ // CJ, R_DEV)
    offsets = jax.random.randint(key, shape, 0, stride, dtype=jnp.int32)
    return offsets + jnp.arange(R_DEV, dtype=jnp.int32) * stride


def plant(values, rng, smallest, high):
    index_at = [jax.random.randint(jax.random.fold_in(rng, axis), (), 0, length) for axis, length in enumerate(values.shape)]
    widest = values.shape.index(max(values.shape))
    beside = index_at[:widest] + [(index_at[widest] + 1) % values.shape[widest]] + index_at[widest + 1:]
    return values.at[tuple(index_at)].set(smallest).at[tuple(beside)].set(high)


def deal_out(key, own, number, rows, amount, top, limit, lean):
    order = jax.random.permutation(key, amount)
    heavy_load, common = load_shares(amount, rows * top, limit, lean, True), load_shares(amount, rows * top, limit, lean, False)
    places = jnp.arange(amount)

    def named(tallies, offset_by):
        used = int((tallies > 0).sum())
        fixed = max(1, used // 4)
        shifted = fixed + (places - fixed + offset_by * (used - fixed)) % max(1, amount - fixed)
        return jnp.zeros((amount,), jnp.int32).at[order[jnp.where(places < fixed, places, shifted)]].set(jnp.asarray(tallies, jnp.int32))

    tallies = jnp.where(number % 4 == 0, named(heavy_load, number // 4), named(common, number - number // 4 - 1))
    mixed = jax.random.permutation(jax.random.fold_in(own, 3), amount)
    donor, taker = mixed[0:amount // 2 * 2:2], mixed[1:amount // 2 * 2:2]
    slack = jnp.minimum(tallies[donor] - 1, limit - tallies[taker]) // 2
    slack = jnp.where((donor == order[0]) | (taker == order[0]) | (tallies[taker] == 0), 0, jnp.maximum(slack, 0))
    shifted = jax.random.randint(jax.random.fold_in(own, 4), (amount // 2,), 0, 1 << 20) % (slack + 1)
    tallies = tallies.at[donor].add(-shifted).at[taker].add(shifted)
    items = jnp.searchsorted(jnp.cumsum(tallies), jnp.arange(rows * top), side="right").astype(jnp.int32)
    listing = items.reshape(top, rows).T
    listing = listing[jax.random.permutation(jax.random.fold_in(own, 1), rows)]
    offset_by = jax.random.randint(jax.random.fold_in(own, 2), (rows, 1), 0, top)
    return jnp.take_along_axis(listing, (jnp.arange(top)[None, :] + offset_by) % top, axis=1)


def load_shares(number_of, total, most, skew, full):
    loads = [(1 << 20) // math.isqrt(standing ** skew) + 1 for standing in range(1, number_of + 1)]
    largest = most if full else min(most, max(-(-total // number_of), total * loads[0] // sum(loads)))
    least = 1 if total - largest >= number_of - 1 else 0
    given, surplus = [largest] + [least] * (number_of - 1), total - largest - least * (number_of - 1)
    while surplus > 0:
        movable = [i for i in range(1, number_of) if given[i] < largest] or [i for i in range(1, number_of) if given[i] < most]
        mass, left = sum([loads[i] for i in movable]), surplus
        for i in movable:
            extra = min(most - given[i], max(1, left * loads[i] // mass), surplus)
            given[i] = given[i] + extra
            surplus = surplus - extra
    return np.array(given)


def setup_inputs(seed: int = 0) -> dict:
    key_list = jax.random.split(jax.random.key(seed), 8)
    residual = draw_residual(jax.random.fold_in(key_list[7], 71), 0)
    inverses = draw_inverses(jax.random.fold_in(key_list[7], 71), 0)
    couplings = draw_couplings(jax.random.fold_in(key_list[7], 71), 0)
    receptors = draw_receptors(jax.random.fold_in(key_list[7], 71), 0)
    owners_keys = jax.random.split(jax.random.fold_in(key_list[4], 1), GRIDS * BLOCKS_I * BLOCKS_J * R_DEV // R_DEV)
    owners_turns = jax.random.permutation(jax.random.fold_in(key_list[4], 3), GRIDS * BLOCKS_I * BLOCKS_J * R_DEV // R_DEV)
    owners = jax.vmap(lambda own, number: deal_out(jax.random.fold_in(key_list[4], 2), own, number, R_DEV, OWNERS, 1, SLOTS, 2))(owners_keys, owners_turns).reshape((GRIDS, BLOCKS_I, BLOCKS_J, R_DEV, 1))
    donors = plant(jax.random.randint(key_list[5], (GRIDS, BLOCKS_I, BLOCKS_J, R_DEV, DONORS), 0, CELLS), jax.random.fold_in(key_list[5], 1), 0, CELLS - 1).astype(jnp.int32)
    weights = draw_weights(jax.random.fold_in(key_list[7], 71), 0)
    return {"residual": residual, "inverses": inverses, "couplings": couplings, "receptors": receptors, "owners": owners, "donors": donors, "weights": weights}


def apply_block(block, vector):
    shaped = block.reshape(block.shape[:-2] + (5, 5, block.shape[-1]))
    return jnp.sum(shaped * vector[..., None, :, :], axis=-2)


def forward_grid(rhs_grid, inverse_grid, coupling_grid):
    def row_step(upper_row, inputs):
        rhs_row, inv_row, coup_row = inputs

        def cell_step(left_value, cell_inputs):
            rhs_cell, inv_cell, coup_cell, upper_cell = cell_inputs
            result = apply_block(inv_cell, rhs_cell + coup_cell[0][None] * upper_cell + coup_cell[1][None] * left_value)
            return result, result

        start = jnp.zeros(rhs_row.shape[1:], jnp.float32)
        _, row_values = lax.scan(cell_step, start, (rhs_row, inv_row, coup_row, upper_row))
        return row_values, row_values

    start_row = jnp.zeros(rhs_grid.shape[1:], jnp.float32)
    _, result = lax.scan(row_step, start_row, (rhs_grid, inverse_grid, coupling_grid))
    return result


def backward_grid(star_grid, inverse_grid, coupling_grid):
    def row_step(lower_row, inputs):
        star_row, inv_row, coup_row = inputs

        def cell_step(right_value, cell_inputs):
            star_cell, inv_cell, coup_cell, lower_cell = cell_inputs
            result = star_cell + apply_block(inv_cell, coup_cell[2][None] * lower_cell + coup_cell[3][None] * right_value)
            return result, result

        start = jnp.zeros(star_row.shape[1:], jnp.float32)
        _, row_values = lax.scan(cell_step, start, (star_row, inv_row, coup_row, lower_row), reverse=True)
        return row_values, row_values

    start_row = jnp.zeros(star_grid.shape[1:], jnp.float32)
    _, result = lax.scan(row_step, start_row, (star_grid, inverse_grid, coupling_grid), reverse=True)
    return result


def reference(residual, inverses, couplings, receptors, owners, donors, weights):
    swept_list = []
    for grid_index in range(GRIDS):
        star = forward_grid(residual[grid_index], inverses[grid_index], couplings[grid_index])
        swept_list.append(backward_grid(star, inverses[grid_index], couplings[grid_index]))
    swept = jnp.stack(swept_list)
    owner_list = owners[..., 0]
    owner_i = owner_list // BLOCKS_J
    owner_j = owner_list % BLOCKS_J
    pencil = donors // CK
    donor_i = owner_i[..., None] * CI + pencil // CJ
    donor_j = owner_j[..., None] * CJ + pencil % CJ
    donor_k = donors % CK
    grid_ids = jnp.arange(GRIDS, dtype=jnp.int32).reshape(GRIDS, 1, 1, 1, 1)
    other_grid = (1 - grid_ids) * jnp.ones_like(donors)
    values = swept[other_grid, donor_i, donor_j, :, donor_k]
    fringe = jnp.sum(values * weights[..., None], axis=-2)
    block_i = jnp.arange(BLOCKS_I, dtype=jnp.int32).reshape(1, BLOCKS_I, 1, 1)
    block_j = jnp.arange(BLOCKS_J, dtype=jnp.int32).reshape(1, 1, BLOCKS_J, 1)
    rec_pencil = receptors // CK
    rec_i = block_i * CI + rec_pencil // CJ
    rec_j = block_j * CJ + rec_pencil % CJ
    rec_k = receptors % CK
    rec_grid = grid_ids[..., 0] * jnp.ones_like(receptors)
    return swept.at[rec_grid, rec_i, rec_j, :, rec_k].set(fringe)
```

```python
import functools

import jax
import jax.numpy as jnp
from jax import lax
from jax.experimental import pallas as pl
from jax.experimental.pallas import tpu as pltpu
from jax.sharding import PartitionSpec as P

MESH = pl.DeviceIdType.MESH
LANES = 128
ROWS = 8
LOW = 8
EMPTY = LANES


def divmod_const(value, by):
    if by & (by - 1) == 0:
        return value >> (by.bit_length() - 1), value & (by - 1)
    return value // by, value % by


def sweep_kernel(
    dims,
    res_hbm,
    inv_hbm,
    cpl_hbm,
    owners,
    donors,
    weights,
    receptors,
    out_hbm,
    code_out,
    reply_out,
    inv_v,
    res_v,
    cpl_v,
    star_v,
    field_v,
    face_send,
    face_recv,
    ask_send,
    ask_recv,
    rows_v,
    rows_s,
    spread,
    reply_send,
    reply_recv,
    in_sem,
    out_sem,
    send_sem,
    recv_sem,
    ask_send_sem,
    ask_recv_sem,
    reply_send_sem,
    reply_recv_sem,
    rows_sem,
):
    ci, cj, comps, blocks, count_rows, count_cols, slot_count = dims
    length = blocks * LANES
    entries = comps * comps
    steps = ci + cj - 1
    tall = ci + 2 * (cj - 1)
    many, count = donors.shape
    owner_count = count_rows * count_cols
    slots = owner_count * slot_count
    grid = lax.axis_index("grid")
    px = lax.axis_index("px")
    py = lax.axis_index("py")
    me = px * count_cols + py
    ahead = px + py
    reach = count_rows + count_cols - 2

    def input_copies(kb):
        lanes = pl.ds(pl.multiple_of(kb * LANES, LANES), LANES)
        mine = pl.ds(cj - 1, ci)
        return (
            pltpu.make_async_copy(
                inv_hbm.at[:, :, :, lanes], inv_v.at[kb, mine], in_sem.at[0, kb]
            ),
            pltpu.make_async_copy(
                res_hbm.at[:, :, :, lanes], res_v.at[kb, mine], in_sem.at[1, kb]
            ),
            pltpu.make_async_copy(
                cpl_hbm.at[:, :, :, lanes],
                cpl_v.at[kb, mine, :, pl.ds(0, 4), :],
                in_sem.at[2, kb],
            ),
        )

    for kb in range(blocks):
        for copy in input_copies(kb):
            copy.start()

    has_prev_row = px > 0
    has_next_row = px < count_rows - 1
    has_prev_col = py > 0
    has_next_col = py < count_cols - 1
    prev_row = {"px": px - 1}
    next_row = {"px": px + 1}
    prev_col = {"py": py - 1}
    next_col = {"py": py + 1}
    sides = (
        (has_prev_row, prev_row),
        (has_next_row, next_row),
        (has_prev_col, prev_col),
        (has_next_col, next_col),
    )

    def other(q):
        return {"grid": 1 - grid, "px": q // count_cols, "py": q % count_cols}

    barrier = pltpu.get_barrier_semaphore()
    for there, device in sides:

        @pl.when(there)
        def _():
            pl.semaphore_signal(barrier, inc=1, device_id=device, device_id_type=MESH)

    @pl.loop(0, owner_count)
    def _(q):
        pl.semaphore_signal(barrier, inc=1, device_id=other(q), device_id_type=MESH)

    def enter():
        near = sum(there.astype(jnp.int32) for there, _ in sides)
        pl.semaphore_wait(barrier, near + owner_count)

    def ask(q):
        return pltpu.make_async_remote_copy(
            src_ref=ask_send.at[q],
            dst_ref=ask_recv.at[me],
            send_sem=ask_send_sem.at[q],
            recv_sem=ask_recv_sem.at[me],
            device_id=other(q),
            device_id_type=MESH,
        )

    def asked(q):
        return pltpu.make_async_remote_copy(
            src_ref=ask_send.at[q],
            dst_ref=ask_recv.at[q],
            send_sem=ask_send_sem.at[q],
            recv_sem=ask_recv_sem.at[q],
            device_id=other(q),
            device_id_type=MESH,
        )

    def reply(q):
        return pltpu.make_async_remote_copy(
            src_ref=reply_send.at[q],
            dst_ref=reply_recv.at[me],
            send_sem=reply_send_sem.at[q],
            recv_sem=reply_recv_sem.at[me],
            device_id=other(q),
            device_id_type=MESH,
        )

    def replied(q):
        return pltpu.make_async_remote_copy(
            src_ref=reply_send.at[q],
            dst_ref=reply_recv.at[q],
            send_sem=reply_send_sem.at[q],
            recv_sem=reply_recv_sem.at[q],
            device_id=other(q),
            device_id_type=MESH,
        )

    def digits(value):
        return [(value >> LOW).astype(jnp.float32), (value & (2**LOW - 1)).astype(jnp.float32)]

    def plan():
        owner = owners[...]
        ones = jnp.where(
            owner == lax.broadcasted_iota(jnp.int32, (owner_count, count), 0), 1.0, 0.0
        )
        before = jnp.where(
            lax.broadcasted_iota(jnp.int32, (count, count), 0)
            < lax.broadcasted_iota(jnp.int32, (count, count), 1),
            1.0,
            0.0,
        ).astype(jnp.bfloat16)
        seen = jnp.dot(ones.astype(jnp.bfloat16), before, preferred_element_type=jnp.float32)
        rank = jnp.sum(seen * ones, axis=0, keepdims=True).astype(jnp.int32)
        place = owner * slot_count + rank
        weight = weights[...]
        high = weight.astype(jnp.bfloat16).astype(jnp.float32)
        mid = (weight - high).astype(jnp.bfloat16).astype(jnp.float32)
        low = weight - high - mid
        cell = receptors[...]
        marks = jnp.concatenate(
            digits(cell) + [jnp.ones((1, count), jnp.float32), jnp.zeros((ROWS - 3, count), jnp.float32)],
            axis=0,
        )
        table = jnp.concatenate(digits(donors[...]) + [high, mid, low, marks], axis=0).astype(
            jnp.bfloat16
        )
        wide = min(2 * LANES, slots)
        lane = lax.broadcasted_iota(jnp.int32, (many, LANES), 1)
        for base in range(0, slots, wide):
            slot = lax.broadcasted_iota(jnp.int32, (wide, count), 0) + base
            pick = jnp.where(slot == place, 1.0, 0.0).astype(jnp.bfloat16)
            got = lax.dot_general(
                table, pick, (((1,), (1,)), ((), ())), preferred_element_type=jnp.float32
            )
            cells = got[:many] * float(2**LOW) + got[many : 2 * many]
            share = got[2 * many : 3 * many] + got[3 * many : 4 * many] + got[4 * many : 5 * many]
            mark = got[5 * many : 5 * many + 3]
            target = (mark[0:1] * float(2**LOW) + mark[1:2]).astype(jnp.int32)
            pencil, k = divmod_const(target, length)
            kb, spot = divmod_const(k, LANES)
            line = kb * (ci * cj) + pencil
            code_out[:, base : base + wide] = jnp.where(
                mark[2:3] > 0.5, line * (2 * LANES) + spot, EMPTY
            )
            for q in range(base // slot_count, (base + wide) // slot_count):
                at = q * slot_count - base
                tile = at // LANES * LANES
                shift = at - tile
                left = cells[:, tile : tile + LANES]
                right = share[:, tile : tile + LANES]
                if shift:
                    left = pltpu.roll(left, LANES - shift, 1)
                if (slot_count - shift) % LANES:
                    right = pltpu.roll(right, (slot_count - shift) % LANES, 1)
                ask_send[q] = jnp.where(lane < slot_count, left, right)

        @pl.when(ahead >= 2)
        def _():
            enter()

        @pl.loop(0, owner_count)
        def _(q):
            ask(q).start()

    def prepare():
        line = lax.broadcasted_iota(jnp.int32, (slot_count, LANES), 1)

        @pl.loop(0, owner_count)
        def _(q):
            asked(q).wait_recv()
            tile = ask_recv[q]
            cell = tile.astype(jnp.int32)
            pencil, k = divmod_const(cell, length)
            kb, _ = divmod_const(k, LANES)
            i, j = divmod_const(pencil, cj)
            row = kb * (tall * cj) + (i + (cj - 1)) * cj + j
            rows_v[pl.ds(pl.multiple_of(q * ROWS, ROWS), ROWS), :] = jnp.clip(
                row, 0, blocks * tall * cj - 1
            )
            turned = tile.T
            first = pl.multiple_of(q * slot_count, slot_count)
            for d in range(many):
                spot = turned[:slot_count, d : d + 1].astype(jnp.int32) & (LANES - 1)
                share = turned[slot_count : 2 * slot_count, d : d + 1]
                spread[d, pl.ds(first, slot_count), :] = jnp.where(line == spot, share, 0.0)

        copy = pltpu.make_async_copy(rows_v, rows_s, rows_sem)
        copy.start()
        copy.wait()

    def send(kind, kb):
        device = (next_row, next_col, prev_row, prev_col)[kind]
        return pltpu.make_async_remote_copy(
            src_ref=face_send.at[kind, kb],
            dst_ref=face_recv.at[kind, kb],
            send_sem=send_sem.at[kind, kb],
            recv_sem=recv_sem.at[kind, kb],
            device_id=device,
            device_id_type=MESH,
        )

    gets = (has_prev_row, has_prev_col, has_next_row, has_next_col)
    puts = (has_next_row, has_next_col, has_prev_row, has_prev_col)

    for kind in range(4):

        @pl.when(jnp.logical_not(gets[kind]))
        def _():
            face_recv[kind] = jnp.zeros(face_recv.shape[1:], jnp.float32)

    sub = lax.broadcasted_iota(jnp.int32, (cj, LANES), 0)

    def product(mat, vec):
        out = []
        for r in range(comps):
            terms = [mat(r * comps + c) * vec[c] for c in range(comps)]
            while len(terms) > 1:
                terms = [
                    terms[t] + terms[t + 1] if t + 1 < len(terms) else terms[t]
                    for t in range(0, len(terms), 2)
                ]
            out.append(terms[0])
        return out

    def wait_recv(kind, kb):
        @pl.when(gets[kind])
        def _():
            send(kind, kb).wait_recv()

    def start_send(kind, kb):
        @pl.when(puts[kind])
        def _():
            send(kind, kb).start()

    inv_flat = inv_v.reshape(blocks, tall * entries * cj, LANES)
    res_flat = res_v.reshape(blocks, tall * comps * cj, LANES)
    cpl_flat = cpl_v.reshape(blocks, tall * cj * ROWS, LANES)
    field_flat = field_v.reshape(blocks, tall * cj * ROWS, LANES)
    field_rows = field_v.reshape(blocks * tall * cj, ROWS, LANES)

    def entry(ref, kb, s, height, e):
        start = s * height * cj + e * cj + cj - 1
        return ref[kb, pl.ds(start, cj, stride=height * cj - 1), :]

    def cell_rows(s, c):
        return pl.ds((s * cj + cj - 1) * ROWS + c, cj, stride=(cj - 1) * ROWS)

    def forward(kb):
        for copy in input_copies(kb):
            copy.wait()
        wait_recv(0, kb)
        wait_recv(1, kb)
        upper = [face_recv[0, kb, pl.ds(c * ROWS, cj), :] for c in range(comps)]
        prev = [jnp.zeros((cj, LANES), jnp.float32)] * comps
        lower = [jnp.zeros((cj, LANES), jnp.float32)] * comps
        for s in range(steps):
            coef_a = cpl_flat[kb, cell_rows(s, 0), :]
            coef_b = cpl_flat[kb, cell_rows(s, 1), :]
            up = prev
            if s < cj:
                up = [jnp.where(sub == cj - 1 - s, upper[c], prev[c]) for c in range(comps)]
            left = [pltpu.roll(p, cj - 1, 0) for p in prev]
            if s < ci:
                left = [
                    jnp.where(
                        sub == cj - 1,
                        jnp.broadcast_to(
                            face_recv[1, kb, pl.ds(c * ROWS + s, 1), :], (cj, LANES)
                        ),
                        left[c],
                    )
                    for c in range(comps)
                ]
            vec = [
                entry(res_flat, kb, s, comps, c) + coef_a * up[c] + coef_b * left[c]
                for c in range(comps)
            ]
            prev = product(lambda e: entry(inv_flat, kb, s, entries, e), vec)
            for c in range(comps):
                star_v[kb, s, c] = prev[c]
                if s >= cj - 1:
                    face_send[1, kb, pl.ds(c * ROWS + s - cj + 1, 1), :] = prev[c][0:1, :]
                if s >= ci - 1:
                    lower[c] = jnp.where(sub == cj + ci - 2 - s, prev[c], lower[c])
        for c in range(comps):
            face_send[0, kb, pl.ds(c * ROWS, cj), :] = lower[c]

        @pl.when((kb == 0) & (ahead < 2))
        def _():
            enter()

        start_send(0, kb)
        start_send(1, kb)

    def out_copy(kb):
        return pltpu.make_async_copy(
            field_v.at[kb, pl.ds(cj - 1, ci)], out_hbm.at[kb], out_sem.at[kb]
        )

    def backward(kb):
        wait_recv(2, kb)
        wait_recv(3, kb)
        under = [face_recv[2, kb, pl.ds(c * ROWS, cj), :] for c in range(comps)]
        prev = [jnp.zeros((cj, LANES), jnp.float32)] * comps
        upper = [jnp.zeros((cj, LANES), jnp.float32)] * comps
        for s in reversed(range(steps)):
            coef_e = cpl_flat[kb, cell_rows(s, 2), :]
            coef_f = cpl_flat[kb, cell_rows(s, 3), :]
            down = prev
            if s >= ci - 1:
                down = [
                    jnp.where(sub == cj + ci - 2 - s, under[c], prev[c]) for c in range(comps)
                ]
            right = [pltpu.roll(p, 1, 0) for p in prev]
            if s >= cj - 1:
                right = [
                    jnp.where(
                        sub == 0,
                        jnp.broadcast_to(
                            face_recv[3, kb, pl.ds(c * ROWS + s - cj + 1, 1), :], (cj, LANES)
                        ),
                        right[c],
                    )
                    for c in range(comps)
                ]
            vec = [coef_e * down[c] + coef_f * right[c] for c in range(comps)]
            prev = product(lambda e: entry(inv_flat, kb, s, entries, e), vec)
            prev = [star_v[kb, s, c] + prev[c] for c in range(comps)]
            for c in range(comps):
                field_flat[kb, cell_rows(s, c), :] = prev[c]
                if s < cj:
                    upper[c] = jnp.where(sub == cj - 1 - s, prev[c], upper[c])
                if s < ci:
                    face_send[3, kb, pl.ds(c * ROWS + s, 1), :] = prev[c][cj - 1 : cj, :]
        for c in range(comps):
            face_send[2, kb, pl.ds(c * ROWS, cj), :] = upper[c]
        start_send(2, kb)
        start_send(3, kb)
        out_copy(kb).start()

    middle = blocks + 1
    last = 2 * blocks + 2
    begin = jnp.where(ahead == reach, 1, blocks + 2)
    early = ahead + 2 <= reach

    @pl.loop(0, last + 1)
    def _(n):
        @pl.when(((n == 0) & (ahead >= 2)) | ((n == middle) & (ahead < 2)))
        def _():
            plan()

        @pl.when((n >= 1) & (n <= blocks))
        def _():
            forward(n - 1)

        @pl.when((n >= begin) & (n < begin + blocks))
        def _():
            backward(n - begin)

        @pl.when(((n == middle) & early) | ((n == last) & jnp.logical_not(early)))
        def _():
            prepare()

    lane8 = lax.broadcasted_iota(jnp.int32, (ROWS, LANES), 1)
    turn = min(16, slot_count)

    @pl.loop(0, owner_count)
    def _(q):
        def body(t, acc):
            for u in range(turn):
                s = t * turn + u
                parts = [
                    field_rows[rows_s[q * ROWS + d, s]]
                    * spread[d, pl.ds(q * slot_count + s, 1), :]
                    for d in range(many)
                ]
                while len(parts) > 1:
                    parts = [parts[i] + parts[i + 1] for i in range(0, len(parts), 2)]
                total = jnp.sum(parts[0], axis=1, keepdims=True)
                acc = jnp.where(lane8 == s, total, acc)
            return acc

        reply_send[q] = lax.fori_loop(
            0, slot_count // turn, body, jnp.zeros((ROWS, LANES), jnp.float32)
        )
        reply(q).start()

    @pl.loop(0, owner_count)
    def _(q):
        replied(q).wait_recv()
        reply_out[q] = reply_recv[q]

    @pl.loop(0, owner_count)
    def _(q):
        ask(q).wait_send()
        reply(q).wait_send()

    for kb in range(blocks):
        out_copy(kb).wait()
        for kind in range(4):

            @pl.when(puts[kind])
            def _():
                send(kind, kb).wait_send()


def run_sweeps(residual, inverses, couplings, owners, donors, weights, receptors):
    ci, comps, cj, length = residual.shape
    many, count = donors.shape
    blocks = length // LANES
    steps = ci + cj - 1
    tall = ci + 2 * (cj - 1)
    rows, cols = lax.axis_size("px"), lax.axis_size("py")
    owner_count = rows * cols
    slot_count = max(2, 2 * count // owner_count)
    slots = owner_count * slot_count
    assert cj == ROWS and ci <= ROWS and many == ROWS and 2 * slot_count <= LANES
    assert ci * cj * length <= 2 ** (2 * LOW)
    dims = (ci, cj, comps, blocks, rows, cols, slot_count)
    face = comps * ROWS
    dma = pltpu.SemaphoreType.DMA
    hbm = pl.BlockSpec(memory_space=pl.ANY)
    vmem = pl.BlockSpec(memory_space=pltpu.VMEM)
    return pl.pallas_call(
        functools.partial(sweep_kernel, dims),
        out_shape=(
            jax.ShapeDtypeStruct((blocks, ci, cj, ROWS, LANES), jnp.float32),
            jax.ShapeDtypeStruct((1, slots), jnp.int32),
            jax.ShapeDtypeStruct((owner_count, ROWS, LANES), jnp.float32),
        ),
        in_specs=[hbm] * 3 + [vmem] * 4,
        out_specs=(hbm, vmem, vmem),
        scratch_shapes=[
            pltpu.VMEM((blocks, tall, comps * comps, cj, LANES), jnp.float32),
            pltpu.VMEM((blocks, tall, comps, cj, LANES), jnp.float32),
            pltpu.VMEM((blocks, tall, cj, ROWS, LANES), jnp.float32),
            pltpu.VMEM((blocks, steps, comps, cj, LANES), jnp.float32),
            pltpu.VMEM((blocks, tall, cj, ROWS, LANES), jnp.float32),
            pltpu.VMEM((4, blocks, face, LANES), jnp.float32),
            pltpu.VMEM((4, blocks, face, LANES), jnp.float32),
            pltpu.VMEM((owner_count, ROWS, LANES), jnp.float32),
            pltpu.VMEM((owner_count, ROWS, LANES), jnp.float32),
            pltpu.VMEM((owner_count * ROWS, LANES), jnp.int32),
            pltpu.SMEM((owner_count * ROWS, LANES), jnp.int32),
            pltpu.VMEM((many, slots, LANES), jnp.float32),
            pltpu.VMEM((owner_count, ROWS, LANES), jnp.float32),
            pltpu.VMEM((owner_count, ROWS, LANES), jnp.float32),
            dma((3, blocks)),
            dma((blocks,)),
            dma((4, blocks)),
            dma((4, blocks)),
            dma((owner_count,)),
            dma((owner_count,)),
            dma((owner_count,)),
            dma((owner_count,)),
            dma,
        ],
        compiler_params=pltpu.CompilerParams(
            collective_id=0, has_side_effects=True, vmem_limit_bytes=52 * 1024 * 1024
        ),
    )(residual, inverses, couplings, owners, donors, weights, receptors)


def place_kernel(dims, code, reply, field, out, work, sem):
    ci, cj, comps, blocks, slot_count = dims
    owner_count = reply.shape[0]
    copy = pltpu.make_async_copy(field, work, sem)
    copy.start()
    copy.wait()
    lane = lax.broadcasted_iota(jnp.int32, (ROWS, LANES), 1)
    lines = work.reshape(blocks * ci * cj, ROWS, LANES)

    @pl.loop(0, owner_count)
    def _(q):
        tile = reply[q]
        for s in range(slot_count):
            line, spot = divmod_const(code[0, q * slot_count + s], 2 * LANES)
            value = jnp.broadcast_to(tile[:, s : s + 1], (ROWS, LANES))
            pltpu.store(lines.at[line], value, mask=lane == spot)

    stack = work.reshape(blocks, ci, cj * ROWS, LANES)

    @pl.loop(0, ci)
    def _(i):
        for kb in range(blocks):
            for c in range(comps):
                out[i, c, :, kb * LANES : (kb + 1) * LANES] = stack[
                    kb, i, pl.ds(c, cj, stride=ROWS), :
                ]


def run_place(code, reply, field, slot_count, comps):
    blocks, ci, cj = field.shape[:3]
    return pl.pallas_call(
        functools.partial(place_kernel, (ci, cj, comps, blocks, slot_count)),
        out_shape=jax.ShapeDtypeStruct((ci, comps, cj, blocks * LANES), jnp.float32),
        in_specs=[
            pl.BlockSpec(memory_space=pltpu.SMEM),
            pl.BlockSpec(memory_space=pltpu.VMEM),
            pl.BlockSpec(memory_space=pl.ANY),
        ],
        out_specs=pl.BlockSpec(memory_space=pltpu.VMEM),
        scratch_shapes=[
            pltpu.VMEM(field.shape, jnp.float32),
            pltpu.SemaphoreType.DMA,
        ],
        compiler_params=pltpu.CompilerParams(vmem_limit_bytes=16 * 1024 * 1024),
    )(code, reply, field)


def local(residual, inverses, couplings, receptors, owners, donors, weights):
    comps = residual.shape[3]
    many = donors.shape[-1]
    count = donors.shape[-2]
    field, code, reply = run_sweeps(
        residual[0].transpose(0, 2, 1, 3),
        inverses[0].transpose(0, 2, 1, 3),
        couplings[0],
        owners.reshape(1, count),
        donors.reshape(count, many).T,
        weights.reshape(count, many).T,
        receptors.reshape(1, count),
    )
    slot_count = code.shape[1] // reply.shape[0]
    update = run_place(code, reply, field, slot_count, comps)
    return update.transpose(0, 2, 1, 3)[None]


def solution(mesh):
    placed = (
        P("grid", "px", "py", None, None),
        P("grid", "px", "py", None, None),
        P("grid", "px", "py", None, None),
        P("grid", "px", "py", None),
        P("grid", "px", "py", None, None),
        P("grid", "px", "py", None, None),
        P("grid", "px", "py", None, None),
    )
    return jax.shard_map(
        local,
        mesh=mesh,
        in_specs=placed,
        out_specs=P("grid", "px", "py", None, None),
        check_vma=False,
    )
```

```python
import functools

import jax
import jax.numpy as jnp
from jax import lax
from jax.experimental import pallas as pl
from jax.experimental.pallas import tpu as pltpu
from jax.sharding import PartitionSpec as P

MESH = pl.DeviceIdType.MESH
LANES = 128
ROWS = 8
LOW = 8
EMPTY = LANES


def divmod_const(value, by):
    if by & (by - 1) == 0:
        return value >> (by.bit_length() - 1), value & (by - 1)
    return value // by, value % by


def sweep_kernel(
    dims,
    res_hbm,
    inv_hbm,
    cpl_hbm,
    owners_hbm,
    donors_hbm,
    weights_hbm,
    receptors_hbm,
    field_v,
    code_out,
    reply_out,
    owners,
    donors,
    weights,
    receptors,
    inv_v,
    res_v,
    cpl_v,
    star_v,
    face_send,
    face_recv,
    ask_send,
    ask_recv,
    rows_v,
    rows_s,
    spread,
    reply_send,
    reply_recv,
    in_sem,
    small_sem,
    send_sem,
    recv_sem,
    ask_send_sem,
    ask_recv_sem,
    reply_send_sem,
    reply_recv_sem,
    rows_sem,
):
    ci, cj, comps, blocks, count_rows, count_cols, slot_count = dims
    length = blocks * LANES
    entries = comps * comps
    steps = ci + cj - 1
    tall = ci + 2 * (cj - 1)
    many, count = donors.shape
    owner_count = count_rows * count_cols
    slots = owner_count * slot_count
    grid = lax.axis_index("grid")
    px = lax.axis_index("px")
    py = lax.axis_index("py")
    me = px * count_cols + py
    ahead = px + py
    reach = count_rows + count_cols - 2

    def input_copies(kb):
        lanes = pl.ds(pl.multiple_of(kb * LANES, LANES), LANES)
        mine = pl.ds(cj - 1, ci)
        return (
            pltpu.make_async_copy(
                inv_hbm.at[:, :, :, lanes], inv_v.at[kb, mine], in_sem.at[0, kb]
            ),
            pltpu.make_async_copy(
                res_hbm.at[:, :, :, lanes], res_v.at[kb, mine], in_sem.at[1, kb]
            ),
            pltpu.make_async_copy(
                cpl_hbm.at[:, :, :, lanes],
                cpl_v.at[kb, mine, :, pl.ds(0, 4), :],
                in_sem.at[2, kb],
            ),
        )

    small_copies = [
        pltpu.make_async_copy(source, target, small_sem.at[t])
        for t, (source, target) in enumerate(
            (
                (owners_hbm, owners),
                (donors_hbm, donors),
                (weights_hbm, weights),
                (receptors_hbm, receptors),
            )
        )
    ]
    for kb in range(blocks):
        for copy in input_copies(kb):
            copy.start()
    for copy in small_copies:
        copy.start()

    has_prev_row = px > 0
    has_next_row = px < count_rows - 1
    has_prev_col = py > 0
    has_next_col = py < count_cols - 1
    prev_row = {"px": px - 1}
    next_row = {"px": px + 1}
    prev_col = {"py": py - 1}
    next_col = {"py": py + 1}
    sides = (
        (has_prev_row, prev_row),
        (has_next_row, next_row),
        (has_prev_col, prev_col),
        (has_next_col, next_col),
    )

    def other(q):
        return {"grid": 1 - grid, "px": q // count_cols, "py": q % count_cols}

    barrier = pltpu.get_barrier_semaphore()
    for there, device in sides:

        @pl.when(there)
        def _():
            pl.semaphore_signal(barrier, inc=1, device_id=device, device_id_type=MESH)

    @pl.loop(0, owner_count)
    def _(q):
        pl.semaphore_signal(barrier, inc=1, device_id=other(q), device_id_type=MESH)

    def enter():
        near = sum(there.astype(jnp.int32) for there, _ in sides)
        pl.semaphore_wait(barrier, near + owner_count)

    def ask(q):
        return pltpu.make_async_remote_copy(
            src_ref=ask_send.at[q],
            dst_ref=ask_recv.at[me],
            send_sem=ask_send_sem.at[q],
            recv_sem=ask_recv_sem.at[me],
            device_id=other(q),
            device_id_type=MESH,
        )

    def asked(q):
        return pltpu.make_async_remote_copy(
            src_ref=ask_send.at[q],
            dst_ref=ask_recv.at[q],
            send_sem=ask_send_sem.at[q],
            recv_sem=ask_recv_sem.at[q],
            device_id=other(q),
            device_id_type=MESH,
        )

    def reply(q):
        return pltpu.make_async_remote_copy(
            src_ref=reply_send.at[q],
            dst_ref=reply_recv.at[me],
            send_sem=reply_send_sem.at[q],
            recv_sem=reply_recv_sem.at[me],
            device_id=other(q),
            device_id_type=MESH,
        )

    def replied(q):
        return pltpu.make_async_remote_copy(
            src_ref=reply_send.at[q],
            dst_ref=reply_recv.at[q],
            send_sem=reply_send_sem.at[q],
            recv_sem=reply_recv_sem.at[q],
            device_id=other(q),
            device_id_type=MESH,
        )

    def digits(value):
        return [(value >> LOW).astype(jnp.float32), (value & (2**LOW - 1)).astype(jnp.float32)]

    def plan():
        for copy in small_copies:
            copy.wait()
        owner = owners[...]
        ones = jnp.where(
            owner == lax.broadcasted_iota(jnp.int32, (owner_count, count), 0), 1.0, 0.0
        )
        before = jnp.where(
            lax.broadcasted_iota(jnp.int32, (count, count), 0)
            < lax.broadcasted_iota(jnp.int32, (count, count), 1),
            1.0,
            0.0,
        ).astype(jnp.bfloat16)
        seen = jnp.dot(ones.astype(jnp.bfloat16), before, preferred_element_type=jnp.float32)
        rank = jnp.sum(seen * ones, axis=0, keepdims=True).astype(jnp.int32)
        place = owner * slot_count + rank
        weight = weights[...]
        high = weight.astype(jnp.bfloat16).astype(jnp.float32)
        mid = (weight - high).astype(jnp.bfloat16).astype(jnp.float32)
        low = weight - high - mid
        cell = receptors[...]
        marks = jnp.concatenate(
            digits(cell) + [jnp.ones((1, count), jnp.float32), jnp.zeros((ROWS - 3, count), jnp.float32)],
            axis=0,
        )
        table = jnp.concatenate(digits(donors[...]) + [high, mid, low, marks], axis=0).astype(
            jnp.bfloat16
        )
        wide = min(2 * LANES, slots)
        lane = lax.broadcasted_iota(jnp.int32, (many, LANES), 1)
        for base in range(0, slots, wide):
            slot = lax.broadcasted_iota(jnp.int32, (wide, count), 0) + base
            pick = jnp.where(slot == place, 1.0, 0.0).astype(jnp.bfloat16)
            got = lax.dot_general(
                table, pick, (((1,), (1,)), ((), ())), preferred_element_type=jnp.float32
            )
            cells = got[:many] * float(2**LOW) + got[many : 2 * many]
            share = got[2 * many : 3 * many] + got[3 * many : 4 * many] + got[4 * many : 5 * many]
            mark = got[5 * many : 5 * many + 3]
            target = (mark[0:1] * float(2**LOW) + mark[1:2]).astype(jnp.int32)
            pencil, k = divmod_const(target, length)
            kb, spot = divmod_const(k, LANES)
            line = kb * (tall * cj) + (cj - 1) * cj + pencil
            code_out[:, base : base + wide] = jnp.where(
                mark[2:3] > 0.5, line * (2 * LANES) + spot, EMPTY
            )
            for q in range(base // slot_count, (base + wide) // slot_count):
                at = q * slot_count - base
                tile = at // LANES * LANES
                shift = at - tile
                left = cells[:, tile : tile + LANES]
                right = share[:, tile : tile + LANES]
                if shift:
                    left = pltpu.roll(left, LANES - shift, 1)
                if (slot_count - shift) % LANES:
                    right = pltpu.roll(right, (slot_count - shift) % LANES, 1)
                ask_send[q] = jnp.where(lane < slot_count, left, right)

        @pl.when(ahead >= 2)
        def _():
            enter()

        @pl.loop(0, owner_count)
        def _(q):
            ask(q).start()

    def prepare():
        line = lax.broadcasted_iota(jnp.int32, (slot_count, LANES), 1)

        @pl.loop(0, owner_count)
        def _(q):
            asked(q).wait_recv()
            tile = ask_recv[q]
            cell = tile.astype(jnp.int32)
            pencil, k = divmod_const(cell, length)
            kb, _ = divmod_const(k, LANES)
            i, j = divmod_const(pencil, cj)
            row = kb * (tall * cj) + (i + (cj - 1)) * cj + j
            rows_v[pl.ds(pl.multiple_of(q * ROWS, ROWS), ROWS), :] = jnp.clip(
                row, 0, blocks * tall * cj - 1
            )
            turned = tile.T
            first = pl.multiple_of(q * slot_count, slot_count)
            for d in range(many):
                spot = turned[:slot_count, d : d + 1].astype(jnp.int32) & (LANES - 1)
                share = turned[slot_count : 2 * slot_count, d : d + 1]
                spread[d, pl.ds(first, slot_count), :] = jnp.where(line == spot, share, 0.0)

        copy = pltpu.make_async_copy(rows_v, rows_s, rows_sem)
        copy.start()
        copy.wait()

    def send(kind, kb):
        device = (next_row, next_col, prev_row, prev_col)[kind]
        return pltpu.make_async_remote_copy(
            src_ref=face_send.at[kind, kb],
            dst_ref=face_recv.at[kind, kb],
            send_sem=send_sem.at[kind, kb],
            recv_sem=recv_sem.at[kind, kb],
            device_id=device,
            device_id_type=MESH,
        )

    gets = (has_prev_row, has_prev_col, has_next_row, has_next_col)
    puts = (has_next_row, has_next_col, has_prev_row, has_prev_col)

    for kind in range(4):

        @pl.when(jnp.logical_not(gets[kind]))
        def _():
            face_recv[kind] = jnp.zeros(face_recv.shape[1:], jnp.float32)

    sub = lax.broadcasted_iota(jnp.int32, (cj, LANES), 0)

    def product(mat, vec):
        out = []
        for r in range(comps):
            terms = [mat(r * comps + c) * vec[c] for c in range(comps)]
            while len(terms) > 1:
                terms = [
                    terms[t] + terms[t + 1] if t + 1 < len(terms) else terms[t]
                    for t in range(0, len(terms), 2)
                ]
            out.append(terms[0])
        return out

    def wait_recv(kind, kb):
        @pl.when(gets[kind])
        def _():
            send(kind, kb).wait_recv()

    def start_send(kind, kb):
        @pl.when(puts[kind])
        def _():
            send(kind, kb).start()

    inv_flat = inv_v.reshape(blocks, tall * entries * cj, LANES)
    res_flat = res_v.reshape(blocks, tall * comps * cj, LANES)
    cpl_flat = cpl_v.reshape(blocks, tall * cj * ROWS, LANES)
    field_flat = field_v.reshape(blocks, tall * cj * ROWS, LANES)
    field_rows = field_v.reshape(blocks * tall * cj, ROWS, LANES)

    def entry(ref, kb, s, height, e):
        start = s * height * cj + e * cj + cj - 1
        return ref[kb, pl.ds(start, cj, stride=height * cj - 1), :]

    def cell_rows(s, c):
        return pl.ds((s * cj + cj - 1) * ROWS + c, cj, stride=(cj - 1) * ROWS)

    def forward(kb):
        for copy in input_copies(kb):
            copy.wait()
        wait_recv(0, kb)
        wait_recv(1, kb)
        upper = [face_recv[0, kb, pl.ds(c * ROWS, cj), :] for c in range(comps)]
        prev = [jnp.zeros((cj, LANES), jnp.float32)] * comps
        lower = [jnp.zeros((cj, LANES), jnp.float32)] * comps
        for s in range(steps):
            coef_a = cpl_flat[kb, cell_rows(s, 0), :]
            coef_b = cpl_flat[kb, cell_rows(s, 1), :]
            up = prev
            if s < cj:
                up = [jnp.where(sub == cj - 1 - s, upper[c], prev[c]) for c in range(comps)]
            left = [pltpu.roll(p, cj - 1, 0) for p in prev]
            if s < ci:
                left = [
                    jnp.where(
                        sub == cj - 1,
                        jnp.broadcast_to(
                            face_recv[1, kb, pl.ds(c * ROWS + s, 1), :], (cj, LANES)
                        ),
                        left[c],
                    )
                    for c in range(comps)
                ]
            vec = [
                entry(res_flat, kb, s, comps, c) + coef_a * up[c] + coef_b * left[c]
                for c in range(comps)
            ]
            prev = product(lambda e: entry(inv_flat, kb, s, entries, e), vec)
            for c in range(comps):
                star_v[kb, s, c] = prev[c]
                if s >= cj - 1:
                    face_send[1, kb, pl.ds(c * ROWS + s - cj + 1, 1), :] = prev[c][0:1, :]
                if s >= ci - 1:
                    lower[c] = jnp.where(sub == cj + ci - 2 - s, prev[c], lower[c])
        for c in range(comps):
            face_send[0, kb, pl.ds(c * ROWS, cj), :] = lower[c]

        @pl.when((kb == 0) & (ahead < 2))
        def _():
            enter()

        start_send(0, kb)
        start_send(1, kb)

    def backward(kb):
        wait_recv(2, kb)
        wait_recv(3, kb)
        under = [face_recv[2, kb, pl.ds(c * ROWS, cj), :] for c in range(comps)]
        prev = [jnp.zeros((cj, LANES), jnp.float32)] * comps
        upper = [jnp.zeros((cj, LANES), jnp.float32)] * comps
        for s in reversed(range(steps)):
            coef_e = cpl_flat[kb, cell_rows(s, 2), :]
            coef_f = cpl_flat[kb, cell_rows(s, 3), :]
            down = prev
            if s >= ci - 1:
                down = [
                    jnp.where(sub == cj + ci - 2 - s, under[c], prev[c]) for c in range(comps)
                ]
            right = [pltpu.roll(p, 1, 0) for p in prev]
            if s >= cj - 1:
                right = [
                    jnp.where(
                        sub == 0,
                        jnp.broadcast_to(
                            face_recv[3, kb, pl.ds(c * ROWS + s - cj + 1, 1), :], (cj, LANES)
                        ),
                        right[c],
                    )
                    for c in range(comps)
                ]
            vec = [coef_e * down[c] + coef_f * right[c] for c in range(comps)]
            prev = product(lambda e: entry(inv_flat, kb, s, entries, e), vec)
            prev = [star_v[kb, s, c] + prev[c] for c in range(comps)]
            for c in range(comps):
                field_flat[kb, cell_rows(s, c), :] = prev[c]
                if s < cj:
                    upper[c] = jnp.where(sub == cj - 1 - s, prev[c], upper[c])
                if s < ci:
                    face_send[3, kb, pl.ds(c * ROWS + s, 1), :] = prev[c][cj - 1 : cj, :]
        for c in range(comps):
            face_send[2, kb, pl.ds(c * ROWS, cj), :] = upper[c]
        start_send(2, kb)
        start_send(3, kb)

    middle = blocks + 1
    last = 2 * blocks + 2
    begin = jnp.where(ahead == reach, 1, blocks + 2)
    early = ahead + 2 <= reach

    @pl.loop(0, last + 1)
    def _(n):
        @pl.when(((n == 0) & (ahead >= 2)) | ((n == middle) & (ahead < 2)))
        def _():
            plan()

        @pl.when((n >= 1) & (n <= blocks))
        def _():
            forward(n - 1)

        @pl.when((n >= begin) & (n < begin + blocks))
        def _():
            backward(n - begin)

        @pl.when(((n == middle) & early) | ((n == last) & jnp.logical_not(early)))
        def _():
            prepare()

    lane8 = lax.broadcasted_iota(jnp.int32, (ROWS, LANES), 1)

    @pl.loop(0, owner_count)
    def _(q):
        acc = jnp.zeros((ROWS, LANES), jnp.float32)
        for s in range(slot_count):
            parts = [
                field_rows[rows_s[q * ROWS + d, s]]
                * spread[d, pl.ds(q * slot_count + s, 1), :]
                for d in range(many)
            ]
            while len(parts) > 1:
                parts = [parts[i] + parts[i + 1] for i in range(0, len(parts), 2)]
            total = jnp.sum(parts[0], axis=1, keepdims=True)
            acc = jnp.where(lane8 == s, total, acc)
        reply_send[q] = acc
        reply(q).start()

    @pl.loop(0, owner_count)
    def _(q):
        replied(q).wait_recv()
        reply_out[q] = reply_recv[q]

    @pl.loop(0, owner_count)
    def _(q):
        ask(q).wait_send()
        reply(q).wait_send()

    for kb in range(blocks):
        for kind in range(4):

            @pl.when(puts[kind])
            def _():
                send(kind, kb).wait_send()


def run_sweeps(residual, inverses, couplings, owners, donors, weights, receptors):
    inputs = (residual, inverses, couplings, owners, donors, weights, receptors)
    ci, comps, cj, length = residual.shape
    many, count = donors.shape
    blocks = length // LANES
    steps = ci + cj - 1
    tall = ci + 2 * (cj - 1)
    rows, cols = lax.axis_size("px"), lax.axis_size("py")
    owner_count = rows * cols
    slot_count = max(2, 2 * count // owner_count)
    slots = owner_count * slot_count
    assert cj == ROWS and ci <= ROWS and many == ROWS and 2 * slot_count <= LANES
    assert ci * cj * length <= 2 ** (2 * LOW)
    dims = (ci, cj, comps, blocks, rows, cols, slot_count)
    face = comps * ROWS
    dma = pltpu.SemaphoreType.DMA
    hbm = pl.BlockSpec(memory_space=pltpu.HBM)
    vmem = pl.BlockSpec(memory_space=pltpu.VMEM)
    return pl.pallas_call(
        functools.partial(sweep_kernel, dims),
        out_shape=(
            pltpu.VMEM((blocks, tall, cj, ROWS, LANES), jnp.float32),
            pltpu.VMEM((1, slots), jnp.int32),
            pltpu.VMEM((owner_count, ROWS, LANES), jnp.float32),
        ),
        in_specs=[hbm] * 7,
        out_specs=(vmem, vmem, vmem),
        scratch_shapes=[
            pltpu.VMEM(owners.shape, owners.dtype),
            pltpu.VMEM(donors.shape, donors.dtype),
            pltpu.VMEM(weights.shape, weights.dtype),
            pltpu.VMEM(receptors.shape, receptors.dtype),
            pltpu.VMEM((blocks, tall, comps * comps, cj, LANES), jnp.float32),
            pltpu.VMEM((blocks, tall, comps, cj, LANES), jnp.float32),
            pltpu.VMEM((blocks, tall, cj, ROWS, LANES), jnp.float32),
            pltpu.VMEM((blocks, steps, comps, cj, LANES), jnp.float32),
            pltpu.VMEM((4, blocks, face, LANES), jnp.float32),
            pltpu.VMEM((4, blocks, face, LANES), jnp.float32),
            pltpu.VMEM((owner_count, ROWS, LANES), jnp.float32),
            pltpu.VMEM((owner_count, ROWS, LANES), jnp.float32),
            pltpu.VMEM((owner_count * ROWS, LANES), jnp.int32),
            pltpu.SMEM((owner_count * ROWS, LANES), jnp.int32),
            pltpu.VMEM((many, slots, LANES), jnp.float32),
            pltpu.VMEM((owner_count, ROWS, LANES), jnp.float32),
            pltpu.VMEM((owner_count, ROWS, LANES), jnp.float32),
            dma((3, blocks)),
            dma((4,)),
            dma((4, blocks)),
            dma((4, blocks)),
            dma((owner_count,)),
            dma((owner_count,)),
            dma((owner_count,)),
            dma((owner_count,)),
            dma,
        ],
        compiler_params=pltpu.CompilerParams(
            collective_id=0, has_side_effects=True, vmem_limit_bytes=40 * 1024 * 1024
        ),
    )(*(pltpu.with_memory_space_constraint(x, pltpu.HBM) for x in inputs))


def place_kernel(dims, code, reply, field, out, work):
    ci, cj, comps, slot_count = dims
    owner_count = reply.shape[0]
    blocks, tall = field.shape[:2]
    lane = lax.broadcasted_iota(jnp.int32, (ROWS, LANES), 1)
    lines = work.reshape(blocks * tall * cj, ROWS, LANES)

    @pl.loop(0, owner_count)
    def _(q):
        tile = reply[q]
        for s in range(slot_count):
            line, spot = divmod_const(code[0, q * slot_count + s], 2 * LANES)
            value = jnp.broadcast_to(tile[:, s : s + 1], (ROWS, LANES))
            pltpu.store(lines.at[line], value, mask=lane == spot)

    stack = work.reshape(blocks, tall, cj * ROWS, LANES)

    @pl.loop(0, ci)
    def _(i):
        for kb in range(blocks):
            for c in range(comps):
                out[i, c, :, kb * LANES : (kb + 1) * LANES] = stack[
                    kb, i + cj - 1, pl.ds(c, cj, stride=ROWS), :
                ]


def run_place(code, reply, field, dims):
    ci, cj, comps, slot_count = dims
    blocks = field.shape[0]
    vmem = pl.BlockSpec(memory_space=pltpu.VMEM)
    return pl.pallas_call(
        functools.partial(place_kernel, dims),
        out_shape=(
            jax.ShapeDtypeStruct((ci, comps, cj, blocks * LANES), jnp.float32),
            jax.ShapeDtypeStruct(field.shape, jnp.float32),
        ),
        in_specs=[pl.BlockSpec(memory_space=pltpu.SMEM), vmem, vmem],
        out_specs=(vmem, vmem),
        input_output_aliases={2: 1},
        compiler_params=pltpu.CompilerParams(vmem_limit_bytes=16 * 1024 * 1024),
    )(code, reply, field)[0]


def local(residual, inverses, couplings, receptors, owners, donors, weights):
    ci, cj, comps = residual.shape[1:4]
    many = donors.shape[-1]
    count = donors.shape[-2]
    field, code, reply = run_sweeps(
        residual[0].transpose(0, 2, 1, 3),
        inverses[0].transpose(0, 2, 1, 3),
        couplings[0],
        owners.reshape(1, count),
        donors.reshape(count, many).T,
        weights.reshape(count, many).T,
        receptors.reshape(1, count),
    )
    slot_count = code.shape[1] // reply.shape[0]
    update = run_place(code, reply, field, (ci, cj, comps, slot_count))
    return update.transpose(0, 2, 1, 3)[None]


def solution(mesh):
    placed = (
        P("grid", "px", "py", None, None),
        P("grid", "px", "py", None, None),
        P("grid", "px", "py", None, None),
        P("grid", "px", "py", None),
        P("grid", "px", "py", None, None),
        P("grid", "px", "py", None, None),
        P("grid", "px", "py", None, None),
    )
    return jax.shard_map(
        local,
        mesh=mesh,
        in_specs=placed,
        out_specs=P("grid", "px", "py", None, None),
        check_vma=False,
    )
```

```python
import functools

import jax
import jax.numpy as jnp
from jax import lax
from jax.experimental import pallas as pl
from jax.experimental.pallas import tpu as pltpu
from jax.sharding import PartitionSpec as P

MESH = pl.DeviceIdType.MESH
LANES = 128
ROWS = 8
LOW = 8
EMPTY = LANES


def divmod_const(value, by):
    if by & (by - 1) == 0:
        return value >> (by.bit_length() - 1), value & (by - 1)
    return value // by, value % by


def sweep_kernel(
    dims,
    res_hbm,
    inv_hbm,
    cpl_hbm,
    owners_hbm,
    donors_hbm,
    weights_hbm,
    receptors_hbm,
    field_v,
    code_out,
    reply_out,
    owners,
    donors,
    weights,
    receptors,
    inv_v,
    res_v,
    cpl_v,
    star_v,
    face_send,
    face_recv,
    ask_send,
    ask_recv,
    rows_v,
    rows_s,
    spread,
    reply_send,
    reply_recv,
    in_sem,
    small_sem,
    send_sem,
    recv_sem,
    ask_send_sem,
    ask_recv_sem,
    reply_send_sem,
    reply_recv_sem,
    rows_sem,
    wave_sem,
):
    ci, cj, comps, blocks, count_rows, count_cols, slot_count = dims
    length = blocks * LANES
    entries = comps * comps
    steps = ci + cj - 1
    tall = ci + 2 * (cj - 1)
    many, count = donors.shape
    owner_count = count_rows * count_cols
    slots = owner_count * slot_count
    grid = lax.axis_index("grid")
    px = lax.axis_index("px")
    py = lax.axis_index("py")
    me = px * count_cols + py
    ahead = px + py
    reach = count_rows + count_cols - 2

    def input_copies(kb):
        lanes = pl.ds(pl.multiple_of(kb * LANES, LANES), LANES)
        mine = pl.ds(cj - 1, ci)
        return (
            pltpu.make_async_copy(
                inv_hbm.at[:, :, :, lanes], inv_v.at[kb, mine], in_sem.at[0, kb]
            ),
            pltpu.make_async_copy(
                res_hbm.at[:, :, :, lanes], res_v.at[kb, mine], in_sem.at[1, kb]
            ),
            pltpu.make_async_copy(
                cpl_hbm.at[:, :, :, lanes],
                cpl_v.at[kb, mine, :, pl.ds(0, 4), :],
                in_sem.at[2, kb],
            ),
        )

    small_copies = [
        pltpu.make_async_copy(source, target, small_sem.at[t])
        for t, (source, target) in enumerate(
            (
                (owners_hbm, owners),
                (donors_hbm, donors),
                (weights_hbm, weights),
                (receptors_hbm, receptors),
            )
        )
    ]
    eager = min(2, blocks)
    for kb in range(eager):
        for copy in input_copies(kb):
            copy.start()
    for copy in small_copies:
        copy.start()

    has_prev_row = px > 0
    has_next_row = px < count_rows - 1
    has_prev_col = py > 0
    has_next_col = py < count_cols - 1
    prev_row = {"px": px - 1}
    next_row = {"px": px + 1}
    prev_col = {"py": py - 1}
    next_col = {"py": py + 1}
    sides = (
        (has_prev_row, prev_row),
        (has_next_row, next_row),
        (has_prev_col, prev_col),
        (has_next_col, next_col),
    )

    def other(q):
        return {"grid": 1 - grid, "px": q // count_cols, "py": q % count_cols}

    barrier = pltpu.get_barrier_semaphore()
    for there, device in sides:

        @pl.when(there)
        def _():
            pl.semaphore_signal(barrier, inc=1, device_id=device, device_id_type=MESH)

    pl.semaphore_signal(
        barrier, inc=1, device_id={"grid": 1 - grid}, device_id_type=MESH
    )

    def enter():
        near = sum(there.astype(jnp.int32) for there, _ in sides)
        pl.semaphore_wait(barrier, near + 1)

    def wave(came_from, goes_to):
        for kind, there, _ in came_from:

            @pl.when(there)
            def _():
                pl.semaphore_wait(wave_sem.at[kind], 1)

        for kind, there, device in goes_to:

            @pl.when(there)
            def _():
                pl.semaphore_signal(
                    wave_sem.at[kind], inc=1, device_id=device, device_id_type=MESH
                )

    def wave_on():
        wave(
            ((0, has_prev_row, prev_row), (1, has_prev_col, prev_col)),
            ((0, has_next_row, next_row), (1, has_next_col, next_col)),
        )

    def wave_back():
        wave(
            ((2, has_next_row, next_row), (3, has_next_col, next_col)),
            ((2, has_prev_row, prev_row), (3, has_prev_col, prev_col)),
        )

    def ask(q):
        return pltpu.make_async_remote_copy(
            src_ref=ask_send.at[q],
            dst_ref=ask_recv.at[me],
            send_sem=ask_send_sem.at[q],
            recv_sem=ask_recv_sem.at[me],
            device_id=other(q),
            device_id_type=MESH,
        )

    def asked(q):
        return pltpu.make_async_remote_copy(
            src_ref=ask_send.at[q],
            dst_ref=ask_recv.at[q],
            send_sem=ask_send_sem.at[q],
            recv_sem=ask_recv_sem.at[q],
            device_id=other(q),
            device_id_type=MESH,
        )

    def reply(q):
        return pltpu.make_async_remote_copy(
            src_ref=reply_send.at[q],
            dst_ref=reply_recv.at[me],
            send_sem=reply_send_sem.at[q],
            recv_sem=reply_recv_sem.at[me],
            device_id=other(q),
            device_id_type=MESH,
        )

    def replied(q):
        return pltpu.make_async_remote_copy(
            src_ref=reply_send.at[q],
            dst_ref=reply_recv.at[q],
            send_sem=reply_send_sem.at[q],
            recv_sem=reply_recv_sem.at[q],
            device_id=other(q),
            device_id_type=MESH,
        )

    def digits(value):
        return [(value >> LOW).astype(jnp.float32), (value & (2**LOW - 1)).astype(jnp.float32)]

    def plan():
        for copy in small_copies:
            copy.wait()
        owner = owners[...]
        ones = jnp.where(
            owner == lax.broadcasted_iota(jnp.int32, (owner_count, count), 0), 1.0, 0.0
        )
        before = jnp.where(
            lax.broadcasted_iota(jnp.int32, (count, count), 0)
            < lax.broadcasted_iota(jnp.int32, (count, count), 1),
            1.0,
            0.0,
        ).astype(jnp.bfloat16)
        seen = jnp.dot(ones.astype(jnp.bfloat16), before, preferred_element_type=jnp.float32)
        rank = jnp.sum(seen * ones, axis=0, keepdims=True).astype(jnp.int32)
        place = owner * slot_count + rank
        weight = weights[...]
        high = weight.astype(jnp.bfloat16).astype(jnp.float32)
        mid = (weight - high).astype(jnp.bfloat16).astype(jnp.float32)
        low = weight - high - mid
        cell = receptors[...]
        marks = jnp.concatenate(
            digits(cell) + [jnp.ones((1, count), jnp.float32), jnp.zeros((ROWS - 3, count), jnp.float32)],
            axis=0,
        )
        table = jnp.concatenate(digits(donors[...]) + [high, mid, low, marks], axis=0).astype(
            jnp.bfloat16
        )
        wide = min(2 * LANES, slots)
        lane = lax.broadcasted_iota(jnp.int32, (many, LANES), 1)
        for base in range(0, slots, wide):
            slot = lax.broadcasted_iota(jnp.int32, (wide, count), 0) + base
            pick = jnp.where(slot == place, 1.0, 0.0).astype(jnp.bfloat16)
            got = lax.dot_general(
                table, pick, (((1,), (1,)), ((), ())), preferred_element_type=jnp.float32
            )
            cells = got[:many] * float(2**LOW) + got[many : 2 * many]
            share = got[2 * many : 3 * many] + got[3 * many : 4 * many] + got[4 * many : 5 * many]
            mark = got[5 * many : 5 * many + 3]
            target = (mark[0:1] * float(2**LOW) + mark[1:2]).astype(jnp.int32)
            pencil, k = divmod_const(target, length)
            kb, spot = divmod_const(k, LANES)
            line = kb * (tall * cj) + (cj - 1) * cj + pencil
            code_out[:, base : base + wide] = jnp.where(
                mark[2:3] > 0.5, line * (2 * LANES) + spot, EMPTY
            )
            for q in range(base // slot_count, (base + wide) // slot_count):
                at = q * slot_count - base
                tile = at // LANES * LANES
                shift = at - tile
                left = cells[:, tile : tile + LANES]
                right = share[:, tile : tile + LANES]
                if shift:
                    left = pltpu.roll(left, LANES - shift, 1)
                if (slot_count - shift) % LANES:
                    right = pltpu.roll(right, (slot_count - shift) % LANES, 1)
                ask_send[q] = jnp.where(lane < slot_count, left, right)

    def send_asks():
        wave_back()

        @pl.loop(0, owner_count)
        def _(q):
            ask(q).start()

    def prepare():
        line = lax.broadcasted_iota(jnp.int32, (slot_count, LANES), 1)

        @pl.loop(0, owner_count)
        def _(q):
            asked(q).wait_recv()
            tile = ask_recv[q]
            cell = tile.astype(jnp.int32)
            pencil, k = divmod_const(cell, length)
            kb, _ = divmod_const(k, LANES)
            i, j = divmod_const(pencil, cj)
            row = kb * (tall * cj) + (i + (cj - 1)) * cj + j
            rows_v[pl.ds(pl.multiple_of(q * ROWS, ROWS), ROWS), :] = jnp.clip(
                row, 0, blocks * tall * cj - 1
            )
            turned = tile.T
            first = pl.multiple_of(q * slot_count, slot_count)
            for d in range(many):
                spot = turned[:slot_count, d : d + 1].astype(jnp.int32) & (LANES - 1)
                share = turned[slot_count : 2 * slot_count, d : d + 1]
                spread[d, pl.ds(first, slot_count), :] = jnp.where(line == spot, share, 0.0)

    def fetch_rows(q, slot):
        return pltpu.make_async_copy(
            rows_v.at[pl.ds(pl.multiple_of(q * ROWS, ROWS), ROWS)],
            rows_s.at[slot],
            rows_sem.at[slot],
        )

    def send(kind, kb):
        device = (next_row, next_col, prev_row, prev_col)[kind]
        return pltpu.make_async_remote_copy(
            src_ref=face_send.at[kind, kb],
            dst_ref=face_recv.at[kind, kb],
            send_sem=send_sem.at[kind, kb],
            recv_sem=recv_sem.at[kind, kb],
            device_id=device,
            device_id_type=MESH,
        )

    idle_first = ahead >= 2
    gets = (has_prev_row, has_prev_col, has_next_row, has_next_col)
    puts = (has_next_row, has_next_col, has_prev_row, has_prev_col)

    for kind in range(4):

        @pl.when(jnp.logical_not(gets[kind]))
        def _():
            face_recv[kind] = jnp.zeros(face_recv.shape[1:], jnp.float32)

    sub = lax.broadcasted_iota(jnp.int32, (cj, LANES), 0)

    def product(mat, vec):
        out = []
        for r in range(comps):
            terms = [mat(r * comps + c) * vec[c] for c in range(comps)]
            while len(terms) > 1:
                terms = [
                    terms[t] + terms[t + 1] if t + 1 < len(terms) else terms[t]
                    for t in range(0, len(terms), 2)
                ]
            out.append(terms[0])
        return out

    def wait_recv(kind, kb):
        @pl.when(gets[kind])
        def _():
            send(kind, kb).wait_recv()

    def start_send(kind, kb):
        @pl.when(puts[kind])
        def _():
            send(kind, kb).start()

    inv_flat = inv_v.reshape(blocks, tall * entries * cj, LANES)
    res_flat = res_v.reshape(blocks, tall * comps * cj, LANES)
    cpl_flat = cpl_v.reshape(blocks, tall * cj * ROWS, LANES)
    field_flat = field_v.reshape(blocks, tall * cj * ROWS, LANES)
    field_rows = field_v.reshape(blocks * tall * cj, ROWS, LANES)

    def entry(ref, kb, s, height, e):
        start = s * height * cj + e * cj + cj - 1
        return ref[kb, pl.ds(start, cj, stride=height * cj - 1), :]

    def cell_rows(s, c):
        return pl.ds((s * cj + cj - 1) * ROWS + c, cj, stride=(cj - 1) * ROWS)

    def forward(kb):
        for copy in input_copies(kb):
            copy.wait()

        @pl.when(kb == 0)
        def _():
            for later in range(eager, blocks):
                for copy in input_copies(later):
                    copy.start()

        wait_recv(0, kb)
        wait_recv(1, kb)
        upper = [face_recv[0, kb, pl.ds(c * ROWS, cj), :] for c in range(comps)]
        prev = [jnp.zeros((cj, LANES), jnp.float32)] * comps
        lower = [jnp.zeros((cj, LANES), jnp.float32)] * comps
        for s in range(steps):
            coef_a = cpl_flat[kb, cell_rows(s, 0), :]
            coef_b = cpl_flat[kb, cell_rows(s, 1), :]
            up = prev
            if s < cj:
                up = [jnp.where(sub == cj - 1 - s, upper[c], prev[c]) for c in range(comps)]
            left = [pltpu.roll(p, cj - 1, 0) for p in prev]
            if s < ci:
                left = [
                    jnp.where(
                        sub == cj - 1,
                        jnp.broadcast_to(
                            face_recv[1, kb, pl.ds(c * ROWS + s, 1), :], (cj, LANES)
                        ),
                        left[c],
                    )
                    for c in range(comps)
                ]
            vec = [
                entry(res_flat, kb, s, comps, c) + coef_a * up[c] + coef_b * left[c]
                for c in range(comps)
            ]
            prev = product(lambda e: entry(inv_flat, kb, s, entries, e), vec)
            for c in range(comps):
                star_v[kb, s, c] = prev[c]
                if s >= cj - 1:
                    face_send[1, kb, pl.ds(c * ROWS + s - cj + 1, 1), :] = prev[c][0:1, :]
                if s >= ci - 1:
                    lower[c] = jnp.where(sub == cj + ci - 2 - s, prev[c], lower[c])
        for c in range(comps):
            face_send[0, kb, pl.ds(c * ROWS, cj), :] = lower[c]

        @pl.when((kb == 0) & jnp.logical_not(idle_first))
        def _():
            enter()

        start_send(0, kb)
        start_send(1, kb)

        @pl.when((kb == 0) & jnp.logical_not(idle_first))
        def _():
            wave_on()

    def backward(kb):
        wait_recv(2, kb)
        wait_recv(3, kb)
        under = [face_recv[2, kb, pl.ds(c * ROWS, cj), :] for c in range(comps)]
        prev = [jnp.zeros((cj, LANES), jnp.float32)] * comps
        upper = [jnp.zeros((cj, LANES), jnp.float32)] * comps
        for s in reversed(range(steps)):
            coef_e = cpl_flat[kb, cell_rows(s, 2), :]
            coef_f = cpl_flat[kb, cell_rows(s, 3), :]
            down = prev
            if s >= ci - 1:
                down = [
                    jnp.where(sub == cj + ci - 2 - s, under[c], prev[c]) for c in range(comps)
                ]
            right = [pltpu.roll(p, 1, 0) for p in prev]
            if s >= cj - 1:
                right = [
                    jnp.where(
                        sub == 0,
                        jnp.broadcast_to(
                            face_recv[3, kb, pl.ds(c * ROWS + s - cj + 1, 1), :], (cj, LANES)
                        ),
                        right[c],
                    )
                    for c in range(comps)
                ]
            vec = [coef_e * down[c] + coef_f * right[c] for c in range(comps)]
            prev = product(lambda e: entry(inv_flat, kb, s, entries, e), vec)
            prev = [star_v[kb, s, c] + prev[c] for c in range(comps)]
            for c in range(comps):
                field_flat[kb, cell_rows(s, c), :] = prev[c]
                if s < cj:
                    upper[c] = jnp.where(sub == cj - 1 - s, prev[c], upper[c])
                if s < ci:
                    face_send[3, kb, pl.ds(c * ROWS + s, 1), :] = prev[c][cj - 1 : cj, :]
        for c in range(comps):
            face_send[2, kb, pl.ds(c * ROWS, cj), :] = upper[c]
        start_send(2, kb)
        start_send(3, kb)

    middle = blocks + 1
    last = 2 * blocks + 2
    begin = jnp.where(ahead == reach, 1, blocks + 2)
    early = ahead + 3 <= reach
    asks_first = ahead * 3 >= reach * 2

    @pl.loop(0, last + 1)
    def _(n):
        @pl.when((n == 0) & idle_first)
        def _():
            enter()
            wave_on()

        @pl.when(((n == 0) & idle_first) | ((n == middle) & jnp.logical_not(idle_first)))
        def _():
            plan()

        @pl.when(((n == 0) & asks_first) | ((n == middle) & jnp.logical_not(asks_first)))
        def _():
            send_asks()

        @pl.when((n >= 1) & (n <= blocks))
        def _():
            forward(n - 1)

        @pl.when((n >= begin) & (n < begin + blocks))
        def _():
            backward(n - begin)

        @pl.when(((n == middle) & early) | ((n == last) & jnp.logical_not(early)))
        def _():
            prepare()

    lane8 = lax.broadcasted_iota(jnp.int32, (ROWS, LANES), 1)

    def gather(q, slot):
        acc = jnp.zeros((ROWS, LANES), jnp.float32)
        for s in range(slot_count):
            parts = [
                field_rows[rows_s[slot, d, s]] * spread[d, pl.ds(q * slot_count + s, 1), :]
                for d in range(many)
            ]
            while len(parts) > 1:
                parts = [parts[i] + parts[i + 1] for i in range(0, len(parts), 2)]
            total = jnp.sum(parts[0], axis=1, keepdims=True)
            acc = jnp.where(lane8 == s, total, acc)
        reply_send[q] = acc
        reply(q).start()

    fetch_rows(0, 0).start()

    @pl.loop(0, owner_count // 2)
    def _(pair):
        q = 2 * pair
        fetch_rows(q + 1, 1).start()
        fetch_rows(q, 0).wait()
        gather(q, 0)

        @pl.when(pair + 1 < owner_count // 2)
        def _():
            fetch_rows(q + 2, 0).start()

        fetch_rows(q + 1, 1).wait()
        gather(q + 1, 1)

    @pl.loop(0, owner_count)
    def _(q):
        replied(q).wait_recv()
        reply_out[q] = reply_recv[q]

    @pl.loop(0, owner_count)
    def _(q):
        ask(q).wait_send()
        reply(q).wait_send()

    for kb in range(blocks):
        for kind in range(4):

            @pl.when(puts[kind])
            def _():
                send(kind, kb).wait_send()


def run_sweeps(residual, inverses, couplings, owners, donors, weights, receptors):
    inputs = (residual, inverses, couplings, owners, donors, weights, receptors)
    ci, comps, cj, length = residual.shape
    many, count = donors.shape
    blocks = length // LANES
    steps = ci + cj - 1
    tall = ci + 2 * (cj - 1)
    rows, cols = lax.axis_size("px"), lax.axis_size("py")
    owner_count = rows * cols
    slot_count = max(2, 2 * count // owner_count)
    slots = owner_count * slot_count
    assert owner_count % 2 == 0 and cj == ROWS and ci <= ROWS and many == ROWS and 2 * slot_count <= LANES
    assert ci * cj * length <= 2 ** (2 * LOW)
    dims = (ci, cj, comps, blocks, rows, cols, slot_count)
    face = comps * ROWS
    dma = pltpu.SemaphoreType.DMA
    hbm = pl.BlockSpec(memory_space=pltpu.HBM)
    vmem = pl.BlockSpec(memory_space=pltpu.VMEM)
    return pl.pallas_call(
        functools.partial(sweep_kernel, dims),
        out_shape=(
            pltpu.VMEM((blocks, tall, cj, ROWS, LANES), jnp.float32),
            pltpu.VMEM((1, slots), jnp.int32),
            pltpu.VMEM((owner_count, ROWS, LANES), jnp.float32),
        ),
        in_specs=[hbm] * 7,
        out_specs=(vmem, vmem, vmem),
        scratch_shapes=[
            pltpu.VMEM(owners.shape, owners.dtype),
            pltpu.VMEM(donors.shape, donors.dtype),
            pltpu.VMEM(weights.shape, weights.dtype),
            pltpu.VMEM(receptors.shape, receptors.dtype),
            pltpu.VMEM((blocks, tall, comps * comps, cj, LANES), jnp.float32),
            pltpu.VMEM((blocks, tall, comps, cj, LANES), jnp.float32),
            pltpu.VMEM((blocks, tall, cj, ROWS, LANES), jnp.float32),
            pltpu.VMEM((blocks, steps, comps, cj, LANES), jnp.float32),
            pltpu.VMEM((4, blocks, face, LANES), jnp.float32),
            pltpu.VMEM((4, blocks, face, LANES), jnp.float32),
            pltpu.VMEM((owner_count, ROWS, LANES), jnp.float32),
            pltpu.VMEM((owner_count, ROWS, LANES), jnp.float32),
            pltpu.VMEM((owner_count * ROWS, LANES), jnp.int32),
            pltpu.SMEM((2, ROWS, LANES), jnp.int32),
            pltpu.VMEM((many, slots, LANES), jnp.float32),
            pltpu.VMEM((owner_count, ROWS, LANES), jnp.float32),
            pltpu.VMEM((owner_count, ROWS, LANES), jnp.float32),
            dma((3, blocks)),
            dma((4,)),
            dma((4, blocks)),
            dma((4, blocks)),
            dma((owner_count,)),
            dma((owner_count,)),
            dma((owner_count,)),
            dma((owner_count,)),
            dma((2,)),
            pltpu.SemaphoreType.REGULAR((4,)),
        ],
        compiler_params=pltpu.CompilerParams(
            collective_id=0, has_side_effects=True, vmem_limit_bytes=40 * 1024 * 1024
        ),
    )(*(pltpu.with_memory_space_constraint(x, pltpu.HBM) for x in inputs))


def place_kernel(dims, code, reply, field, out, work):
    ci, cj, comps, slot_count = dims
    owner_count = reply.shape[0]
    blocks, tall = field.shape[:2]
    lane = lax.broadcasted_iota(jnp.int32, (ROWS, LANES), 1)
    lines = work.reshape(blocks * tall * cj, ROWS, LANES)

    @pl.loop(0, owner_count)
    def _(q):
        tile = reply[q]
        for s in range(slot_count):
            line, spot = divmod_const(code[0, q * slot_count + s], 2 * LANES)
            value = jnp.broadcast_to(tile[:, s : s + 1], (ROWS, LANES))
            pltpu.store(lines.at[line], value, mask=lane == spot)

    stack = work.reshape(blocks, tall, cj * ROWS, LANES)

    @pl.loop(0, ci)
    def _(i):
        for kb in range(blocks):
            for c in range(comps):
                out[i, c, :, kb * LANES : (kb + 1) * LANES] = stack[
                    kb, i + cj - 1, pl.ds(c, cj, stride=ROWS), :
                ]


def run_place(code, reply, field, dims):
    ci, cj, comps, slot_count = dims
    blocks = field.shape[0]
    vmem = pl.BlockSpec(memory_space=pltpu.VMEM)
    return pl.pallas_call(
        functools.partial(place_kernel, dims),
        out_shape=(
            jax.ShapeDtypeStruct((ci, comps, cj, blocks * LANES), jnp.float32),
            jax.ShapeDtypeStruct(field.shape, jnp.float32),
        ),
        in_specs=[pl.BlockSpec(memory_space=pltpu.SMEM), vmem, vmem],
        out_specs=(vmem, vmem),
        input_output_aliases={2: 1},
        compiler_params=pltpu.CompilerParams(vmem_limit_bytes=16 * 1024 * 1024),
    )(code, reply, field)[0]


def local(residual, inverses, couplings, receptors, owners, donors, weights):
    ci, cj, comps = residual.shape[1:4]
    many = donors.shape[-1]
    count = donors.shape[-2]
    field, code, reply = run_sweeps(
        residual[0].transpose(0, 2, 1, 3),
        inverses[0].transpose(0, 2, 1, 3),
        couplings[0],
        owners.reshape(1, count),
        donors.reshape(count, many).T,
        weights.reshape(count, many).T,
        receptors.reshape(1, count),
    )
    slot_count = code.shape[1] // reply.shape[0]
    update = run_place(code, reply, field, (ci, cj, comps, slot_count))
    return update.transpose(0, 2, 1, 3)[None]


def solution(mesh):
    placed = (
        P("grid", "px", "py", None, None),
        P("grid", "px", "py", None, None),
        P("grid", "px", "py", None, None),
        P("grid", "px", "py", None),
        P("grid", "px", "py", None, None),
        P("grid", "px", "py", None, None),
        P("grid", "px", "py", None, None),
    )
    return jax.shard_map(
        local,
        mesh=mesh,
        in_specs=placed,
        out_specs=P("grid", "px", "py", None, None),
        check_vma=False,
    )
```

```python
import functools

import jax
import jax.numpy as jnp
from jax import lax
from jax.experimental import pallas as pl
from jax.experimental.pallas import tpu as pltpu
from jax.sharding import PartitionSpec as P

MESH = pl.DeviceIdType.MESH
LANES = 128
ROWS = 8
LOW = 8
EMPTY = LANES
FETCHES = 4


def divmod_const(value, by):
    if by & (by - 1) == 0:
        return value >> (by.bit_length() - 1), value & (by - 1)
    return value // by, value % by


def sweep_kernel(
    dims,
    res_hbm,
    inv_hbm,
    cpl_hbm,
    owners_hbm,
    donors_hbm,
    weights_hbm,
    receptors_hbm,
    field_v,
    code_out,
    reply_out,
    owners,
    donors,
    weights,
    receptors,
    inv_v,
    res_v,
    cpl_v,
    star_v,
    face_send,
    face_recv,
    ask_send,
    ask_recv,
    rows_v,
    rows_s,
    spread,
    reply_send,
    reply_recv,
    in_sem,
    small_sem,
    send_sem,
    recv_sem,
    ask_send_sem,
    ask_recv_sem,
    reply_send_sem,
    reply_recv_sem,
    rows_sem,
    wave_sem,
):
    ci, cj, comps, blocks, count_rows, count_cols, slot_count = dims
    length = blocks * LANES
    entries = comps * comps
    steps = ci + cj - 1
    tall = ci + 2 * (cj - 1)
    many, count = donors.shape
    owner_count = count_rows * count_cols
    slots = owner_count * slot_count
    grid = lax.axis_index("grid")
    px = lax.axis_index("px")
    py = lax.axis_index("py")
    me = px * count_cols + py
    ahead = px + py
    reach = count_rows + count_cols - 2

    def input_copies(kb):
        lanes = pl.ds(pl.multiple_of(kb * LANES, LANES), LANES)
        mine = pl.ds(cj - 1, ci)
        return (
            pltpu.make_async_copy(
                inv_hbm.at[:, :, :, lanes], inv_v.at[kb, mine], in_sem.at[0, kb]
            ),
            pltpu.make_async_copy(
                res_hbm.at[:, :, :, lanes], res_v.at[kb, mine], in_sem.at[1, kb]
            ),
            pltpu.make_async_copy(
                cpl_hbm.at[:, :, :, lanes],
                cpl_v.at[kb, mine, :, pl.ds(0, 4), :],
                in_sem.at[2, kb],
            ),
        )

    small_copies = [
        pltpu.make_async_copy(source, target, small_sem.at[t])
        for t, (source, target) in enumerate(
            (
                (owners_hbm, owners),
                (donors_hbm, donors),
                (weights_hbm, weights),
                (receptors_hbm, receptors),
            )
        )
    ]
    eager = min(2, blocks)
    for kb in range(eager):
        for copy in input_copies(kb):
            copy.start()
    for copy in small_copies:
        copy.start()

    has_prev_row = px > 0
    has_next_row = px < count_rows - 1
    has_prev_col = py > 0
    has_next_col = py < count_cols - 1
    prev_row = {"px": px - 1}
    next_row = {"px": px + 1}
    prev_col = {"py": py - 1}
    next_col = {"py": py + 1}
    sides = (
        (has_prev_row, prev_row),
        (has_next_row, next_row),
        (has_prev_col, prev_col),
        (has_next_col, next_col),
    )

    def other(q):
        return {"grid": 1 - grid, "px": q // count_cols, "py": q % count_cols}

    barrier = pltpu.get_barrier_semaphore()
    for there, device in sides:

        @pl.when(there)
        def _():
            pl.semaphore_signal(barrier, inc=1, device_id=device, device_id_type=MESH)

    pl.semaphore_signal(
        barrier, inc=1, device_id={"grid": 1 - grid}, device_id_type=MESH
    )

    def enter():
        near = sum(there.astype(jnp.int32) for there, _ in sides)
        pl.semaphore_wait(barrier, near + 1)

    def wave(came_from, goes_to):
        for kind, there, _ in came_from:

            @pl.when(there)
            def _():
                pl.semaphore_wait(wave_sem.at[kind], 1)

        for kind, there, device in goes_to:

            @pl.when(there)
            def _():
                pl.semaphore_signal(
                    wave_sem.at[kind], inc=1, device_id=device, device_id_type=MESH
                )

    def wave_on():
        wave(
            ((0, has_prev_row, prev_row), (1, has_prev_col, prev_col)),
            ((0, has_next_row, next_row), (1, has_next_col, next_col)),
        )

    def wave_back():
        wave(
            ((2, has_next_row, next_row), (3, has_next_col, next_col)),
            ((2, has_prev_row, prev_row), (3, has_prev_col, prev_col)),
        )

    def ask(q):
        return pltpu.make_async_remote_copy(
            src_ref=ask_send.at[q],
            dst_ref=ask_recv.at[me],
            send_sem=ask_send_sem.at[q],
            recv_sem=ask_recv_sem.at[me],
            device_id=other(q),
            device_id_type=MESH,
        )

    def asked(q):
        return pltpu.make_async_remote_copy(
            src_ref=ask_send.at[q],
            dst_ref=ask_recv.at[q],
            send_sem=ask_send_sem.at[q],
            recv_sem=ask_recv_sem.at[q],
            device_id=other(q),
            device_id_type=MESH,
        )

    def reply(q):
        return pltpu.make_async_remote_copy(
            src_ref=reply_send.at[q],
            dst_ref=reply_recv.at[me],
            send_sem=reply_send_sem.at[q],
            recv_sem=reply_recv_sem.at[me],
            device_id=other(q),
            device_id_type=MESH,
        )

    def replied(q):
        return pltpu.make_async_remote_copy(
            src_ref=reply_send.at[q],
            dst_ref=reply_recv.at[q],
            send_sem=reply_send_sem.at[q],
            recv_sem=reply_recv_sem.at[q],
            device_id=other(q),
            device_id_type=MESH,
        )

    def digits(value):
        return [(value >> LOW).astype(jnp.float32), (value & (2**LOW - 1)).astype(jnp.float32)]

    def plan():
        for copy in small_copies:
            copy.wait()
        owner = owners[...]
        ones = jnp.where(
            owner == lax.broadcasted_iota(jnp.int32, (owner_count, count), 0), 1.0, 0.0
        )
        before = jnp.where(
            lax.broadcasted_iota(jnp.int32, (count, count), 0)
            < lax.broadcasted_iota(jnp.int32, (count, count), 1),
            1.0,
            0.0,
        ).astype(jnp.bfloat16)
        seen = jnp.dot(ones.astype(jnp.bfloat16), before, preferred_element_type=jnp.float32)
        rank = jnp.sum(seen * ones, axis=0, keepdims=True).astype(jnp.int32)
        place = owner * slot_count + rank
        weight = weights[...]
        high = weight.astype(jnp.bfloat16).astype(jnp.float32)
        mid = (weight - high).astype(jnp.bfloat16).astype(jnp.float32)
        low = weight - high - mid
        cell = receptors[...]
        marks = jnp.concatenate(
            digits(cell) + [jnp.ones((1, count), jnp.float32), jnp.zeros((ROWS - 3, count), jnp.float32)],
            axis=0,
        )
        table = jnp.concatenate(digits(donors[...]) + [high, mid, low, marks], axis=0).astype(
            jnp.bfloat16
        )
        wide = min(2 * LANES, slots)
        lane = lax.broadcasted_iota(jnp.int32, (many, LANES), 1)
        for base in range(0, slots, wide):
            slot = lax.broadcasted_iota(jnp.int32, (wide, count), 0) + base
            pick = jnp.where(slot == place, 1.0, 0.0).astype(jnp.bfloat16)
            got = lax.dot_general(
                table, pick, (((1,), (1,)), ((), ())), preferred_element_type=jnp.float32
            )
            cells = got[:many] * float(2**LOW) + got[many : 2 * many]
            share = got[2 * many : 3 * many] + got[3 * many : 4 * many] + got[4 * many : 5 * many]
            mark = got[5 * many : 5 * many + 3]
            target = (mark[0:1] * float(2**LOW) + mark[1:2]).astype(jnp.int32)
            pencil, k = divmod_const(target, length)
            kb, spot = divmod_const(k, LANES)
            line = kb * (tall * cj) + (cj - 1) * cj + pencil
            code_out[:, base : base + wide] = jnp.where(
                mark[2:3] > 0.5, line * (2 * LANES) + spot, EMPTY
            )
            for q in range(base // slot_count, (base + wide) // slot_count):
                at = q * slot_count - base
                tile = at // LANES * LANES
                shift = at - tile
                left = cells[:, tile : tile + LANES]
                right = share[:, tile : tile + LANES]
                if shift:
                    left = pltpu.roll(left, LANES - shift, 1)
                if (slot_count - shift) % LANES:
                    right = pltpu.roll(right, (slot_count - shift) % LANES, 1)
                ask_send[q] = jnp.where(lane < slot_count, left, right)

    def send_asks():
        wave_back()

        @pl.loop(0, owner_count)
        def _(q):
            ask(q).start()

    def prepare():
        line = lax.broadcasted_iota(jnp.int32, (slot_count, LANES), 1)

        @pl.loop(0, owner_count)
        def _(q):
            asked(q).wait_recv()
            tile = ask_recv[q]
            cell = tile.astype(jnp.int32)
            pencil, k = divmod_const(cell, length)
            kb, _ = divmod_const(k, LANES)
            i, j = divmod_const(pencil, cj)
            row = kb * (tall * cj) + (i + (cj - 1)) * cj + j
            rows_v[pl.ds(pl.multiple_of(q * ROWS, ROWS), ROWS), :] = jnp.clip(
                row, 0, blocks * tall * cj - 1
            )
            turned = tile.T
            first = pl.multiple_of(q * slot_count, slot_count)
            for d in range(many):
                spot = turned[:slot_count, d : d + 1].astype(jnp.int32) & (LANES - 1)
                share = turned[slot_count : 2 * slot_count, d : d + 1]
                spread[d, pl.ds(first, slot_count), :] = jnp.where(line == spot, share, 0.0)

    def fetch_rows(q, slot):
        return pltpu.make_async_copy(
            rows_v.at[pl.ds(pl.multiple_of(q * ROWS, ROWS), ROWS)],
            rows_s.at[slot],
            rows_sem.at[slot],
        )

    def send(kind, kb):
        device = (next_row, next_col, prev_row, prev_col)[kind]
        return pltpu.make_async_remote_copy(
            src_ref=face_send.at[kind, kb],
            dst_ref=face_recv.at[kind, kb],
            send_sem=send_sem.at[kind, kb],
            recv_sem=recv_sem.at[kind, kb],
            device_id=device,
            device_id_type=MESH,
        )

    wave_first = ahead >= 1
    idle_first = ahead >= 2
    gets = (has_prev_row, has_prev_col, has_next_row, has_next_col)
    puts = (has_next_row, has_next_col, has_prev_row, has_prev_col)

    for kind in range(4):

        @pl.when(jnp.logical_not(gets[kind]))
        def _():
            face_recv[kind] = jnp.zeros(face_recv.shape[1:], jnp.float32)

    sub = lax.broadcasted_iota(jnp.int32, (cj, LANES), 0)

    def product(mat, vec):
        out = []
        for r in range(comps):
            terms = [mat(r * comps + c) * vec[c] for c in range(comps)]
            while len(terms) > 1:
                terms = [
                    terms[t] + terms[t + 1] if t + 1 < len(terms) else terms[t]
                    for t in range(0, len(terms), 2)
                ]
            out.append(terms[0])
        return out

    def wait_recv(kind, kb):
        @pl.when(gets[kind])
        def _():
            send(kind, kb).wait_recv()

    def start_send(kind, kb):
        @pl.when(puts[kind])
        def _():
            send(kind, kb).start()

    inv_flat = inv_v.reshape(blocks, tall * entries * cj, LANES)
    res_flat = res_v.reshape(blocks, tall * comps * cj, LANES)
    cpl_flat = cpl_v.reshape(blocks, tall * cj * ROWS, LANES)
    field_flat = field_v.reshape(blocks, tall * cj * ROWS, LANES)
    field_rows = field_v.reshape(blocks * tall * cj, ROWS, LANES)

    def entry(ref, kb, s, height, e):
        start = s * height * cj + e * cj + cj - 1
        return ref[kb, pl.ds(start, cj, stride=height * cj - 1), :]

    def cell_rows(s, c):
        return pl.ds((s * cj + cj - 1) * ROWS + c, cj, stride=(cj - 1) * ROWS)

    def forward(kb):
        for copy in input_copies(kb):
            copy.wait()

        @pl.when(kb == 0)
        def _():
            for later in range(eager, blocks):
                for copy in input_copies(later):
                    copy.start()

        wait_recv(0, kb)
        wait_recv(1, kb)
        upper = [face_recv[0, kb, pl.ds(c * ROWS, cj), :] for c in range(comps)]
        prev = [jnp.zeros((cj, LANES), jnp.float32)] * comps
        lower = [jnp.zeros((cj, LANES), jnp.float32)] * comps
        for s in range(steps):
            coef_a = cpl_flat[kb, cell_rows(s, 0), :]
            coef_b = cpl_flat[kb, cell_rows(s, 1), :]
            up = prev
            if s < cj:
                up = [jnp.where(sub == cj - 1 - s, upper[c], prev[c]) for c in range(comps)]
            left = [pltpu.roll(p, cj - 1, 0) for p in prev]
            if s < ci:
                left = [
                    jnp.where(
                        sub == cj - 1,
                        jnp.broadcast_to(
                            face_recv[1, kb, pl.ds(c * ROWS + s, 1), :], (cj, LANES)
                        ),
                        left[c],
                    )
                    for c in range(comps)
                ]
            vec = [
                entry(res_flat, kb, s, comps, c) + coef_a * up[c] + coef_b * left[c]
                for c in range(comps)
            ]
            prev = product(lambda e: entry(inv_flat, kb, s, entries, e), vec)
            for c in range(comps):
                star_v[kb, s, c] = prev[c]
                if s >= cj - 1:
                    face_send[1, kb, pl.ds(c * ROWS + s - cj + 1, 1), :] = prev[c][0:1, :]
                if s >= ci - 1:
                    lower[c] = jnp.where(sub == cj + ci - 2 - s, prev[c], lower[c])
        for c in range(comps):
            face_send[0, kb, pl.ds(c * ROWS, cj), :] = lower[c]

        @pl.when((kb == 0) & jnp.logical_not(wave_first))
        def _():
            enter()

        start_send(0, kb)
        start_send(1, kb)

        @pl.when((kb == 0) & jnp.logical_not(wave_first))
        def _():
            wave_on()

    def backward(kb):
        wait_recv(2, kb)
        wait_recv(3, kb)
        under = [face_recv[2, kb, pl.ds(c * ROWS, cj), :] for c in range(comps)]
        prev = [jnp.zeros((cj, LANES), jnp.float32)] * comps
        upper = [jnp.zeros((cj, LANES), jnp.float32)] * comps
        for s in reversed(range(steps)):
            coef_e = cpl_flat[kb, cell_rows(s, 2), :]
            coef_f = cpl_flat[kb, cell_rows(s, 3), :]
            down = prev
            if s >= ci - 1:
                down = [
                    jnp.where(sub == cj + ci - 2 - s, under[c], prev[c]) for c in range(comps)
                ]
            right = [pltpu.roll(p, 1, 0) for p in prev]
            if s >= cj - 1:
                right = [
                    jnp.where(
                        sub == 0,
                        jnp.broadcast_to(
                            face_recv[3, kb, pl.ds(c * ROWS + s - cj + 1, 1), :], (cj, LANES)
                        ),
                        right[c],
                    )
                    for c in range(comps)
                ]
            vec = [coef_e * down[c] + coef_f * right[c] for c in range(comps)]
            prev = product(lambda e: entry(inv_flat, kb, s, entries, e), vec)
            prev = [star_v[kb, s, c] + prev[c] for c in range(comps)]
            for c in range(comps):
                field_flat[kb, cell_rows(s, c), :] = prev[c]
                if s < cj:
                    upper[c] = jnp.where(sub == cj - 1 - s, prev[c], upper[c])
                if s < ci:
                    face_send[3, kb, pl.ds(c * ROWS + s, 1), :] = prev[c][cj - 1 : cj, :]
        for c in range(comps):
            face_send[2, kb, pl.ds(c * ROWS, cj), :] = upper[c]
        start_send(2, kb)
        start_send(3, kb)

    middle = blocks + 1
    last = 2 * blocks + 2
    begin = jnp.where(ahead == reach, 1, blocks + 2)
    early = ahead * 3 <= reach
    asks_first = ahead * 3 >= reach * 2

    @pl.loop(0, last + 1)
    def _(n):
        @pl.when((n == 0) & wave_first)
        def _():
            enter()
            wave_on()

        @pl.when(((n == 0) & idle_first) | ((n == middle) & jnp.logical_not(idle_first)))
        def _():
            plan()

        @pl.when(((n == 0) & asks_first) | ((n == middle) & jnp.logical_not(asks_first)))
        def _():
            send_asks()

        @pl.when((n >= 1) & (n <= blocks))
        def _():
            forward(n - 1)

        @pl.when((n >= begin) & (n < begin + blocks))
        def _():
            backward(n - begin)

        @pl.when(((n == middle) & early) | ((n == last) & jnp.logical_not(early)))
        def _():
            prepare()

    lane8 = lax.broadcasted_iota(jnp.int32, (ROWS, LANES), 1)

    def gather(q, slot):
        acc = jnp.zeros((ROWS, LANES), jnp.float32)
        for s in range(slot_count):
            parts = [
                field_rows[rows_s[slot, d, s]] * spread[d, pl.ds(q * slot_count + s, 1), :]
                for d in range(many)
            ]
            while len(parts) > 1:
                parts = [parts[i] + parts[i + 1] for i in range(0, len(parts), 2)]
            total = jnp.sum(parts[0], axis=1, keepdims=True)
            acc = jnp.where(lane8 == s, total, acc)
        reply_send[q] = acc
        reply(q).start()

    for slot in range(FETCHES - 1):
        fetch_rows(slot, slot).start()

    @pl.loop(0, owner_count // FETCHES)
    def _(turn):
        for slot in range(FETCHES):
            q = turn * FETCHES + slot
            following = q + FETCHES - 1

            @pl.when(following < owner_count)
            def _():
                fetch_rows(following, (slot + FETCHES - 1) % FETCHES).start()

            fetch_rows(q, slot).wait()
            gather(q, slot)

    @pl.loop(0, owner_count)
    def _(q):
        replied(q).wait_recv()
        reply_out[q] = reply_recv[q]

    @pl.loop(0, owner_count)
    def _(q):
        ask(q).wait_send()
        reply(q).wait_send()

    for kb in range(blocks):
        for kind in range(4):

            @pl.when(puts[kind])
            def _():
                send(kind, kb).wait_send()


def run_sweeps(residual, inverses, couplings, owners, donors, weights, receptors):
    inputs = (residual, inverses, couplings, owners, donors, weights, receptors)
    ci, comps, cj, length = residual.shape
    many, count = donors.shape
    blocks = length // LANES
    steps = ci + cj - 1
    tall = ci + 2 * (cj - 1)
    rows, cols = lax.axis_size("px"), lax.axis_size("py")
    owner_count = rows * cols
    slot_count = max(2, 2 * count // owner_count)
    slots = owner_count * slot_count
    assert owner_count % FETCHES == 0 and cj == ROWS and ci <= ROWS and many == ROWS and 2 * slot_count <= LANES
    assert ci * cj * length <= 2 ** (2 * LOW)
    dims = (ci, cj, comps, blocks, rows, cols, slot_count)
    face = comps * ROWS
    dma = pltpu.SemaphoreType.DMA
    hbm = pl.BlockSpec(memory_space=pltpu.HBM)
    vmem = pl.BlockSpec(memory_space=pltpu.VMEM)
    return pl.pallas_call(
        functools.partial(sweep_kernel, dims),
        out_shape=(
            pltpu.VMEM((blocks, tall, cj, ROWS, LANES), jnp.float32),
            pltpu.VMEM((1, slots), jnp.int32),
            pltpu.VMEM((owner_count, ROWS, LANES), jnp.float32),
        ),
        in_specs=[hbm] * 7,
        out_specs=(vmem, vmem, vmem),
        scratch_shapes=[
            pltpu.VMEM(owners.shape, owners.dtype),
            pltpu.VMEM(donors.shape, donors.dtype),
            pltpu.VMEM(weights.shape, weights.dtype),
            pltpu.VMEM(receptors.shape, receptors.dtype),
            pltpu.VMEM((blocks, tall, comps * comps, cj, LANES), jnp.float32),
            pltpu.VMEM((blocks, tall, comps, cj, LANES), jnp.float32),
            pltpu.VMEM((blocks, tall, cj, ROWS, LANES), jnp.float32),
            pltpu.VMEM((blocks, steps, comps, cj, LANES), jnp.float32),
            pltpu.VMEM((4, blocks, face, LANES), jnp.float32),
            pltpu.VMEM((4, blocks, face, LANES), jnp.float32),
            pltpu.VMEM((owner_count, ROWS, LANES), jnp.float32),
            pltpu.VMEM((owner_count, ROWS, LANES), jnp.float32),
            pltpu.VMEM((owner_count * ROWS, LANES), jnp.int32),
            pltpu.SMEM((FETCHES, ROWS, LANES), jnp.int32),
            pltpu.VMEM((many, slots, LANES), jnp.float32),
            pltpu.VMEM((owner_count, ROWS, LANES), jnp.float32),
            pltpu.VMEM((owner_count, ROWS, LANES), jnp.float32),
            dma((3, blocks)),
            dma((4,)),
            dma((4, blocks)),
            dma((4, blocks)),
            dma((owner_count,)),
            dma((owner_count,)),
            dma((owner_count,)),
            dma((owner_count,)),
            dma((FETCHES,)),
            pltpu.SemaphoreType.REGULAR((4,)),
        ],
        compiler_params=pltpu.CompilerParams(
            collective_id=0, has_side_effects=True, vmem_limit_bytes=40 * 1024 * 1024
        ),
    )(*(pltpu.with_memory_space_constraint(x, pltpu.HBM) for x in inputs))


def place_kernel(dims, code, reply, field, out, work):
    ci, cj, comps, slot_count = dims
    owner_count = reply.shape[0]
    blocks, tall = field.shape[:2]
    lane = lax.broadcasted_iota(jnp.int32, (ROWS, LANES), 1)
    lines = work.reshape(blocks * tall * cj, ROWS, LANES)

    @pl.loop(0, owner_count)
    def _(q):
        tile = reply[q]
        for s in range(slot_count):
            line, spot = divmod_const(code[0, q * slot_count + s], 2 * LANES)
            value = jnp.broadcast_to(tile[:, s : s + 1], (ROWS, LANES))
            pltpu.store(lines.at[line], value, mask=lane == spot)

    stack = work.reshape(blocks, tall, cj * ROWS, LANES)

    @pl.loop(0, ci)
    def _(i):
        for kb in range(blocks):
            for c in range(comps):
                out[i, c, :, kb * LANES : (kb + 1) * LANES] = stack[
                    kb, i + cj - 1, pl.ds(c, cj, stride=ROWS), :
                ]


def run_place(code, reply, field, dims):
    ci, cj, comps, slot_count = dims
    blocks = field.shape[0]
    vmem = pl.BlockSpec(memory_space=pltpu.VMEM)
    return pl.pallas_call(
        functools.partial(place_kernel, dims),
        out_shape=(
            jax.ShapeDtypeStruct((ci, comps, cj, blocks * LANES), jnp.float32),
            jax.ShapeDtypeStruct(field.shape, jnp.float32),
        ),
        in_specs=[pl.BlockSpec(memory_space=pltpu.SMEM), vmem, vmem],
        out_specs=(vmem, vmem),
        input_output_aliases={2: 1},
        compiler_params=pltpu.CompilerParams(vmem_limit_bytes=16 * 1024 * 1024),
    )(code, reply, field)[0]


def local(residual, inverses, couplings, receptors, owners, donors, weights):
    ci, cj, comps = residual.shape[1:4]
    many = donors.shape[-1]
    count = donors.shape[-2]
    field, code, reply = run_sweeps(
        residual[0].transpose(0, 2, 1, 3),
        inverses[0].transpose(0, 2, 1, 3),
        couplings[0],
        owners.reshape(1, count),
        donors.reshape(count, many).T,
        weights.reshape(count, many).T,
        receptors.reshape(1, count),
    )
    slot_count = code.shape[1] // reply.shape[0]
    update = run_place(code, reply, field, (ci, cj, comps, slot_count))
    return update.transpose(0, 2, 1, 3)[None]


def solution(mesh):
    placed = (
        P("grid", "px", "py", None, None),
        P("grid", "px", "py", None, None),
        P("grid", "px", "py", None, None),
        P("grid", "px", "py", None),
        P("grid", "px", "py", None, None),
        P("grid", "px", "py", None, None),
        P("grid", "px", "py", None, None),
    )
    return jax.shard_map(
        local,
        mesh=mesh,
        in_specs=placed,
        out_specs=P("grid", "px", "py", None, None),
        check_vma=False,
    )
```

```python
import functools

import jax
import jax.numpy as jnp
from jax import lax
from jax.experimental import pallas as pl
from jax.experimental.pallas import tpu as pltpu
from jax.sharding import PartitionSpec as P

MESH = pl.DeviceIdType.MESH
LANES = 128
ROWS = 8
LOW = 8
EMPTY = LANES
FETCHES = 4


def divmod_const(value, by):
    if by & (by - 1) == 0:
        return value >> (by.bit_length() - 1), value & (by - 1)
    return value // by, value % by


def sweep_kernel(
    dims,
    res_hbm,
    inv_hbm,
    cpl_hbm,
    owners_hbm,
    donors_hbm,
    weights_hbm,
    receptors_hbm,
    field_v,
    code_out,
    reply_out,
    owners,
    donors,
    weights,
    receptors,
    inv_v,
    res_v,
    cpl_v,
    star_v,
    face_send,
    face_recv,
    ask_send,
    ask_recv,
    rows_v,
    rows_s,
    spread,
    reply_send,
    reply_recv,
    in_sem,
    small_sem,
    send_sem,
    recv_sem,
    ship_send_sem,
    ship_recv_sem,
    ask_send_sem,
    ask_recv_sem,
    reply_send_sem,
    reply_recv_sem,
    rows_sem,
    wave_sem,
):
    ci, cj, comps, blocks, count_rows, count_cols, slot_count = dims
    length = blocks * LANES
    entries = comps * comps
    steps = ci + cj - 1
    pitch = ci + cj - 1
    many, count = donors.shape
    owner_count = count_rows * count_cols
    slots = owner_count * slot_count
    grid = lax.axis_index("grid")
    px = lax.axis_index("px")
    py = lax.axis_index("py")
    me = px * count_cols + py
    ahead = px + py
    reach = count_rows + count_cols - 2

    first_core = grid == 0
    second_core = grid == 1

    def is_far(at):
        return at * 2 >= reach

    def is_beyond(at):
        return at >= 1

    far = is_far(ahead)
    beyond = is_beyond(ahead)
    own_forward = second_core | jnp.logical_not(far)
    own_backward = second_core | jnp.logical_not(beyond)
    taken_forward = second_core & far
    taken_backward = second_core & beyond

    def rows_of(chunk):
        return pl.ds(chunk * pitch + cj - 1, ci)

    def inputs_of(kb, chunk):
        lanes = pl.ds(pl.multiple_of(kb * LANES, LANES), LANES)
        rows = rows_of(chunk)
        return (
            (inv_hbm.at[:, :, :, lanes], inv_v.at[rows]),
            (cpl_hbm.at[:, :, :, lanes], cpl_v.at[rows, :, pl.ds(0, 4), :]),
            (res_hbm.at[:, :, :, lanes], res_v.at[rows]),
        )

    def input_copies(kb):
        return [
            pltpu.make_async_copy(source, target, in_sem.at[t, kb])
            for t, (source, target) in enumerate(inputs_of(kb, kb))
        ]

    def ship(kind, kb):
        if kind < 3:
            source, target = inputs_of(kb, blocks + kb)[kind]
        elif kind == 3:
            source, target = star_v.at[kb], star_v.at[blocks + kb]
        else:
            source, target = field_v.at[rows_of(blocks + kb)], field_v.at[rows_of(kb)]
        return pltpu.make_async_remote_copy(
            src_ref=source,
            dst_ref=target,
            send_sem=ship_send_sem.at[kind, kb],
            recv_sem=ship_recv_sem.at[kind, kb],
            device_id={"grid": 1 - grid},
            device_id_type=MESH,
        )

    small_copies = [
        pltpu.make_async_copy(source, target, small_sem.at[t])
        for t, (source, target) in enumerate(
            (
                (owners_hbm, owners),
                (donors_hbm, donors),
                (weights_hbm, weights),
                (receptors_hbm, receptors),
            )
        )
    ]
    eager = min(2, blocks)

    @pl.when(own_forward)
    def _():
        for kb in range(eager):
            for copy in input_copies(kb):
                copy.start()

    for copy in small_copies:
        copy.start()

    has_prev_row = px > 0
    has_next_row = px < count_rows - 1
    has_prev_col = py > 0
    has_next_col = py < count_cols - 1
    prev_row = {"px": px - 1}
    next_row = {"px": px + 1}
    prev_col = {"py": py - 1}
    next_col = {"py": py + 1}
    sides = (
        (has_prev_row, prev_row),
        (has_next_row, next_row),
        (has_prev_col, prev_col),
        (has_next_col, next_col),
    )

    def other(q):
        return {"grid": 1 - grid, "px": q // count_cols, "py": q % count_cols}

    barrier = pltpu.get_barrier_semaphore()
    for there, device in sides:

        @pl.when(there)
        def _():
            for core in range(2):
                pl.semaphore_signal(
                    barrier, inc=1, device_id=dict(device, grid=core), device_id_type=MESH
                )

    pl.semaphore_signal(
        barrier, inc=1, device_id={"grid": 1 - grid}, device_id_type=MESH
    )

    def enter():
        near = sum(there.astype(jnp.int32) for there, _ in sides)
        pl.semaphore_wait(barrier, 2 * near + 1)

    def wave(came_from, goes_to):
        for kind, there, _ in came_from:

            @pl.when(there)
            def _():
                pl.semaphore_wait(wave_sem.at[kind], 1)

        for kind, there, device in goes_to:

            @pl.when(there)
            def _():
                pl.semaphore_signal(
                    wave_sem.at[kind], inc=1, device_id=device, device_id_type=MESH
                )

    def wave_on():
        wave(
            ((0, has_prev_row, prev_row), (1, has_prev_col, prev_col)),
            ((0, has_next_row, next_row), (1, has_next_col, next_col)),
        )

    def wave_back():
        wave(
            ((2, has_next_row, next_row), (3, has_next_col, next_col)),
            ((2, has_prev_row, prev_row), (3, has_prev_col, prev_col)),
        )

    def ask(q):
        return pltpu.make_async_remote_copy(
            src_ref=ask_send.at[q],
            dst_ref=ask_recv.at[me],
            send_sem=ask_send_sem.at[q],
            recv_sem=ask_recv_sem.at[me],
            device_id=other(q),
            device_id_type=MESH,
        )

    def asked(q):
        return pltpu.make_async_remote_copy(
            src_ref=ask_send.at[q],
            dst_ref=ask_recv.at[q],
            send_sem=ask_send_sem.at[q],
            recv_sem=ask_recv_sem.at[q],
            device_id=other(q),
            device_id_type=MESH,
        )

    def reply(q):
        return pltpu.make_async_remote_copy(
            src_ref=reply_send.at[q],
            dst_ref=reply_recv.at[me],
            send_sem=reply_send_sem.at[q],
            recv_sem=reply_recv_sem.at[me],
            device_id=other(q),
            device_id_type=MESH,
        )

    def replied(q):
        return pltpu.make_async_remote_copy(
            src_ref=reply_send.at[q],
            dst_ref=reply_recv.at[q],
            send_sem=reply_send_sem.at[q],
            recv_sem=reply_recv_sem.at[q],
            device_id=other(q),
            device_id_type=MESH,
        )

    def digits(value):
        return [(value >> LOW).astype(jnp.float32), (value & (2**LOW - 1)).astype(jnp.float32)]

    def plan():
        for copy in small_copies:
            copy.wait()
        owner = owners[...]
        ones = jnp.where(
            owner == lax.broadcasted_iota(jnp.int32, (owner_count, count), 0), 1.0, 0.0
        )
        before = jnp.where(
            lax.broadcasted_iota(jnp.int32, (count, count), 0)
            < lax.broadcasted_iota(jnp.int32, (count, count), 1),
            1.0,
            0.0,
        ).astype(jnp.bfloat16)
        seen = jnp.dot(ones.astype(jnp.bfloat16), before, preferred_element_type=jnp.float32)
        rank = jnp.sum(seen * ones, axis=0, keepdims=True).astype(jnp.int32)
        place = owner * slot_count + rank
        weight = weights[...]
        high = weight.astype(jnp.bfloat16).astype(jnp.float32)
        mid = (weight - high).astype(jnp.bfloat16).astype(jnp.float32)
        low = weight - high - mid
        cell = receptors[...]
        marks = jnp.concatenate(
            digits(cell) + [jnp.ones((1, count), jnp.float32), jnp.zeros((ROWS - 3, count), jnp.float32)],
            axis=0,
        )
        table = jnp.concatenate(digits(donors[...]) + [high, mid, low, marks], axis=0).astype(
            jnp.bfloat16
        )
        wide = min(2 * LANES, slots)
        lane = lax.broadcasted_iota(jnp.int32, (many, LANES), 1)
        for base in range(0, slots, wide):
            slot = lax.broadcasted_iota(jnp.int32, (wide, count), 0) + base
            pick = jnp.where(slot == place, 1.0, 0.0).astype(jnp.bfloat16)
            got = lax.dot_general(
                table, pick, (((1,), (1,)), ((), ())), preferred_element_type=jnp.float32
            )
            cells = got[:many] * float(2**LOW) + got[many : 2 * many]
            share = got[2 * many : 3 * many] + got[3 * many : 4 * many] + got[4 * many : 5 * many]
            mark = got[5 * many : 5 * many + 3]
            target = (mark[0:1] * float(2**LOW) + mark[1:2]).astype(jnp.int32)
            pencil, k = divmod_const(target, length)
            kb, spot = divmod_const(k, LANES)
            line = kb * (pitch * cj) + (cj - 1) * cj + pencil
            code_out[:, base : base + wide] = jnp.where(
                mark[2:3] > 0.5, line * (2 * LANES) + spot, EMPTY
            )
            for q in range(base // slot_count, (base + wide) // slot_count):
                at = q * slot_count - base
                tile = at // LANES * LANES
                shift = at - tile
                left = cells[:, tile : tile + LANES]
                right = share[:, tile : tile + LANES]
                if shift:
                    left = pltpu.roll(left, LANES - shift, 1)
                if (slot_count - shift) % LANES:
                    right = pltpu.roll(right, (slot_count - shift) % LANES, 1)
                ask_send[q] = jnp.where(lane < slot_count, left, right)

    def send_asks():
        wave_back()

        @pl.loop(0, owner_count)
        def _(q):
            ask(q).start()

    def prepare():
        line = lax.broadcasted_iota(jnp.int32, (slot_count, LANES), 1)

        @pl.loop(0, owner_count)
        def _(q):
            asked(q).wait_recv()
            tile = ask_recv[q]
            cell = tile.astype(jnp.int32)
            pencil, k = divmod_const(cell, length)
            kb, _ = divmod_const(k, LANES)
            i, j = divmod_const(pencil, cj)
            row = kb * (pitch * cj) + (i + (cj - 1)) * cj + j
            rows_v[pl.ds(pl.multiple_of(q * ROWS, ROWS), ROWS), :] = jnp.clip(
                row, 0, field_v.shape[0] * cj - 1
            )
            turned = tile.T
            first = pl.multiple_of(q * slot_count, slot_count)
            for d in range(many):
                spot = turned[:slot_count, d : d + 1].astype(jnp.int32) & (LANES - 1)
                share = turned[slot_count : 2 * slot_count, d : d + 1]
                spread[d, pl.ds(first, slot_count), :] = jnp.where(line == spot, share, 0.0)

    def fetch_rows(q, slot):
        return pltpu.make_async_copy(
            rows_v.at[pl.ds(pl.multiple_of(q * ROWS, ROWS), ROWS)],
            rows_s.at[slot],
            rows_sem.at[slot],
        )

    def send(kind, chunk):
        device = (next_row, next_col, prev_row, prev_col)[kind]
        taken = chunk >= blocks
        moves = (first_core | taken) & (is_far(ahead + 1) if kind < 2 else is_beyond(ahead - 1))
        target = chunk - jnp.where(taken, blocks, 0) + jnp.where(moves, blocks, 0)
        return pltpu.make_async_remote_copy(
            src_ref=face_send.at[kind, chunk],
            dst_ref=face_recv.at[kind, target],
            send_sem=send_sem.at[kind, chunk],
            recv_sem=recv_sem.at[kind, target],
            device_id=dict(device, grid=jnp.where(moves, 1, jnp.where(taken, 0, grid))),
            device_id_type=MESH,
        )

    def arrival(kind, chunk):
        return pltpu.make_async_remote_copy(
            src_ref=face_send.at[kind, chunk],
            dst_ref=face_recv.at[kind, chunk],
            send_sem=send_sem.at[kind, chunk],
            recv_sem=recv_sem.at[kind, chunk],
            device_id={"grid": 1 - grid},
            device_id_type=MESH,
        )

    wave_first = ahead >= 1
    idle_first = ahead >= 2
    gets = (has_prev_row, has_prev_col, has_next_row, has_next_col)
    puts = (has_next_row, has_next_col, has_prev_row, has_prev_col)

    for kind in range(4):

        @pl.when(jnp.logical_not(gets[kind]))
        def _():
            face_recv[kind] = jnp.zeros(face_recv.shape[1:], jnp.float32)

    sub = lax.broadcasted_iota(jnp.int32, (cj, LANES), 0)

    def product(mat, vec):
        out = []
        for r in range(comps):
            terms = [mat(r * comps + c) * vec[c] for c in range(comps)]
            while len(terms) > 1:
                terms = [
                    terms[t] + terms[t + 1] if t + 1 < len(terms) else terms[t]
                    for t in range(0, len(terms), 2)
                ]
            out.append(terms[0])
        return out

    def wait_recv(kind, kb):
        @pl.when(gets[kind])
        def _():
            arrival(kind, kb).wait_recv()

    def start_send(kind, kb):
        @pl.when(puts[kind])
        def _():
            send(kind, kb).start()

    inv_flat = inv_v.reshape(inv_v.shape[0] * entries * cj, LANES)
    res_flat = res_v.reshape(res_v.shape[0] * comps * cj, LANES)
    cpl_flat = cpl_v.reshape(cpl_v.shape[0] * cj * ROWS, LANES)
    field_flat = field_v.reshape(field_v.shape[0] * cj * ROWS, LANES)
    field_rows = field_v.reshape(field_v.shape[0] * cj, ROWS, LANES)

    def entry(ref, kb, s, height, e):
        base = pl.multiple_of(kb * (pitch * height * cj), ROWS)
        start = base + (s * height * cj + e * cj + cj - 1)
        return ref[pl.ds(start, cj, stride=height * cj - 1), :]

    def cell_rows(kb, s, c):
        base = pl.multiple_of(kb * (pitch * cj * ROWS), ROWS)
        return pl.ds(base + ((s * cj + cj - 1) * ROWS + c), cj, stride=(cj - 1) * ROWS)

    def forward(kb):
        @pl.when(kb < blocks)
        def _():
            for copy in input_copies(kb):
                copy.wait()

        @pl.when(kb >= blocks)
        def _():
            for kind in range(3):
                ship(kind, kb - blocks).wait_recv()

        @pl.when(kb == 0)
        def _():
            for later in range(eager, blocks):
                for copy in input_copies(later):
                    copy.start()

        wait_recv(0, kb)
        wait_recv(1, kb)
        upper = [face_recv[0, kb, pl.ds(c * ROWS, cj), :] for c in range(comps)]
        prev = [jnp.zeros((cj, LANES), jnp.float32)] * comps
        lower = [jnp.zeros((cj, LANES), jnp.float32)] * comps
        for s in range(steps):
            coef_a = cpl_flat[cell_rows(kb, s, 0), :]
            coef_b = cpl_flat[cell_rows(kb, s, 1), :]
            up = prev
            if s < cj:
                up = [jnp.where(sub == cj - 1 - s, upper[c], prev[c]) for c in range(comps)]
            left = [pltpu.roll(p, cj - 1, 0) for p in prev]
            if s < ci:
                left = [
                    jnp.where(
                        sub == cj - 1,
                        jnp.broadcast_to(
                            face_recv[1, kb, pl.ds(c * ROWS + s, 1), :], (cj, LANES)
                        ),
                        left[c],
                    )
                    for c in range(comps)
                ]
            vec = [
                entry(res_flat, kb, s, comps, c) + coef_a * up[c] + coef_b * left[c]
                for c in range(comps)
            ]
            prev = product(lambda e: entry(inv_flat, kb, s, entries, e), vec)
            for c in range(comps):
                star_v[kb, s, c] = prev[c]
                if s >= cj - 1:
                    face_send[1, kb, pl.ds(c * ROWS + s - cj + 1, 1), :] = prev[c][0:1, :]
                if s >= ci - 1:
                    lower[c] = jnp.where(sub == cj + ci - 2 - s, prev[c], lower[c])
        for c in range(comps):
            face_send[0, kb, pl.ds(c * ROWS, cj), :] = lower[c]

        @pl.when((kb == 0) & jnp.logical_not(wave_first))
        def _():
            enter()

        start_send(0, kb)
        start_send(1, kb)

        @pl.when((kb == 0) & jnp.logical_not(wave_first))
        def _():
            wave_on()

        @pl.when(first_core & beyond)
        def _():
            ship(3, kb).start()

    def backward(kb):
        @pl.when((kb >= blocks) & jnp.logical_not(far))
        def _():
            for kind in (0, 1, 3):
                ship(kind, kb - blocks).wait_recv()

        wait_recv(2, kb)
        wait_recv(3, kb)
        under = [face_recv[2, kb, pl.ds(c * ROWS, cj), :] for c in range(comps)]
        prev = [jnp.zeros((cj, LANES), jnp.float32)] * comps
        upper = [jnp.zeros((cj, LANES), jnp.float32)] * comps
        for s in reversed(range(steps)):
            coef_e = cpl_flat[cell_rows(kb, s, 2), :]
            coef_f = cpl_flat[cell_rows(kb, s, 3), :]
            down = prev
            if s >= ci - 1:
                down = [
                    jnp.where(sub == cj + ci - 2 - s, under[c], prev[c]) for c in range(comps)
                ]
            right = [pltpu.roll(p, 1, 0) for p in prev]
            if s >= cj - 1:
                right = [
                    jnp.where(
                        sub == 0,
                        jnp.broadcast_to(
                            face_recv[3, kb, pl.ds(c * ROWS + s - cj + 1, 1), :], (cj, LANES)
                        ),
                        right[c],
                    )
                    for c in range(comps)
                ]
            vec = [coef_e * down[c] + coef_f * right[c] for c in range(comps)]
            prev = product(lambda e: entry(inv_flat, kb, s, entries, e), vec)
            prev = [star_v[kb, s, c] + prev[c] for c in range(comps)]
            for c in range(comps):
                field_flat[cell_rows(kb, s, c), :] = prev[c]
                if s < cj:
                    upper[c] = jnp.where(sub == cj - 1 - s, prev[c], upper[c])
                if s < ci:
                    face_send[3, kb, pl.ds(c * ROWS + s, 1), :] = prev[c][cj - 1 : cj, :]
        for c in range(comps):
            face_send[2, kb, pl.ds(c * ROWS, cj), :] = upper[c]
        start_send(2, kb)
        start_send(3, kb)

        @pl.when(kb >= blocks)
        def _():
            ship(4, kb - blocks).start()

    middle = 2 * blocks + 1
    last = 4 * blocks + 2
    begin = jnp.where(ahead == reach, 1, middle + 1)
    early = (ahead * 3 <= reach) | (first_core & beyond)
    asks_first = ahead * 3 >= reach * 2

    def ship_inputs():
        for kb in range(blocks):
            ship(0, kb).start()
            ship(1, kb).start()

            @pl.when(far)
            def _():
                ship(2, kb).start()

    @pl.loop(0, last + 1)
    def _(n):
        @pl.when((n == 0) & wave_first)
        def _():
            enter()

        @pl.when(first_core & beyond & (n == jnp.where(far, 0, middle)))
        def _():
            ship_inputs()

        @pl.when((n == 0) & wave_first)
        def _():
            wave_on()

        @pl.when(((n == 0) & idle_first) | ((n == middle) & jnp.logical_not(idle_first)))
        def _():
            plan()

        @pl.when(((n == 0) & asks_first) | ((n == middle) & jnp.logical_not(asks_first)))
        def _():
            send_asks()

        ahead_chunk = n - 1
        own = (ahead_chunk >= 0) & (ahead_chunk < blocks) & own_forward
        taken = (ahead_chunk >= blocks) & (ahead_chunk < 2 * blocks) & taken_forward

        @pl.when(own | taken)
        def _():
            forward(ahead_chunk)

        back_chunk = n - begin
        own = (back_chunk >= 0) & (back_chunk < blocks) & own_backward
        taken = (back_chunk >= blocks) & (back_chunk < 2 * blocks) & taken_backward

        @pl.when(own | taken)
        def _():
            backward(back_chunk)

        @pl.when(((n == middle) & early) | ((n == last) & jnp.logical_not(early)))
        def _():
            prepare()

    @pl.when(first_core & beyond)
    def _():
        for kb in range(blocks):
            ship(4, kb).wait_recv()

    lane8 = lax.broadcasted_iota(jnp.int32, (ROWS, LANES), 1)

    def gather(q, slot):
        acc = jnp.zeros((ROWS, LANES), jnp.float32)
        for s in range(slot_count):
            parts = [
                field_rows[rows_s[slot, d, s]] * spread[d, pl.ds(q * slot_count + s, 1), :]
                for d in range(many)
            ]
            while len(parts) > 1:
                parts = [parts[i] + parts[i + 1] for i in range(0, len(parts), 2)]
            total = jnp.sum(parts[0], axis=1, keepdims=True)
            acc = jnp.where(lane8 == s, total, acc)
        reply_send[q] = acc
        reply(q).start()

    for slot in range(FETCHES - 1):
        fetch_rows(slot, slot).start()

    @pl.loop(0, owner_count // FETCHES)
    def _(turn):
        for slot in range(FETCHES):
            q = turn * FETCHES + slot
            following = q + FETCHES - 1

            @pl.when(following < owner_count)
            def _():
                fetch_rows(following, (slot + FETCHES - 1) % FETCHES).start()

            fetch_rows(q, slot).wait()
            gather(q, slot)

    @pl.loop(0, owner_count)
    def _(q):
        replied(q).wait_recv()
        reply_out[q] = reply_recv[q]

    @pl.loop(0, owner_count)
    def _(q):
        ask(q).wait_send()
        reply(q).wait_send()

    for chunk in range(2 * blocks):
        own = chunk < blocks
        for kind in range(4):
            if kind < 2:
                done = own_forward if own else taken_forward
            else:
                done = own_backward if own else taken_backward

            @pl.when(puts[kind] & done)
            def _():
                send(kind, chunk).wait_send()

    for kb in range(blocks):
        for kind in range(5):
            sent = (
                first_core & beyond,
                first_core & beyond,
                first_core & far,
                first_core & beyond & jnp.logical_not(far),
                taken_backward,
            )[kind]

            @pl.when(sent)
            def _():
                ship(kind, kb).wait_send()


def run_sweeps(residual, inverses, couplings, owners, donors, weights, receptors):
    inputs = (residual, inverses, couplings, owners, donors, weights, receptors)
    ci, comps, cj, length = residual.shape
    many, count = donors.shape
    blocks = length // LANES
    steps = ci + cj - 1
    tall = 2 * blocks * (ci + cj - 1) + cj - 1
    rows, cols = lax.axis_size("px"), lax.axis_size("py")
    owner_count = rows * cols
    slot_count = max(2, 2 * count // owner_count)
    slots = owner_count * slot_count
    assert owner_count % FETCHES == 0 and cj == ROWS and ci <= ROWS and many == ROWS and 2 * slot_count <= LANES
    assert ci * cj * length <= 2 ** (2 * LOW)
    dims = (ci, cj, comps, blocks, rows, cols, slot_count)
    face = comps * ROWS
    dma = pltpu.SemaphoreType.DMA
    hbm = pl.BlockSpec(memory_space=pltpu.HBM)
    vmem = pl.BlockSpec(memory_space=pltpu.VMEM)
    return pl.pallas_call(
        functools.partial(sweep_kernel, dims),
        out_shape=(
            pltpu.VMEM((tall, cj, ROWS, LANES), jnp.float32),
            pltpu.VMEM((1, slots), jnp.int32),
            pltpu.VMEM((owner_count, ROWS, LANES), jnp.float32),
        ),
        in_specs=[hbm] * 7,
        out_specs=(vmem, vmem, vmem),
        scratch_shapes=[
            pltpu.VMEM(owners.shape, owners.dtype),
            pltpu.VMEM(donors.shape, donors.dtype),
            pltpu.VMEM(weights.shape, weights.dtype),
            pltpu.VMEM(receptors.shape, receptors.dtype),
            pltpu.VMEM((tall, comps * comps, cj, LANES), jnp.float32),
            pltpu.VMEM((tall, comps, cj, LANES), jnp.float32),
            pltpu.VMEM((tall, cj, ROWS, LANES), jnp.float32),
            pltpu.VMEM((2 * blocks, steps, comps, cj, LANES), jnp.float32),
            pltpu.VMEM((4, 2 * blocks, face, LANES), jnp.float32),
            pltpu.VMEM((4, 2 * blocks, face, LANES), jnp.float32),
            pltpu.VMEM((owner_count, ROWS, LANES), jnp.float32),
            pltpu.VMEM((owner_count, ROWS, LANES), jnp.float32),
            pltpu.VMEM((owner_count * ROWS, LANES), jnp.int32),
            pltpu.SMEM((FETCHES, ROWS, LANES), jnp.int32),
            pltpu.VMEM((many, slots, LANES), jnp.float32),
            pltpu.VMEM((owner_count, ROWS, LANES), jnp.float32),
            pltpu.VMEM((owner_count, ROWS, LANES), jnp.float32),
            dma((3, blocks)),
            dma((4,)),
            dma((4, 2 * blocks)),
            dma((4, 2 * blocks)),
            dma((5, blocks)),
            dma((5, blocks)),
            dma((owner_count,)),
            dma((owner_count,)),
            dma((owner_count,)),
            dma((owner_count,)),
            dma((FETCHES,)),
            pltpu.SemaphoreType.REGULAR((4,)),
        ],
        compiler_params=pltpu.CompilerParams(
            collective_id=0, has_side_effects=True, vmem_limit_bytes=53 * 1024 * 1024
        ),
    )(*(pltpu.with_memory_space_constraint(x, pltpu.HBM) for x in inputs))


def place_kernel(dims, code, reply, field, out, work):
    ci, cj, comps, slot_count = dims
    owner_count = reply.shape[0]
    blocks = out.shape[3] // LANES
    pitch = ci + cj - 1
    lane = lax.broadcasted_iota(jnp.int32, (ROWS, LANES), 1)
    lines = work.reshape(work.shape[0] * cj, ROWS, LANES)

    @pl.loop(0, owner_count)
    def _(q):
        tile = reply[q]
        for s in range(slot_count):
            line, spot = divmod_const(code[0, q * slot_count + s], 2 * LANES)
            value = jnp.broadcast_to(tile[:, s : s + 1], (ROWS, LANES))
            pltpu.store(lines.at[line], value, mask=lane == spot)

    stack = work.reshape(work.shape[0], cj * ROWS, LANES)

    @pl.loop(0, ci)
    def _(i):
        for kb in range(blocks):
            for c in range(comps):
                out[i, c, :, kb * LANES : (kb + 1) * LANES] = stack[
                    kb * pitch + cj - 1 + i, pl.ds(c, cj, stride=ROWS), :
                ]


def run_place(code, reply, field, length, dims):
    ci, cj, comps, slot_count = dims
    vmem = pl.BlockSpec(memory_space=pltpu.VMEM)
    return pl.pallas_call(
        functools.partial(place_kernel, dims),
        out_shape=(
            jax.ShapeDtypeStruct((ci, comps, cj, length), jnp.float32),
            jax.ShapeDtypeStruct(field.shape, jnp.float32),
        ),
        in_specs=[pl.BlockSpec(memory_space=pltpu.SMEM), vmem, vmem],
        out_specs=(vmem, vmem),
        input_output_aliases={2: 1},
        compiler_params=pltpu.CompilerParams(vmem_limit_bytes=16 * 1024 * 1024),
    )(code, reply, field)[0]


def local(residual, inverses, couplings, receptors, owners, donors, weights):
    ci, cj, comps = residual.shape[1:4]
    many = donors.shape[-1]
    count = donors.shape[-2]
    field, code, reply = run_sweeps(
        residual[0].transpose(0, 2, 1, 3),
        inverses[0].transpose(0, 2, 1, 3),
        couplings[0],
        owners.reshape(1, count),
        donors.reshape(count, many).T,
        weights.reshape(count, many).T,
        receptors.reshape(1, count),
    )
    slot_count = code.shape[1] // reply.shape[0]
    update = run_place(code, reply, field, residual.shape[4], (ci, cj, comps, slot_count))
    return update.transpose(0, 2, 1, 3)[None]


def solution(mesh):
    placed = (
        P("grid", "px", "py", None, None),
        P("grid", "px", "py", None, None),
        P("grid", "px", "py", None, None),
        P("grid", "px", "py", None),
        P("grid", "px", "py", None, None),
        P("grid", "px", "py", None, None),
        P("grid", "px", "py", None, None),
    )
    return jax.shard_map(
        local,
        mesh=mesh,
        in_specs=placed,
        out_specs=P("grid", "px", "py", None, None),
        check_vma=False,
    )
```

```python
import functools

import jax
import jax.numpy as jnp
from jax import lax
from jax.experimental import pallas as pl
from jax.experimental.pallas import tpu as pltpu
from jax.sharding import PartitionSpec as P

MESH = pl.DeviceIdType.MESH
LANES = 128
ROWS = 8
LOW = 8
EMPTY = LANES
FETCHES = 4


def divmod_const(value, by):
    if by & (by - 1) == 0:
        return value >> (by.bit_length() - 1), value & (by - 1)
    return value // by, value % by


def sweep_kernel(
    dims,
    res_hbm,
    inv_hbm,
    cpl_hbm,
    owners_hbm,
    donors_hbm,
    weights_hbm,
    receptors_hbm,
    field_v,
    code_out,
    reply_out,
    owners,
    donors,
    weights,
    receptors,
    inv_v,
    res_v,
    cpl_v,
    star_v,
    face_send,
    face_recv,
    ask_send,
    ask_recv,
    rows_v,
    rows_s,
    spread,
    reply_send,
    reply_recv,
    in_sem,
    small_sem,
    send_sem,
    recv_sem,
    ship_send_sem,
    ship_recv_sem,
    ask_send_sem,
    ask_recv_sem,
    reply_send_sem,
    reply_recv_sem,
    rows_sem,
    wave_sem,
):
    ci, cj, comps, blocks, count_rows, count_cols, slot_count = dims
    length = blocks * LANES
    entries = comps * comps
    steps = ci + cj - 1
    pitch = ci + cj - 1
    many, count = donors.shape
    owner_count = count_rows * count_cols
    slots = owner_count * slot_count
    grid = lax.axis_index("grid")
    px = lax.axis_index("px")
    py = lax.axis_index("py")
    me = px * count_cols + py
    ahead = px + py
    reach = count_rows + count_cols - 2

    first_core = grid == 0
    second_core = grid == 1

    def is_far(at):
        return at * 3 >= reach * 2

    def is_beyond(at):
        return at >= 1

    far = is_far(ahead)
    beyond = is_beyond(ahead)
    own_forward = second_core | jnp.logical_not(far)
    own_backward = second_core | jnp.logical_not(beyond)
    taken_forward = second_core & far
    taken_backward = second_core & beyond

    def rows_of(chunk):
        return pl.ds(chunk * pitch + cj - 1, ci)

    def inputs_of(kb, chunk):
        lanes = pl.ds(pl.multiple_of(kb * LANES, LANES), LANES)
        rows = rows_of(chunk)
        return (
            (inv_hbm.at[:, :, :, lanes], inv_v.at[rows]),
            (cpl_hbm.at[:, :, :, lanes], cpl_v.at[rows, :, pl.ds(0, 4), :]),
            (res_hbm.at[:, :, :, lanes], res_v.at[rows]),
        )

    def input_copies(kb):
        return [
            pltpu.make_async_copy(source, target, in_sem.at[t, kb])
            for t, (source, target) in enumerate(inputs_of(kb, kb))
        ]

    def ship(kind, kb):
        if kind < 3:
            source, target = inputs_of(kb, blocks + kb)[kind]
        elif kind == 3:
            source, target = star_v.at[kb], star_v.at[blocks + kb]
        else:
            source, target = field_v.at[rows_of(blocks + kb)], field_v.at[rows_of(kb)]
        return pltpu.make_async_remote_copy(
            src_ref=source,
            dst_ref=target,
            send_sem=ship_send_sem.at[kind, kb],
            recv_sem=ship_recv_sem.at[kind, kb],
            device_id={"grid": 1 - grid},
            device_id_type=MESH,
        )

    small_copies = [
        pltpu.make_async_copy(source, target, small_sem.at[t])
        for t, (source, target) in enumerate(
            (
                (owners_hbm, owners),
                (donors_hbm, donors),
                (weights_hbm, weights),
                (receptors_hbm, receptors),
            )
        )
    ]
    eager = min(2, blocks)

    @pl.when(own_forward)
    def _():
        for kb in range(eager):
            for copy in input_copies(kb):
                copy.start()

    for copy in small_copies:
        copy.start()

    has_prev_row = px > 0
    has_next_row = px < count_rows - 1
    has_prev_col = py > 0
    has_next_col = py < count_cols - 1
    prev_row = {"px": px - 1}
    next_row = {"px": px + 1}
    prev_col = {"py": py - 1}
    next_col = {"py": py + 1}
    sides = (
        (has_prev_row, prev_row),
        (has_next_row, next_row),
        (has_prev_col, prev_col),
        (has_next_col, next_col),
    )

    def other(q):
        return {"grid": 1 - grid, "px": q // count_cols, "py": q % count_cols}

    barrier = pltpu.get_barrier_semaphore()
    for there, device in sides:

        @pl.when(there)
        def _():
            for core in range(2):
                pl.semaphore_signal(
                    barrier, inc=1, device_id=dict(device, grid=core), device_id_type=MESH
                )

    pl.semaphore_signal(
        barrier, inc=1, device_id={"grid": 1 - grid}, device_id_type=MESH
    )

    def enter():
        near = sum(there.astype(jnp.int32) for there, _ in sides)
        pl.semaphore_wait(barrier, 2 * near + 1)

    def wave(came_from, goes_to):
        for kind, there, _ in came_from:

            @pl.when(there)
            def _():
                pl.semaphore_wait(wave_sem.at[kind], 1)

        for kind, there, device in goes_to:

            @pl.when(there)
            def _():
                pl.semaphore_signal(
                    wave_sem.at[kind], inc=1, device_id=device, device_id_type=MESH
                )

    def wave_on():
        wave(
            ((0, has_prev_row, prev_row), (1, has_prev_col, prev_col)),
            ((0, has_next_row, next_row), (1, has_next_col, next_col)),
        )

    def wave_back():
        wave(
            ((2, has_next_row, next_row), (3, has_next_col, next_col)),
            ((2, has_prev_row, prev_row), (3, has_prev_col, prev_col)),
        )

    def ask(q):
        return pltpu.make_async_remote_copy(
            src_ref=ask_send.at[q],
            dst_ref=ask_recv.at[me],
            send_sem=ask_send_sem.at[q],
            recv_sem=ask_recv_sem.at[me],
            device_id=other(q),
            device_id_type=MESH,
        )

    def asked(q):
        return pltpu.make_async_remote_copy(
            src_ref=ask_send.at[q],
            dst_ref=ask_recv.at[q],
            send_sem=ask_send_sem.at[q],
            recv_sem=ask_recv_sem.at[q],
            device_id=other(q),
            device_id_type=MESH,
        )

    def reply(q):
        return pltpu.make_async_remote_copy(
            src_ref=reply_send.at[q],
            dst_ref=reply_recv.at[me],
            send_sem=reply_send_sem.at[q],
            recv_sem=reply_recv_sem.at[me],
            device_id=other(q),
            device_id_type=MESH,
        )

    def replied(q):
        return pltpu.make_async_remote_copy(
            src_ref=reply_send.at[q],
            dst_ref=reply_recv.at[q],
            send_sem=reply_send_sem.at[q],
            recv_sem=reply_recv_sem.at[q],
            device_id=other(q),
            device_id_type=MESH,
        )

    def digits(value):
        return [(value >> LOW).astype(jnp.float32), (value & (2**LOW - 1)).astype(jnp.float32)]

    def plan():
        for copy in small_copies:
            copy.wait()
        owner = owners[...]
        ones = jnp.where(
            owner == lax.broadcasted_iota(jnp.int32, (owner_count, count), 0), 1.0, 0.0
        )
        before = jnp.where(
            lax.broadcasted_iota(jnp.int32, (count, count), 0)
            < lax.broadcasted_iota(jnp.int32, (count, count), 1),
            1.0,
            0.0,
        ).astype(jnp.bfloat16)
        seen = jnp.dot(ones.astype(jnp.bfloat16), before, preferred_element_type=jnp.float32)
        rank = jnp.sum(seen * ones, axis=0, keepdims=True).astype(jnp.int32)
        place = owner * slot_count + rank
        weight = weights[...]
        high = weight.astype(jnp.bfloat16).astype(jnp.float32)
        mid = (weight - high).astype(jnp.bfloat16).astype(jnp.float32)
        low = weight - high - mid
        cell = receptors[...]
        marks = jnp.concatenate(
            digits(cell) + [jnp.ones((1, count), jnp.float32), jnp.zeros((ROWS - 3, count), jnp.float32)],
            axis=0,
        )
        table = jnp.concatenate(digits(donors[...]) + [high, mid, low, marks], axis=0).astype(
            jnp.bfloat16
        )
        wide = min(2 * LANES, slots)
        lane = lax.broadcasted_iota(jnp.int32, (many, LANES), 1)
        for base in range(0, slots, wide):
            slot = lax.broadcasted_iota(jnp.int32, (wide, count), 0) + base
            pick = jnp.where(slot == place, 1.0, 0.0).astype(jnp.bfloat16)
            got = lax.dot_general(
                table, pick, (((1,), (1,)), ((), ())), preferred_element_type=jnp.float32
            )
            cells = got[:many] * float(2**LOW) + got[many : 2 * many]
            share = got[2 * many : 3 * many] + got[3 * many : 4 * many] + got[4 * many : 5 * many]
            mark = got[5 * many : 5 * many + 3]
            target = (mark[0:1] * float(2**LOW) + mark[1:2]).astype(jnp.int32)
            pencil, k = divmod_const(target, length)
            kb, spot = divmod_const(k, LANES)
            line = kb * (pitch * cj) + (cj - 1) * cj + pencil
            code_out[:, base : base + wide] = jnp.where(
                mark[2:3] > 0.5, line * (2 * LANES) + spot, EMPTY
            )
            for q in range(base // slot_count, (base + wide) // slot_count):
                at = q * slot_count - base
                tile = at // LANES * LANES
                shift = at - tile
                left = cells[:, tile : tile + LANES]
                right = share[:, tile : tile + LANES]
                if shift:
                    left = pltpu.roll(left, LANES - shift, 1)
                if (slot_count - shift) % LANES:
                    right = pltpu.roll(right, (slot_count - shift) % LANES, 1)
                ask_send[q] = jnp.where(lane < slot_count, left, right)

    def send_asks():
        wave_back()

        @pl.loop(0, owner_count)
        def _(q):
            ask(q).start()

    def prepare():
        line = lax.broadcasted_iota(jnp.int32, (slot_count, LANES), 1)

        @pl.loop(0, owner_count)
        def _(q):
            asked(q).wait_recv()
            tile = ask_recv[q]
            cell = tile.astype(jnp.int32)
            pencil, k = divmod_const(cell, length)
            kb, _ = divmod_const(k, LANES)
            i, j = divmod_const(pencil, cj)
            row = kb * (pitch * cj) + (i + (cj - 1)) * cj + j
            rows_v[pl.ds(pl.multiple_of(q * ROWS, ROWS), ROWS), :] = jnp.clip(
                row, 0, field_v.shape[0] * cj - 1
            ) * ROWS
            turned = tile.T
            first = pl.multiple_of(q * slot_count, slot_count)
            for d in range(many):
                spot = turned[:slot_count, d : d + 1].astype(jnp.int32) & (LANES - 1)
                share = turned[slot_count : 2 * slot_count, d : d + 1]
                spread[d, pl.ds(first, slot_count), :] = jnp.where(line == spot, share, 0.0)

    def fetch_rows(q, slot):
        return pltpu.make_async_copy(
            rows_v.at[pl.ds(pl.multiple_of(q * ROWS, ROWS), ROWS)],
            rows_s.at[slot],
            rows_sem.at[slot],
        )

    def send(kind, chunk):
        device = (next_row, next_col, prev_row, prev_col)[kind]
        taken = chunk >= blocks
        moves = (first_core | taken) & (is_far(ahead + 1) if kind < 2 else is_beyond(ahead - 1))
        target = chunk - jnp.where(taken, blocks, 0) + jnp.where(moves, blocks, 0)
        return pltpu.make_async_remote_copy(
            src_ref=face_send.at[kind, chunk],
            dst_ref=face_recv.at[kind, target],
            send_sem=send_sem.at[kind, chunk],
            recv_sem=recv_sem.at[kind, target],
            device_id=dict(device, grid=jnp.where(moves, 1, jnp.where(taken, 0, grid))),
            device_id_type=MESH,
        )

    def arrival(kind, chunk):
        return pltpu.make_async_remote_copy(
            src_ref=face_send.at[kind, chunk],
            dst_ref=face_recv.at[kind, chunk],
            send_sem=send_sem.at[kind, chunk],
            recv_sem=recv_sem.at[kind, chunk],
            device_id={"grid": 1 - grid},
            device_id_type=MESH,
        )

    wave_first = ahead >= 1
    idle_first = ahead >= 2
    gets = (has_prev_row, has_prev_col, has_next_row, has_next_col)
    puts = (has_next_row, has_next_col, has_prev_row, has_prev_col)

    for kind in range(4):

        @pl.when(jnp.logical_not(gets[kind]))
        def _():
            face_recv[kind] = jnp.zeros(face_recv.shape[1:], jnp.float32)

    sub = lax.broadcasted_iota(jnp.int32, (cj, LANES), 0)

    def product(mat, vec):
        out = []
        for r in range(comps):
            terms = [mat(r * comps + c) * vec[c] for c in range(comps)]
            while len(terms) > 1:
                terms = [
                    terms[t] + terms[t + 1] if t + 1 < len(terms) else terms[t]
                    for t in range(0, len(terms), 2)
                ]
            out.append(terms[0])
        return out

    def wait_recv(kind, kb):
        @pl.when(gets[kind])
        def _():
            arrival(kind, kb).wait_recv()

    def start_send(kind, kb):
        @pl.when(puts[kind])
        def _():
            send(kind, kb).start()

    inv_flat = inv_v.reshape(inv_v.shape[0] * entries * cj, LANES)
    res_flat = res_v.reshape(res_v.shape[0] * comps * cj, LANES)
    cpl_flat = cpl_v.reshape(cpl_v.shape[0] * cj * ROWS, LANES)
    field_flat = field_v.reshape(field_v.shape[0] * cj * ROWS, LANES)

    def entry(ref, kb, s, height, e):
        base = pl.multiple_of(kb * (pitch * height * cj), ROWS)
        start = base + (s * height * cj + e * cj + cj - 1)
        return ref[pl.ds(start, cj, stride=height * cj - 1), :]

    def cell_rows(kb, s, c):
        base = pl.multiple_of(kb * (pitch * cj * ROWS), ROWS)
        return pl.ds(base + ((s * cj + cj - 1) * ROWS + c), cj, stride=(cj - 1) * ROWS)

    def forward(kb):
        @pl.when(kb < blocks)
        def _():
            for copy in input_copies(kb):
                copy.wait()

        @pl.when(kb >= blocks)
        def _():
            for kind in range(3):
                ship(kind, kb - blocks).wait_recv()

        @pl.when(kb == 0)
        def _():
            for later in range(eager, blocks):
                for copy in input_copies(later):
                    copy.start()

        wait_recv(0, kb)
        wait_recv(1, kb)
        upper = [face_recv[0, kb, pl.ds(c * ROWS, cj), :] for c in range(comps)]
        prev = [jnp.zeros((cj, LANES), jnp.float32)] * comps
        lower = [jnp.zeros((cj, LANES), jnp.float32)] * comps
        for s in range(steps):
            coef_a = cpl_flat[cell_rows(kb, s, 0), :]
            coef_b = cpl_flat[cell_rows(kb, s, 1), :]
            up = prev
            if s < cj:
                up = [jnp.where(sub == cj - 1 - s, upper[c], prev[c]) for c in range(comps)]
            left = [pltpu.roll(p, cj - 1, 0) for p in prev]
            if s < ci:
                left = [
                    jnp.where(
                        sub == cj - 1,
                        jnp.broadcast_to(
                            face_recv[1, kb, pl.ds(c * ROWS + s, 1), :], (cj, LANES)
                        ),
                        left[c],
                    )
                    for c in range(comps)
                ]
            vec = [
                entry(res_flat, kb, s, comps, c) + coef_a * up[c] + coef_b * left[c]
                for c in range(comps)
            ]
            prev = product(lambda e: entry(inv_flat, kb, s, entries, e), vec)
            for c in range(comps):
                star_v[kb, s, c] = prev[c]
                if s >= cj - 1:
                    face_send[1, kb, pl.ds(c * ROWS + s - cj + 1, 1), :] = prev[c][0:1, :]
                if s >= ci - 1:
                    lower[c] = jnp.where(sub == cj + ci - 2 - s, prev[c], lower[c])
        for c in range(comps):
            face_send[0, kb, pl.ds(c * ROWS, cj), :] = lower[c]

        @pl.when((kb == 0) & jnp.logical_not(wave_first))
        def _():
            enter()

        start_send(0, kb)
        start_send(1, kb)

        @pl.when((kb == 0) & jnp.logical_not(wave_first))
        def _():
            wave_on()

        @pl.when(first_core & beyond)
        def _():
            ship(3, kb).start()

    def backward(kb):
        @pl.when((kb >= blocks) & jnp.logical_not(far))
        def _():
            for kind in (0, 1, 3):
                ship(kind, kb - blocks).wait_recv()

        wait_recv(2, kb)
        wait_recv(3, kb)
        under = [face_recv[2, kb, pl.ds(c * ROWS, cj), :] for c in range(comps)]
        prev = [jnp.zeros((cj, LANES), jnp.float32)] * comps
        upper = [jnp.zeros((cj, LANES), jnp.float32)] * comps
        for s in reversed(range(steps)):
            coef_e = cpl_flat[cell_rows(kb, s, 2), :]
            coef_f = cpl_flat[cell_rows(kb, s, 3), :]
            down = prev
            if s >= ci - 1:
                down = [
                    jnp.where(sub == cj + ci - 2 - s, under[c], prev[c]) for c in range(comps)
                ]
            right = [pltpu.roll(p, 1, 0) for p in prev]
            if s >= cj - 1:
                right = [
                    jnp.where(
                        sub == 0,
                        jnp.broadcast_to(
                            face_recv[3, kb, pl.ds(c * ROWS + s - cj + 1, 1), :], (cj, LANES)
                        ),
                        right[c],
                    )
                    for c in range(comps)
                ]
            vec = [coef_e * down[c] + coef_f * right[c] for c in range(comps)]
            prev = product(lambda e: entry(inv_flat, kb, s, entries, e), vec)
            prev = [star_v[kb, s, c] + prev[c] for c in range(comps)]
            for c in range(comps):
                field_flat[cell_rows(kb, s, c), :] = prev[c]
                if s < cj:
                    upper[c] = jnp.where(sub == cj - 1 - s, prev[c], upper[c])
                if s < ci:
                    face_send[3, kb, pl.ds(c * ROWS + s, 1), :] = prev[c][cj - 1 : cj, :]
        for c in range(comps):
            face_send[2, kb, pl.ds(c * ROWS, cj), :] = upper[c]
        start_send(2, kb)
        start_send(3, kb)

        @pl.when(kb >= blocks)
        def _():
            ship(4, kb - blocks).start()

    middle = 2 * blocks + 1
    last = 4 * blocks + 2
    begin = jnp.where(ahead == reach, 1, middle + 1)
    early = (ahead * 3 <= reach) | (first_core & beyond)
    asks_first = far | (second_core & (ahead * 2 >= reach))

    def ship_inputs():
        for kb in range(blocks):
            ship(0, kb).start()
            ship(1, kb).start()

            @pl.when(far)
            def _():
                ship(2, kb).start()

    @pl.loop(0, last + 1)
    def _(n):
        @pl.when((n == 0) & wave_first)
        def _():
            enter()

        @pl.when(first_core & beyond & (n == 0))
        def _():
            ship_inputs()

        @pl.when((n == 0) & wave_first)
        def _():
            wave_on()

        @pl.when(((n == 0) & idle_first) | ((n == middle) & jnp.logical_not(idle_first)))
        def _():
            plan()

        @pl.when(((n == 0) & asks_first) | ((n == middle) & jnp.logical_not(asks_first)))
        def _():
            send_asks()

        ahead_chunk = n - 1
        own = (ahead_chunk >= 0) & (ahead_chunk < blocks) & own_forward
        taken = (ahead_chunk >= blocks) & (ahead_chunk < 2 * blocks) & taken_forward

        @pl.when(own | taken)
        def _():
            forward(ahead_chunk)

        back_chunk = n - begin
        own = (back_chunk >= 0) & (back_chunk < blocks) & own_backward
        taken = (back_chunk >= blocks) & (back_chunk < 2 * blocks) & taken_backward

        @pl.when(own | taken)
        def _():
            backward(back_chunk)

        @pl.when(((n == middle) & early) | ((n == last) & jnp.logical_not(early)))
        def _():
            prepare()

    @pl.when(first_core & beyond)
    def _():
        for kb in range(blocks):
            ship(4, kb).wait_recv()

    lane8 = lax.broadcasted_iota(jnp.int32, (ROWS, LANES), 1)

    def gather(q, slot):
        acc = jnp.zeros((ROWS, LANES), jnp.float32)
        for s in range(slot_count):
            parts = [
                field_flat[pl.ds(rows_s[slot, d, s], ROWS), :] * spread[d, pl.ds(q * slot_count + s, 1), :]
                for d in range(many)
            ]
            while len(parts) > 1:
                parts = [parts[i] + parts[i + 1] for i in range(0, len(parts), 2)]
            total = jnp.sum(parts[0], axis=1, keepdims=True)
            acc = jnp.where(lane8 == s, total, acc)
        reply_send[q] = acc
        reply(q).start()

    for slot in range(FETCHES - 1):
        fetch_rows(slot, slot).start()

    @pl.loop(0, owner_count // FETCHES)
    def _(turn):
        for slot in range(FETCHES):
            q = turn * FETCHES + slot
            following = q + FETCHES - 1

            @pl.when(following < owner_count)
            def _():
                fetch_rows(following, (slot + FETCHES - 1) % FETCHES).start()

            fetch_rows(q, slot).wait()
            gather(q, slot)

    @pl.loop(0, owner_count)
    def _(q):
        replied(q).wait_recv()
        reply_out[q] = reply_recv[q]

    @pl.loop(0, owner_count)
    def _(q):
        ask(q).wait_send()
        reply(q).wait_send()

    for chunk in range(2 * blocks):
        own = chunk < blocks
        for kind in range(4):
            if kind < 2:
                done = own_forward if own else taken_forward
            else:
                done = own_backward if own else taken_backward

            @pl.when(puts[kind] & done)
            def _():
                send(kind, chunk).wait_send()

    for kb in range(blocks):
        for kind in range(5):
            sent = (
                first_core & beyond,
                first_core & beyond,
                first_core & far,
                first_core & beyond & jnp.logical_not(far),
                taken_backward,
            )[kind]

            @pl.when(sent)
            def _():
                ship(kind, kb).wait_send()


def run_sweeps(residual, inverses, couplings, owners, donors, weights, receptors):
    inputs = (residual, inverses, couplings, owners, donors, weights, receptors)
    ci, comps, cj, length = residual.shape
    many, count = donors.shape
    blocks = length // LANES
    steps = ci + cj - 1
    tall = 2 * blocks * (ci + cj - 1) + cj - 1
    rows, cols = lax.axis_size("px"), lax.axis_size("py")
    owner_count = rows * cols
    slot_count = max(2, 2 * count // owner_count)
    slots = owner_count * slot_count
    assert owner_count % FETCHES == 0 and cj == ROWS and ci <= ROWS and many == ROWS and 2 * slot_count <= LANES
    assert ci * cj * length <= 2 ** (2 * LOW)
    dims = (ci, cj, comps, blocks, rows, cols, slot_count)
    face = comps * ROWS
    dma = pltpu.SemaphoreType.DMA
    hbm = pl.BlockSpec(memory_space=pltpu.HBM)
    vmem = pl.BlockSpec(memory_space=pltpu.VMEM)
    return pl.pallas_call(
        functools.partial(sweep_kernel, dims),
        out_shape=(
            pltpu.VMEM((tall, cj, ROWS, LANES), jnp.float32),
            pltpu.VMEM((1, slots), jnp.int32),
            pltpu.VMEM((owner_count, ROWS, LANES), jnp.float32),
        ),
        in_specs=[hbm] * 7,
        out_specs=(vmem, vmem, vmem),
        scratch_shapes=[
            pltpu.VMEM(owners.shape, owners.dtype),
            pltpu.VMEM(donors.shape, donors.dtype),
            pltpu.VMEM(weights.shape, weights.dtype),
            pltpu.VMEM(receptors.shape, receptors.dtype),
            pltpu.VMEM((tall, comps * comps, cj, LANES), jnp.float32),
            pltpu.VMEM((tall, comps, cj, LANES), jnp.float32),
            pltpu.VMEM((tall, cj, ROWS, LANES), jnp.float32),
            pltpu.VMEM((2 * blocks, steps, comps, cj, LANES), jnp.float32),
            pltpu.VMEM((4, 2 * blocks, face, LANES), jnp.float32),
            pltpu.VMEM((4, 2 * blocks, face, LANES), jnp.float32),
            pltpu.VMEM((owner_count, ROWS, LANES), jnp.float32),
            pltpu.VMEM((owner_count, ROWS, LANES), jnp.float32),
            pltpu.VMEM((owner_count * ROWS, LANES), jnp.int32),
            pltpu.SMEM((FETCHES, ROWS, LANES), jnp.int32),
            pltpu.VMEM((many, slots, LANES), jnp.float32),
            pltpu.VMEM((owner_count, ROWS, LANES), jnp.float32),
            pltpu.VMEM((owner_count, ROWS, LANES), jnp.float32),
            dma((3, blocks)),
            dma((4,)),
            dma((4, 2 * blocks)),
            dma((4, 2 * blocks)),
            dma((5, blocks)),
            dma((5, blocks)),
            dma((owner_count,)),
            dma((owner_count,)),
            dma((owner_count,)),
            dma((owner_count,)),
            dma((FETCHES,)),
            pltpu.SemaphoreType.REGULAR((4,)),
        ],
        compiler_params=pltpu.CompilerParams(
            collective_id=0, has_side_effects=True, vmem_limit_bytes=53 * 1024 * 1024
        ),
    )(*(pltpu.with_memory_space_constraint(x, pltpu.HBM) for x in inputs))


def place_kernel(dims, code, reply, field, out, work):
    ci, cj, comps, slot_count = dims
    owner_count = reply.shape[0]
    blocks = out.shape[3] // LANES
    pitch = ci + cj - 1
    lane = lax.broadcasted_iota(jnp.int32, (ROWS, LANES), 1)
    lines = work.reshape(work.shape[0] * cj, ROWS, LANES)

    @pl.loop(0, owner_count)
    def _(q):
        tile = reply[q]
        for s in range(slot_count):
            line, spot = divmod_const(code[0, q * slot_count + s], 2 * LANES)
            value = jnp.broadcast_to(tile[:, s : s + 1], (ROWS, LANES))
            pltpu.store(lines.at[line], value, mask=lane == spot)

    stack = work.reshape(work.shape[0], cj * ROWS, LANES)

    @pl.loop(0, ci)
    def _(i):
        for kb in range(blocks):
            for c in range(comps):
                out[i, c, :, kb * LANES : (kb + 1) * LANES] = stack[
                    kb * pitch + cj - 1 + i, pl.ds(c, cj, stride=ROWS), :
                ]


def run_place(code, reply, field, length, dims):
    ci, cj, comps, slot_count = dims
    vmem = pl.BlockSpec(memory_space=pltpu.VMEM)
    return pl.pallas_call(
        functools.partial(place_kernel, dims),
        out_shape=(
            jax.ShapeDtypeStruct((ci, comps, cj, length), jnp.float32),
            jax.ShapeDtypeStruct(field.shape, jnp.float32),
        ),
        in_specs=[pl.BlockSpec(memory_space=pltpu.SMEM), vmem, vmem],
        out_specs=(vmem, vmem),
        input_output_aliases={2: 1},
        compiler_params=pltpu.CompilerParams(vmem_limit_bytes=16 * 1024 * 1024),
    )(code, reply, field)[0]


def local(residual, inverses, couplings, receptors, owners, donors, weights):
    ci, cj, comps = residual.shape[1:4]
    many = donors.shape[-1]
    count = donors.shape[-2]
    field, code, reply = run_sweeps(
        residual[0].transpose(0, 2, 1, 3),
        inverses[0].transpose(0, 2, 1, 3),
        couplings[0],
        owners.reshape(1, count),
        donors.reshape(count, many).T,
        weights.reshape(count, many).T,
        receptors.reshape(1, count),
    )
    slot_count = code.shape[1] // reply.shape[0]
    update = run_place(code, reply, field, residual.shape[4], (ci, cj, comps, slot_count))
    return update.transpose(0, 2, 1, 3)[None]


def solution(mesh):
    placed = (
        P("grid", "px", "py", None, None),
        P("grid", "px", "py", None, None),
        P("grid", "px", "py", None, None),
        P("grid", "px", "py", None),
        P("grid", "px", "py", None, None),
        P("grid", "px", "py", None, None),
        P("grid", "px", "py", None, None),
    )
    return jax.shard_map(
        local,
        mesh=mesh,
        in_specs=placed,
        out_specs=P("grid", "px", "py", None, None),
        check_vma=False,
    )
```

```python
import functools

import jax
import jax.numpy as jnp
from jax import lax
from jax.experimental import pallas as pl
from jax.experimental.pallas import tpu as pltpu
from jax.sharding import PartitionSpec as P

MESH = pl.DeviceIdType.MESH
LANES = 128
ROWS = 8
LOW = 8
EMPTY = LANES
FETCHES = 4


def divmod_const(value, by):
    if by & (by - 1) == 0:
        return value >> (by.bit_length() - 1), value & (by - 1)
    return value // by, value % by


def sweep_kernel(
    dims,
    res_hbm,
    inv_hbm,
    cpl_hbm,
    owners_hbm,
    donors_hbm,
    weights_hbm,
    receptors_hbm,
    field_v,
    code_out,
    reply_out,
    owners,
    donors,
    weights,
    receptors,
    inv_v,
    res_v,
    cpl_v,
    star_v,
    face_send,
    face_recv,
    ask_send,
    ask_recv,
    rows_v,
    rows_s,
    spread,
    reply_send,
    reply_recv,
    in_sem,
    small_sem,
    send_sem,
    recv_sem,
    ship_send_sem,
    ship_recv_sem,
    ask_send_sem,
    ask_recv_sem,
    reply_send_sem,
    reply_recv_sem,
    rows_sem,
    wave_sem,
):
    ci, cj, comps, blocks, count_rows, count_cols, slot_count = dims
    length = blocks * LANES
    entries = comps * comps
    steps = ci + cj - 1
    pitch = ci + cj - 1
    many, count = donors.shape
    owner_count = count_rows * count_cols
    slots = owner_count * slot_count
    grid = lax.axis_index("grid")
    px = lax.axis_index("px")
    py = lax.axis_index("py")
    me = px * count_cols + py
    ahead = px + py
    reach = count_rows + count_cols - 2

    first_core = grid == 0
    second_core = grid == 1

    def is_far(at):
        return at * 3 >= reach * 2

    def is_beyond(at):
        return at >= 1

    far = is_far(ahead)
    beyond = is_beyond(ahead)
    own_forward = second_core | jnp.logical_not(far)
    own_backward = second_core | jnp.logical_not(beyond)
    taken_forward = second_core & far
    taken_backward = second_core & beyond

    def rows_of(chunk):
        return pl.ds(chunk * pitch + cj - 1, ci)

    def inputs_of(kb, chunk):
        lanes = pl.ds(pl.multiple_of(kb * LANES, LANES), LANES)
        rows = rows_of(chunk)
        return (
            (inv_hbm.at[:, :, :, lanes], inv_v.at[rows]),
            (cpl_hbm.at[:, :, :, lanes], cpl_v.at[rows, :, pl.ds(0, 4), :]),
            (res_hbm.at[:, :, :, lanes], res_v.at[rows]),
        )

    def input_copies(kb):
        return [
            pltpu.make_async_copy(source, target, in_sem.at[t, kb])
            for t, (source, target) in enumerate(inputs_of(kb, kb))
        ]

    def ship(kind, kb):
        if kind < 3:
            source, target = inputs_of(kb, blocks + kb)[kind]
        elif kind == 3:
            source, target = star_v.at[kb], star_v.at[blocks + kb]
        else:
            source, target = field_v.at[rows_of(blocks + kb)], field_v.at[rows_of(kb)]
        return pltpu.make_async_remote_copy(
            src_ref=source,
            dst_ref=target,
            send_sem=ship_send_sem.at[kind, kb],
            recv_sem=ship_recv_sem.at[kind, kb],
            device_id={"grid": 1 - grid},
            device_id_type=MESH,
        )

    small_copies = [
        pltpu.make_async_copy(source, target, small_sem.at[t])
        for t, (source, target) in enumerate(
            (
                (owners_hbm, owners),
                (donors_hbm, donors),
                (weights_hbm, weights),
                (receptors_hbm, receptors),
            )
        )
    ]
    eager = min(2, blocks)

    @pl.when(own_forward)
    def _():
        for kb in range(eager):
            for copy in input_copies(kb):
                copy.start()

    for copy in small_copies:
        copy.start()

    has_prev_row = px > 0
    has_next_row = px < count_rows - 1
    has_prev_col = py > 0
    has_next_col = py < count_cols - 1
    prev_row = {"px": px - 1}
    next_row = {"px": px + 1}
    prev_col = {"py": py - 1}
    next_col = {"py": py + 1}
    sides = (
        (has_prev_row, prev_row),
        (has_next_row, next_row),
        (has_prev_col, prev_col),
        (has_next_col, next_col),
    )

    def other(q):
        return {"grid": 1 - grid, "px": q // count_cols, "py": q % count_cols}

    barrier = pltpu.get_barrier_semaphore()
    for there, device in sides:

        @pl.when(there)
        def _():
            for core in range(2):
                pl.semaphore_signal(
                    barrier, inc=1, device_id=dict(device, grid=core), device_id_type=MESH
                )

    pl.semaphore_signal(
        barrier, inc=1, device_id={"grid": 1 - grid}, device_id_type=MESH
    )

    def enter():
        near = sum(there.astype(jnp.int32) for there, _ in sides)
        pl.semaphore_wait(barrier, 2 * near + 1)

    def wave(came_from, goes_to):
        for kind, there, _ in came_from:

            @pl.when(there)
            def _():
                pl.semaphore_wait(wave_sem.at[kind], 1)

        for kind, there, device in goes_to:

            @pl.when(there)
            def _():
                pl.semaphore_signal(
                    wave_sem.at[kind], inc=1, device_id=device, device_id_type=MESH
                )

    def wave_on():
        wave(
            ((0, has_prev_row, prev_row), (1, has_prev_col, prev_col)),
            ((0, has_next_row, next_row), (1, has_next_col, next_col)),
        )

    def wave_back():
        wave(
            ((2, has_next_row, next_row), (3, has_next_col, next_col)),
            ((2, has_prev_row, prev_row), (3, has_prev_col, prev_col)),
        )

    def ask(q):
        return pltpu.make_async_remote_copy(
            src_ref=ask_send.at[q],
            dst_ref=ask_recv.at[me],
            send_sem=ask_send_sem.at[q],
            recv_sem=ask_recv_sem.at[me],
            device_id=other(q),
            device_id_type=MESH,
        )

    def asked(q):
        return pltpu.make_async_remote_copy(
            src_ref=ask_send.at[q],
            dst_ref=ask_recv.at[q],
            send_sem=ask_send_sem.at[q],
            recv_sem=ask_recv_sem.at[q],
            device_id=other(q),
            device_id_type=MESH,
        )

    def reply(q):
        return pltpu.make_async_remote_copy(
            src_ref=reply_send.at[q],
            dst_ref=reply_recv.at[me],
            send_sem=reply_send_sem.at[q],
            recv_sem=reply_recv_sem.at[me],
            device_id=other(q),
            device_id_type=MESH,
        )

    def replied(q):
        return pltpu.make_async_remote_copy(
            src_ref=reply_send.at[q],
            dst_ref=reply_recv.at[q],
            send_sem=reply_send_sem.at[q],
            recv_sem=reply_recv_sem.at[q],
            device_id=other(q),
            device_id_type=MESH,
        )

    def digits(value):
        return [(value >> LOW).astype(jnp.float32), (value & (2**LOW - 1)).astype(jnp.float32)]

    def plan():
        for copy in small_copies:
            copy.wait()
        owner = owners[...]
        ones = jnp.where(
            owner == lax.broadcasted_iota(jnp.int32, (owner_count, count), 0), 1.0, 0.0
        )
        before = jnp.where(
            lax.broadcasted_iota(jnp.int32, (count, count), 0)
            < lax.broadcasted_iota(jnp.int32, (count, count), 1),
            1.0,
            0.0,
        ).astype(jnp.bfloat16)
        seen = jnp.dot(ones.astype(jnp.bfloat16), before, preferred_element_type=jnp.float32)
        rank = jnp.sum(seen * ones, axis=0, keepdims=True).astype(jnp.int32)
        place = owner * slot_count + rank
        weight = weights[...]
        high = weight.astype(jnp.bfloat16).astype(jnp.float32)
        mid = (weight - high).astype(jnp.bfloat16).astype(jnp.float32)
        low = weight - high - mid
        cell = receptors[...]
        marks = jnp.concatenate(
            digits(cell) + [jnp.ones((1, count), jnp.float32), jnp.zeros((ROWS - 3, count), jnp.float32)],
            axis=0,
        )
        table = jnp.concatenate(digits(donors[...]) + [high, mid, low, marks], axis=0).astype(
            jnp.bfloat16
        )
        wide = min(2 * LANES, slots)
        lane = lax.broadcasted_iota(jnp.int32, (many, LANES), 1)
        for base in range(0, slots, wide):
            slot = lax.broadcasted_iota(jnp.int32, (wide, count), 0) + base
            pick = jnp.where(slot == place, 1.0, 0.0).astype(jnp.bfloat16)
            got = lax.dot_general(
                table, pick, (((1,), (1,)), ((), ())), preferred_element_type=jnp.float32
            )
            cells = got[:many] * float(2**LOW) + got[many : 2 * many]
            share = got[2 * many : 3 * many] + got[3 * many : 4 * many] + got[4 * many : 5 * many]
            mark = got[5 * many : 5 * many + 3]
            target = (mark[0:1] * float(2**LOW) + mark[1:2]).astype(jnp.int32)
            pencil, k = divmod_const(target, length)
            kb, spot = divmod_const(k, LANES)
            line = kb * (pitch * cj) + (cj - 1) * cj + pencil
            code_out[:, base : base + wide] = jnp.where(
                mark[2:3] > 0.5, line * (2 * LANES) + spot, EMPTY
            )
            for q in range(base // slot_count, (base + wide) // slot_count):
                at = q * slot_count - base
                tile = at // LANES * LANES
                shift = at - tile
                left = cells[:, tile : tile + LANES]
                right = share[:, tile : tile + LANES]
                if shift:
                    left = pltpu.roll(left, LANES - shift, 1)
                if (slot_count - shift) % LANES:
                    right = pltpu.roll(right, (slot_count - shift) % LANES, 1)
                ask_send[q] = jnp.where(lane < slot_count, left, right)

    def send_asks():
        wave_back()

        @pl.loop(0, owner_count)
        def _(q):
            ask(q).start()

    def prepare():
        line = lax.broadcasted_iota(jnp.int32, (slot_count, LANES), 1)

        @pl.loop(0, owner_count)
        def _(q):
            asked(q).wait_recv()
            tile = ask_recv[q]
            cell = tile.astype(jnp.int32)
            pencil, k = divmod_const(cell, length)
            kb, _ = divmod_const(k, LANES)
            i, j = divmod_const(pencil, cj)
            row = kb * (pitch * cj) + (i + (cj - 1)) * cj + j
            rows_v[pl.ds(pl.multiple_of(q * ROWS, ROWS), ROWS), :] = jnp.clip(
                row, 0, field_v.shape[0] * cj - 1
            ) * ROWS
            turned = tile.T
            first = pl.multiple_of(q * slot_count, slot_count)
            for d in range(many):
                spot = turned[:slot_count, d : d + 1].astype(jnp.int32) & (LANES - 1)
                share = turned[slot_count : 2 * slot_count, d : d + 1]
                spread[d, pl.ds(first, slot_count), :] = jnp.where(line == spot, share, 0.0)

        for slot in range(FETCHES - 1):
            fetch_rows(turn_of(slot), slot).start()

    def turn_of(t):
        return (me + (owner_count - 1) - t) % owner_count

    def fetch_rows(q, slot):
        return pltpu.make_async_copy(
            rows_v.at[pl.ds(pl.multiple_of(q * ROWS, ROWS), ROWS)],
            rows_s.at[slot],
            rows_sem.at[slot],
        )

    def send(kind, chunk):
        device = (next_row, next_col, prev_row, prev_col)[kind]
        taken = chunk >= blocks
        moves = (first_core | taken) & (is_far(ahead + 1) if kind < 2 else is_beyond(ahead - 1))
        target = chunk - jnp.where(taken, blocks, 0) + jnp.where(moves, blocks, 0)
        return pltpu.make_async_remote_copy(
            src_ref=face_send.at[kind, chunk],
            dst_ref=face_recv.at[kind, target],
            send_sem=send_sem.at[kind, chunk],
            recv_sem=recv_sem.at[kind, target],
            device_id=dict(device, grid=jnp.where(moves, 1, jnp.where(taken, 0, grid))),
            device_id_type=MESH,
        )

    def arrival(kind, chunk):
        return pltpu.make_async_remote_copy(
            src_ref=face_send.at[kind, chunk],
            dst_ref=face_recv.at[kind, chunk],
            send_sem=send_sem.at[kind, chunk],
            recv_sem=recv_sem.at[kind, chunk],
            device_id={"grid": 1 - grid},
            device_id_type=MESH,
        )

    wave_first = ahead >= 1
    idle_first = ahead >= 2
    gets = (has_prev_row, has_prev_col, has_next_row, has_next_col)
    puts = (has_next_row, has_next_col, has_prev_row, has_prev_col)

    for kind in range(4):

        @pl.when(jnp.logical_not(gets[kind]))
        def _():
            face_recv[kind] = jnp.zeros(face_recv.shape[1:], jnp.float32)

    sub = lax.broadcasted_iota(jnp.int32, (cj, LANES), 0)

    def product(mat, vec):
        out = []
        for r in range(comps):
            terms = [mat(r * comps + c) * vec[c] for c in range(comps)]
            while len(terms) > 1:
                terms = [
                    terms[t] + terms[t + 1] if t + 1 < len(terms) else terms[t]
                    for t in range(0, len(terms), 2)
                ]
            out.append(terms[0])
        return out

    def wait_recv(kind, kb):
        @pl.when(gets[kind])
        def _():
            arrival(kind, kb).wait_recv()

    def start_send(kind, kb):
        @pl.when(puts[kind])
        def _():
            send(kind, kb).start()

    inv_flat = inv_v.reshape(inv_v.shape[0] * entries * cj, LANES)
    res_flat = res_v.reshape(res_v.shape[0] * comps * cj, LANES)
    cpl_flat = cpl_v.reshape(cpl_v.shape[0] * cj * ROWS, LANES)
    field_flat = field_v.reshape(field_v.shape[0] * cj * ROWS, LANES)

    def entry(ref, kb, s, height, e):
        base = pl.multiple_of(kb * (pitch * height * cj), ROWS)
        start = base + (s * height * cj + e * cj + cj - 1)
        return ref[pl.ds(start, cj, stride=height * cj - 1), :]

    def cell_rows(kb, s, c):
        base = pl.multiple_of(kb * (pitch * cj * ROWS), ROWS)
        return pl.ds(base + ((s * cj + cj - 1) * ROWS + c), cj, stride=(cj - 1) * ROWS)

    def forward(kb):
        @pl.when(kb < blocks)
        def _():
            for copy in input_copies(kb):
                copy.wait()

        @pl.when(kb >= blocks)
        def _():
            for kind in range(3):
                ship(kind, kb - blocks).wait_recv()

        @pl.when(kb == 0)
        def _():
            for later in range(eager, blocks):
                for copy in input_copies(later):
                    copy.start()

        wait_recv(0, kb)
        wait_recv(1, kb)
        upper = [face_recv[0, kb, pl.ds(c * ROWS, cj), :] for c in range(comps)]
        prev = [jnp.zeros((cj, LANES), jnp.float32)] * comps
        lower = [jnp.zeros((cj, LANES), jnp.float32)] * comps
        for s in range(steps):
            coef_a = cpl_flat[cell_rows(kb, s, 0), :]
            coef_b = cpl_flat[cell_rows(kb, s, 1), :]
            up = prev
            if s < cj:
                up = [jnp.where(sub == cj - 1 - s, upper[c], prev[c]) for c in range(comps)]
            left = [pltpu.roll(p, cj - 1, 0) for p in prev]
            if s < ci:
                left = [
                    jnp.where(
                        sub == cj - 1,
                        jnp.broadcast_to(
                            face_recv[1, kb, pl.ds(c * ROWS + s, 1), :], (cj, LANES)
                        ),
                        left[c],
                    )
                    for c in range(comps)
                ]
            vec = [
                entry(res_flat, kb, s, comps, c) + coef_a * up[c] + coef_b * left[c]
                for c in range(comps)
            ]
            prev = product(lambda e: entry(inv_flat, kb, s, entries, e), vec)
            for c in range(comps):
                star_v[kb, s, c] = prev[c]
                if s >= cj - 1:
                    face_send[1, kb, pl.ds(c * ROWS + s - cj + 1, 1), :] = prev[c][0:1, :]
                if s >= ci - 1:
                    lower[c] = jnp.where(sub == cj + ci - 2 - s, prev[c], lower[c])
        for c in range(comps):
            face_send[0, kb, pl.ds(c * ROWS, cj), :] = lower[c]

        @pl.when((kb == 0) & jnp.logical_not(wave_first))
        def _():
            enter()

        start_send(0, kb)
        start_send(1, kb)

        @pl.when((kb == 0) & jnp.logical_not(wave_first))
        def _():
            wave_on()

        @pl.when(first_core & beyond)
        def _():
            ship(3, kb).start()

    def backward(kb):
        @pl.when((kb >= blocks) & jnp.logical_not(far))
        def _():
            for kind in (0, 1, 3):
                ship(kind, kb - blocks).wait_recv()

        wait_recv(2, kb)
        wait_recv(3, kb)
        under = [face_recv[2, kb, pl.ds(c * ROWS, cj), :] for c in range(comps)]
        prev = [jnp.zeros((cj, LANES), jnp.float32)] * comps
        upper = [jnp.zeros((cj, LANES), jnp.float32)] * comps
        for s in reversed(range(steps)):
            coef_e = cpl_flat[cell_rows(kb, s, 2), :]
            coef_f = cpl_flat[cell_rows(kb, s, 3), :]
            down = prev
            if s >= ci - 1:
                down = [
                    jnp.where(sub == cj + ci - 2 - s, under[c], prev[c]) for c in range(comps)
                ]
            right = [pltpu.roll(p, 1, 0) for p in prev]
            if s >= cj - 1:
                right = [
                    jnp.where(
                        sub == 0,
                        jnp.broadcast_to(
                            face_recv[3, kb, pl.ds(c * ROWS + s - cj + 1, 1), :], (cj, LANES)
                        ),
                        right[c],
                    )
                    for c in range(comps)
                ]
            vec = [coef_e * down[c] + coef_f * right[c] for c in range(comps)]
            prev = product(lambda e: entry(inv_flat, kb, s, entries, e), vec)
            prev = [star_v[kb, s, c] + prev[c] for c in range(comps)]
            for c in range(comps):
                field_flat[cell_rows(kb, s, c), :] = prev[c]
                if s < cj:
                    upper[c] = jnp.where(sub == cj - 1 - s, prev[c], upper[c])
                if s < ci:
                    face_send[3, kb, pl.ds(c * ROWS + s, 1), :] = prev[c][cj - 1 : cj, :]
        for c in range(comps):
            face_send[2, kb, pl.ds(c * ROWS, cj), :] = upper[c]
        start_send(2, kb)
        start_send(3, kb)

        @pl.when(kb >= blocks)
        def _():
            ship(4, kb - blocks).start()

    middle = 2 * blocks + 1
    last = 4 * blocks + 2
    begin = jnp.where(ahead == reach, 1, middle + 1)
    early = (ahead * 3 <= reach) | (first_core & beyond)
    asks_first = far | (second_core & (ahead * 2 >= reach))

    def ship_inputs():
        for kb in range(blocks):
            ship(0, kb).start()
            ship(1, kb).start()

            @pl.when(far)
            def _():
                ship(2, kb).start()

    @pl.loop(0, last + 1)
    def _(n):
        @pl.when((n == 0) & wave_first)
        def _():
            enter()

        @pl.when(first_core & beyond & (n == 0))
        def _():
            ship_inputs()

        @pl.when((n == 0) & wave_first)
        def _():
            wave_on()

        @pl.when(((n == 0) & idle_first) | ((n == middle) & jnp.logical_not(idle_first)))
        def _():
            plan()

        @pl.when(((n == 0) & asks_first) | ((n == middle) & jnp.logical_not(asks_first)))
        def _():
            send_asks()

        ahead_chunk = n - 1
        own = (ahead_chunk >= 0) & (ahead_chunk < blocks) & own_forward
        taken = (ahead_chunk >= blocks) & (ahead_chunk < 2 * blocks) & taken_forward

        @pl.when(own | taken)
        def _():
            forward(ahead_chunk)

        back_chunk = n - begin
        own = (back_chunk >= 0) & (back_chunk < blocks) & own_backward
        taken = (back_chunk >= blocks) & (back_chunk < 2 * blocks) & taken_backward

        @pl.when(own | taken)
        def _():
            backward(back_chunk)

        @pl.when(((n == middle) & early) | ((n == last) & jnp.logical_not(early)))
        def _():
            prepare()

    @pl.when(first_core & beyond)
    def _():
        for kb in range(blocks):
            ship(4, kb).wait_recv()

    lane8 = lax.broadcasted_iota(jnp.int32, (ROWS, LANES), 1)

    def gather(q, slot):
        acc = jnp.zeros((ROWS, LANES), jnp.float32)
        for s in range(slot_count):
            parts = [
                field_flat[pl.ds(rows_s[slot, d, s], ROWS), :] * spread[d, pl.ds(q * slot_count + s, 1), :]
                for d in range(many)
            ]
            while len(parts) > 1:
                parts = [parts[i] + parts[i + 1] for i in range(0, len(parts), 2)]
            total = jnp.sum(parts[0], axis=1, keepdims=True)
            acc = jnp.where(lane8 == s, total, acc)
        reply_send[q] = acc
        reply(q).start()

    @pl.loop(0, owner_count // FETCHES)
    def _(turn):
        for slot in range(FETCHES):
            t = turn * FETCHES + slot
            following = t + FETCHES - 1

            @pl.when(following < owner_count)
            def _():
                fetch_rows(turn_of(following), (slot + FETCHES - 1) % FETCHES).start()

            fetch_rows(turn_of(t), slot).wait()
            gather(turn_of(t), slot)

    @pl.loop(0, owner_count)
    def _(q):
        ask(q).wait_send()
        reply(q).wait_send()

    for chunk in range(2 * blocks):
        own = chunk < blocks
        for kind in range(4):
            if kind < 2:
                done = own_forward if own else taken_forward
            else:
                done = own_backward if own else taken_backward

            @pl.when(puts[kind] & done)
            def _():
                send(kind, chunk).wait_send()

    for kb in range(blocks):
        for kind in range(5):
            sent = (
                first_core & beyond,
                first_core & beyond,
                first_core & far,
                first_core & beyond & jnp.logical_not(far),
                taken_backward,
            )[kind]

            @pl.when(sent)
            def _():
                ship(kind, kb).wait_send()

    @pl.loop(0, owner_count)
    def _(q):
        replied(q).wait_recv()
        reply_out[q] = reply_recv[q]


def run_sweeps(residual, inverses, couplings, owners, donors, weights, receptors):
    inputs = (residual, inverses, couplings, owners, donors, weights, receptors)
    ci, comps, cj, length = residual.shape
    many, count = donors.shape
    blocks = length // LANES
    steps = ci + cj - 1
    tall = 2 * blocks * (ci + cj - 1) + cj - 1
    rows, cols = lax.axis_size("px"), lax.axis_size("py")
    owner_count = rows * cols
    slot_count = max(2, 2 * count // owner_count)
    slots = owner_count * slot_count
    assert owner_count % FETCHES == 0 and cj == ROWS and ci <= ROWS and many == ROWS and 2 * slot_count <= LANES
    assert ci * cj * length <= 2 ** (2 * LOW)
    dims = (ci, cj, comps, blocks, rows, cols, slot_count)
    face = comps * ROWS
    dma = pltpu.SemaphoreType.DMA
    hbm = pl.BlockSpec(memory_space=pltpu.HBM)
    vmem = pl.BlockSpec(memory_space=pltpu.VMEM)
    return pl.pallas_call(
        functools.partial(sweep_kernel, dims),
        out_shape=(
            pltpu.VMEM((tall, cj, ROWS, LANES), jnp.float32),
            pltpu.VMEM((1, slots), jnp.int32),
            pltpu.VMEM((owner_count, ROWS, LANES), jnp.float32),
        ),
        in_specs=[hbm] * 7,
        out_specs=(vmem, vmem, vmem),
        scratch_shapes=[
            pltpu.VMEM(owners.shape, owners.dtype),
            pltpu.VMEM(donors.shape, donors.dtype),
            pltpu.VMEM(weights.shape, weights.dtype),
            pltpu.VMEM(receptors.shape, receptors.dtype),
            pltpu.VMEM((tall, comps * comps, cj, LANES), jnp.float32),
            pltpu.VMEM((tall, comps, cj, LANES), jnp.float32),
            pltpu.VMEM((tall, cj, ROWS, LANES), jnp.float32),
            pltpu.VMEM((2 * blocks, steps, comps, cj, LANES), jnp.float32),
            pltpu.VMEM((4, 2 * blocks, face, LANES), jnp.float32),
            pltpu.VMEM((4, 2 * blocks, face, LANES), jnp.float32),
            pltpu.VMEM((owner_count, ROWS, LANES), jnp.float32),
            pltpu.VMEM((owner_count, ROWS, LANES), jnp.float32),
            pltpu.VMEM((owner_count * ROWS, LANES), jnp.int32),
            pltpu.SMEM((FETCHES, ROWS, LANES), jnp.int32),
            pltpu.VMEM((many, slots, LANES), jnp.float32),
            pltpu.VMEM((owner_count, ROWS, LANES), jnp.float32),
            pltpu.VMEM((owner_count, ROWS, LANES), jnp.float32),
            dma((3, blocks)),
            dma((4,)),
            dma((4, 2 * blocks)),
            dma((4, 2 * blocks)),
            dma((5, blocks)),
            dma((5, blocks)),
            dma((owner_count,)),
            dma((owner_count,)),
            dma((owner_count,)),
            dma((owner_count,)),
            dma((FETCHES,)),
            pltpu.SemaphoreType.REGULAR((4,)),
        ],
        compiler_params=pltpu.CompilerParams(
            collective_id=0, has_side_effects=True, vmem_limit_bytes=53 * 1024 * 1024
        ),
    )(*(pltpu.with_memory_space_constraint(x, pltpu.HBM) for x in inputs))


def place_kernel(dims, code, reply, field, out_hbm, work, out, out_sem):
    ci, cj, comps, slot_count = dims
    owner_count = reply.shape[0]
    blocks = out.shape[3] // LANES
    pitch = ci + cj - 1
    lane = lax.broadcasted_iota(jnp.int32, (ROWS, LANES), 1)
    lines = work.reshape(work.shape[0] * cj, ROWS, LANES)

    @pl.loop(0, owner_count)
    def _(q):
        tile = reply[q]
        for s in range(slot_count):
            line, spot = divmod_const(code[0, q * slot_count + s], 2 * LANES)
            value = jnp.broadcast_to(tile[:, s : s + 1], (ROWS, LANES))
            pltpu.store(lines.at[line], value, mask=lane == spot)

    stack = work.reshape(work.shape[0], cj * ROWS, LANES)

    def out_copy(i):
        return pltpu.make_async_copy(out.at[i], out_hbm.at[i], out_sem.at[i])

    @pl.loop(0, ci)
    def _(i):
        for kb in range(blocks):
            for c in range(comps):
                out[i, c, :, kb * LANES : (kb + 1) * LANES] = stack[
                    kb * pitch + cj - 1 + i, pl.ds(c, cj, stride=ROWS), :
                ]
        out_copy(i).start()

    @pl.loop(0, ci)
    def _(i):
        out_copy(i).wait()


def run_place(code, reply, field, length, dims):
    ci, cj, comps, slot_count = dims
    vmem = pl.BlockSpec(memory_space=pltpu.VMEM)
    return pl.pallas_call(
        functools.partial(place_kernel, dims),
        out_shape=(
            jax.ShapeDtypeStruct((ci, comps, cj, length), jnp.float32),
            jax.ShapeDtypeStruct(field.shape, jnp.float32),
        ),
        in_specs=[pl.BlockSpec(memory_space=pltpu.SMEM), vmem, vmem],
        out_specs=(pl.BlockSpec(memory_space=pltpu.HBM), vmem),
        scratch_shapes=[
            pltpu.VMEM((ci, comps, cj, length), jnp.float32),
            pltpu.SemaphoreType.DMA((ci,)),
        ],
        input_output_aliases={2: 1},
        compiler_params=pltpu.CompilerParams(vmem_limit_bytes=16 * 1024 * 1024),
    )(code, reply, field)[0]


def local(residual, inverses, couplings, receptors, owners, donors, weights):
    ci, cj, comps = residual.shape[1:4]
    many = donors.shape[-1]
    count = donors.shape[-2]
    field, code, reply = run_sweeps(
        residual[0].transpose(0, 2, 1, 3),
        inverses[0].transpose(0, 2, 1, 3),
        couplings[0],
        owners.reshape(1, count),
        donors.reshape(count, many).T,
        weights.reshape(count, many).T,
        receptors.reshape(1, count),
    )
    slot_count = code.shape[1] // reply.shape[0]
    update = run_place(code, reply, field, residual.shape[4], (ci, cj, comps, slot_count))
    return update.transpose(0, 2, 1, 3)[None]


def solution(mesh):
    placed = (
        P("grid", "px", "py", None, None),
        P("grid", "px", "py", None, None),
        P("grid", "px", "py", None, None),
        P("grid", "px", "py", None),
        P("grid", "px", "py", None, None),
        P("grid", "px", "py", None, None),
        P("grid", "px", "py", None, None),
    )
    return jax.shard_map(
        local,
        mesh=mesh,
        in_specs=placed,
        out_specs=P("grid", "px", "py", None, None),
        check_vma=False,
    )
```

```python
import functools

import jax
import jax.numpy as jnp
from jax import lax
from jax.experimental import pallas as pl
from jax.experimental.pallas import tpu as pltpu
from jax.sharding import PartitionSpec as P

MESH = pl.DeviceIdType.MESH
LANES = 128
ROWS = 8
LOW = 8
EMPTY = LANES
FETCHES = 4


def divmod_const(value, by):
    if by & (by - 1) == 0:
        return value >> (by.bit_length() - 1), value & (by - 1)
    return value // by, value % by


def sweep_kernel(
    dims,
    res_hbm,
    inv_hbm,
    cpl_hbm,
    owners_hbm,
    donors_hbm,
    weights_hbm,
    receptors_hbm,
    field_v,
    code_out,
    reply_out,
    owners,
    donors,
    weights,
    receptors,
    inv_v,
    res_v,
    cpl_v,
    star_v,
    face_send,
    face_recv,
    ask_send,
    ask_recv,
    rows_v,
    rows_s,
    spread,
    reply_send,
    reply_recv,
    in_sem,
    small_sem,
    send_sem,
    recv_sem,
    ship_send_sem,
    ship_recv_sem,
    ask_send_sem,
    ask_recv_sem,
    reply_send_sem,
    reply_recv_sem,
    rows_sem,
    wave_sem,
):
    ci, cj, comps, blocks, count_rows, count_cols, slot_count = dims
    length = blocks * LANES
    entries = comps * comps
    steps = ci + cj - 1
    pitch = ci + cj - 1
    many, count = donors.shape
    owner_count = count_rows * count_cols
    slots = owner_count * slot_count
    grid = lax.axis_index("grid")
    px = lax.axis_index("px")
    py = lax.axis_index("py")
    me = px * count_cols + py
    ahead = px + py
    reach = count_rows + count_cols - 2

    first_core = grid == 0
    second_core = grid == 1

    def is_far(at):
        return at * 3 >= reach * 2

    def is_beyond(at):
        return at >= 1

    far = is_far(ahead)
    beyond = is_beyond(ahead)
    own_forward = second_core | jnp.logical_not(far)
    own_backward = second_core | jnp.logical_not(beyond)
    taken_forward = second_core & far
    taken_backward = second_core & beyond

    def rows_of(chunk):
        return pl.ds(chunk * pitch + cj - 1, ci)

    def inputs_of(kb, chunk):
        lanes = pl.ds(pl.multiple_of(kb * LANES, LANES), LANES)
        rows = rows_of(chunk)
        return (
            (inv_hbm.at[:, :, :, lanes], inv_v.at[rows]),
            (cpl_hbm.at[:, :, :, lanes], cpl_v.at[rows, :, pl.ds(0, 4), :]),
            (res_hbm.at[:, :, :, lanes], res_v.at[rows]),
        )

    def input_copies(kb):
        return [
            pltpu.make_async_copy(source, target, in_sem.at[t, kb])
            for t, (source, target) in enumerate(inputs_of(kb, kb))
        ]

    def ship(kind, kb):
        if kind < 3:
            source, target = inputs_of(kb, blocks + kb)[kind]
        elif kind == 3:
            source, target = star_v.at[kb], star_v.at[blocks + kb]
        else:
            source, target = field_v.at[rows_of(blocks + kb)], field_v.at[rows_of(kb)]
        return pltpu.make_async_remote_copy(
            src_ref=source,
            dst_ref=target,
            send_sem=ship_send_sem.at[kind, kb],
            recv_sem=ship_recv_sem.at[kind, kb],
            device_id={"grid": 1 - grid},
            device_id_type=MESH,
        )

    small_copies = [
        pltpu.make_async_copy(source, target, small_sem.at[t])
        for t, (source, target) in enumerate(
            (
                (owners_hbm, owners),
                (donors_hbm, donors),
                (weights_hbm, weights),
                (receptors_hbm, receptors),
            )
        )
    ]
    eager = min(2, blocks)

    @pl.when(own_forward)
    def _():
        for kb in range(eager):
            for copy in input_copies(kb):
                copy.start()

    for copy in small_copies:
        copy.start()

    has_prev_row = px > 0
    has_next_row = px < count_rows - 1
    has_prev_col = py > 0
    has_next_col = py < count_cols - 1
    prev_row = {"px": px - 1}
    next_row = {"px": px + 1}
    prev_col = {"py": py - 1}
    next_col = {"py": py + 1}
    sides = (
        (has_prev_row, prev_row),
        (has_next_row, next_row),
        (has_prev_col, prev_col),
        (has_next_col, next_col),
    )

    def other(q):
        return {"grid": 1 - grid, "px": q // count_cols, "py": q % count_cols}

    barrier = pltpu.get_barrier_semaphore()
    for there, device in sides:

        @pl.when(there)
        def _():
            for core in range(2):
                pl.semaphore_signal(
                    barrier, inc=1, device_id=dict(device, grid=core), device_id_type=MESH
                )

    pl.semaphore_signal(
        barrier, inc=1, device_id={"grid": 1 - grid}, device_id_type=MESH
    )

    def enter():
        near = sum(there.astype(jnp.int32) for there, _ in sides)
        pl.semaphore_wait(barrier, 2 * near + 1)

    def wave(came_from, goes_to):
        for kind, there, _ in came_from:

            @pl.when(there)
            def _():
                pl.semaphore_wait(wave_sem.at[kind], 1)

        for kind, there, device in goes_to:

            @pl.when(there)
            def _():
                pl.semaphore_signal(
                    wave_sem.at[kind], inc=1, device_id=device, device_id_type=MESH
                )

    def wave_on():
        wave(
            ((0, has_prev_row, prev_row), (1, has_prev_col, prev_col)),
            ((0, has_next_row, next_row), (1, has_next_col, next_col)),
        )

    def wave_back():
        wave(
            ((2, has_next_row, next_row), (3, has_next_col, next_col)),
            ((2, has_prev_row, prev_row), (3, has_prev_col, prev_col)),
        )

    def ask(q):
        return pltpu.make_async_remote_copy(
            src_ref=ask_send.at[q],
            dst_ref=ask_recv.at[me],
            send_sem=ask_send_sem.at[q],
            recv_sem=ask_recv_sem.at[me],
            device_id=other(q),
            device_id_type=MESH,
        )

    def asked(q):
        return pltpu.make_async_remote_copy(
            src_ref=ask_send.at[q],
            dst_ref=ask_recv.at[q],
            send_sem=ask_send_sem.at[q],
            recv_sem=ask_recv_sem.at[q],
            device_id=other(q),
            device_id_type=MESH,
        )

    def reply(q):
        return pltpu.make_async_remote_copy(
            src_ref=reply_send.at[q],
            dst_ref=reply_recv.at[me],
            send_sem=reply_send_sem.at[q],
            recv_sem=reply_recv_sem.at[me],
            device_id=other(q),
            device_id_type=MESH,
        )

    def replied(q):
        return pltpu.make_async_remote_copy(
            src_ref=reply_send.at[q],
            dst_ref=reply_recv.at[q],
            send_sem=reply_send_sem.at[q],
            recv_sem=reply_recv_sem.at[q],
            device_id=other(q),
            device_id_type=MESH,
        )

    def digits(value):
        return [(value >> LOW).astype(jnp.float32), (value & (2**LOW - 1)).astype(jnp.float32)]

    def plan():
        for copy in small_copies:
            copy.wait()
        owner = owners[...]
        ones = jnp.where(
            owner == lax.broadcasted_iota(jnp.int32, (owner_count, count), 0), 1.0, 0.0
        )
        before = jnp.where(
            lax.broadcasted_iota(jnp.int32, (count, count), 0)
            < lax.broadcasted_iota(jnp.int32, (count, count), 1),
            1.0,
            0.0,
        ).astype(jnp.bfloat16)
        seen = jnp.dot(ones.astype(jnp.bfloat16), before, preferred_element_type=jnp.float32)
        rank = jnp.sum(seen * ones, axis=0, keepdims=True).astype(jnp.int32)
        place = owner * slot_count + rank
        weight = weights[...]
        high = weight.astype(jnp.bfloat16).astype(jnp.float32)
        mid = (weight - high).astype(jnp.bfloat16).astype(jnp.float32)
        low = weight - high - mid
        cell = receptors[...]
        marks = jnp.concatenate(
            digits(cell) + [jnp.ones((1, count), jnp.float32), jnp.zeros((ROWS - 3, count), jnp.float32)],
            axis=0,
        )
        table = jnp.concatenate(digits(donors[...]) + [high, mid, low, marks], axis=0).astype(
            jnp.bfloat16
        )
        wide = min(2 * LANES, slots)
        lane = lax.broadcasted_iota(jnp.int32, (many, LANES), 1)
        for base in range(0, slots, wide):
            slot = lax.broadcasted_iota(jnp.int32, (wide, count), 0) + base
            pick = jnp.where(slot == place, 1.0, 0.0).astype(jnp.bfloat16)
            got = lax.dot_general(
                table, pick, (((1,), (1,)), ((), ())), preferred_element_type=jnp.float32
            )
            cells = got[:many] * float(2**LOW) + got[many : 2 * many]
            share = got[2 * many : 3 * many] + got[3 * many : 4 * many] + got[4 * many : 5 * many]
            mark = got[5 * many : 5 * many + 3]
            target = (mark[0:1] * float(2**LOW) + mark[1:2]).astype(jnp.int32)
            pencil, k = divmod_const(target, length)
            kb, spot = divmod_const(k, LANES)
            line = kb * (pitch * cj) + (cj - 1) * cj + pencil
            code_out[:, base : base + wide] = jnp.where(
                mark[2:3] > 0.5, line * (ROWS * 2 * LANES) + spot, EMPTY
            )
            for q in range(base // slot_count, (base + wide) // slot_count):
                at = q * slot_count - base
                tile = at // LANES * LANES
                shift = at - tile
                left = cells[:, tile : tile + LANES]
                right = share[:, tile : tile + LANES]
                if shift:
                    left = pltpu.roll(left, LANES - shift, 1)
                if (slot_count - shift) % LANES:
                    right = pltpu.roll(right, (slot_count - shift) % LANES, 1)
                ask_send[q] = jnp.where(lane < slot_count, left, right)

    def send_asks():
        wave_back()

        @pl.loop(0, owner_count)
        def _(q):
            ask(q).start()

    def prepare():
        line = lax.broadcasted_iota(jnp.int32, (slot_count, LANES), 1)

        @pl.loop(0, owner_count)
        def _(q):
            asked(q).wait_recv()
            tile = ask_recv[q]
            cell = tile.astype(jnp.int32)
            pencil, k = divmod_const(cell, length)
            kb, _ = divmod_const(k, LANES)
            i, j = divmod_const(pencil, cj)
            row = kb * (pitch * cj) + (i + (cj - 1)) * cj + j
            rows_v[pl.ds(pl.multiple_of(q * ROWS, ROWS), ROWS), :] = jnp.clip(
                row, 0, field_v.shape[0] * cj - 1
            ) * ROWS
            turned = tile.T
            first = pl.multiple_of(q * slot_count, slot_count)
            for d in range(many):
                spot = turned[:slot_count, d : d + 1].astype(jnp.int32) & (LANES - 1)
                share = turned[slot_count : 2 * slot_count, d : d + 1]
                spread[d, pl.ds(first, slot_count), :] = jnp.where(line == spot, share, 0.0)

        for slot in range(FETCHES - 1):
            fetch_rows(turn_of(slot), slot).start()

    def turn_of(t):
        return (me + (owner_count - 1) - t) % owner_count

    def fetch_rows(q, slot):
        return pltpu.make_async_copy(
            rows_v.at[pl.ds(pl.multiple_of(q * ROWS, ROWS), ROWS)],
            rows_s.at[slot],
            rows_sem.at[slot],
        )

    def send(kind, chunk):
        device = (next_row, next_col, prev_row, prev_col)[kind]
        taken = chunk >= blocks
        moves = (first_core | taken) & (is_far(ahead + 1) if kind < 2 else is_beyond(ahead - 1))
        target = chunk - jnp.where(taken, blocks, 0) + jnp.where(moves, blocks, 0)
        return pltpu.make_async_remote_copy(
            src_ref=face_send.at[kind, chunk],
            dst_ref=face_recv.at[kind, target],
            send_sem=send_sem.at[kind, chunk],
            recv_sem=recv_sem.at[kind, target],
            device_id=dict(device, grid=jnp.where(moves, 1, jnp.where(taken, 0, grid))),
            device_id_type=MESH,
        )

    def arrival(kind, chunk):
        return pltpu.make_async_remote_copy(
            src_ref=face_send.at[kind, chunk],
            dst_ref=face_recv.at[kind, chunk],
            send_sem=send_sem.at[kind, chunk],
            recv_sem=recv_sem.at[kind, chunk],
            device_id={"grid": 1 - grid},
            device_id_type=MESH,
        )

    wave_first = ahead >= 1
    idle_first = ahead >= 2
    gets = (has_prev_row, has_prev_col, has_next_row, has_next_col)
    puts = (has_next_row, has_next_col, has_prev_row, has_prev_col)

    for kind in range(4):

        @pl.when(jnp.logical_not(gets[kind]))
        def _():
            face_recv[kind] = jnp.zeros(face_recv.shape[1:], jnp.float32)

    sub = lax.broadcasted_iota(jnp.int32, (cj, LANES), 0)

    def product(mat, vec):
        out = []
        for r in range(comps):
            terms = [mat(r * comps + c) * vec[c] for c in range(comps)]
            while len(terms) > 1:
                terms = [
                    terms[t] + terms[t + 1] if t + 1 < len(terms) else terms[t]
                    for t in range(0, len(terms), 2)
                ]
            out.append(terms[0])
        return out

    def wait_recv(kind, kb):
        @pl.when(gets[kind])
        def _():
            arrival(kind, kb).wait_recv()

    def start_send(kind, kb):
        @pl.when(puts[kind])
        def _():
            send(kind, kb).start()

    inv_flat = inv_v.reshape(inv_v.shape[0] * entries * cj, LANES)
    res_flat = res_v.reshape(res_v.shape[0] * comps * cj, LANES)
    cpl_flat = cpl_v.reshape(cpl_v.shape[0] * cj * ROWS, LANES)
    field_flat = field_v.reshape(field_v.shape[0] * cj * ROWS, LANES)

    def entry(ref, kb, s, height, e):
        base = pl.multiple_of(kb * (pitch * height * cj), ROWS)
        start = base + (s * height * cj + e * cj + cj - 1)
        return ref[pl.ds(start, cj, stride=height * cj - 1), :]

    def cell_rows(kb, s, c):
        base = pl.multiple_of(kb * (pitch * cj * ROWS), ROWS)
        return pl.ds(base + ((s * cj + cj - 1) * ROWS + c), cj, stride=(cj - 1) * ROWS)

    def forward(kb):
        @pl.when(kb < blocks)
        def _():
            for copy in input_copies(kb):
                copy.wait()

        @pl.when(kb >= blocks)
        def _():
            for kind in range(3):
                ship(kind, kb - blocks).wait_recv()

        @pl.when(kb == 0)
        def _():
            for later in range(eager, blocks):
                for copy in input_copies(later):
                    copy.start()

        wait_recv(0, kb)
        wait_recv(1, kb)
        upper = [face_recv[0, kb, pl.ds(c * ROWS, cj), :] for c in range(comps)]
        prev = [jnp.zeros((cj, LANES), jnp.float32)] * comps
        lower = [jnp.zeros((cj, LANES), jnp.float32)] * comps
        for s in range(steps):
            coef_a = cpl_flat[cell_rows(kb, s, 0), :]
            coef_b = cpl_flat[cell_rows(kb, s, 1), :]
            up = prev
            if s < cj:
                up = [jnp.where(sub == cj - 1 - s, upper[c], prev[c]) for c in range(comps)]
            left = [pltpu.roll(p, cj - 1, 0) for p in prev]
            if s < ci:
                left = [
                    jnp.where(
                        sub == cj - 1,
                        jnp.broadcast_to(
                            face_recv[1, kb, pl.ds(c * ROWS + s, 1), :], (cj, LANES)
                        ),
                        left[c],
                    )
                    for c in range(comps)
                ]
            vec = [
                entry(res_flat, kb, s, comps, c) + coef_a * up[c] + coef_b * left[c]
                for c in range(comps)
            ]
            prev = product(lambda e: entry(inv_flat, kb, s, entries, e), vec)
            for c in range(comps):
                star_v[kb, s, c] = prev[c]
                if s >= cj - 1:
                    face_send[1, kb, pl.ds(c * ROWS + s - cj + 1, 1), :] = prev[c][0:1, :]
                if s >= ci - 1:
                    lower[c] = jnp.where(sub == cj + ci - 2 - s, prev[c], lower[c])
        for c in range(comps):
            face_send[0, kb, pl.ds(c * ROWS, cj), :] = lower[c]

        @pl.when((kb == 0) & jnp.logical_not(wave_first))
        def _():
            enter()

        start_send(0, kb)
        start_send(1, kb)

        @pl.when((kb == 0) & jnp.logical_not(wave_first))
        def _():
            wave_on()

        @pl.when(first_core & beyond)
        def _():
            ship(3, kb).start()

    def backward(kb):
        @pl.when((kb >= blocks) & jnp.logical_not(far))
        def _():
            for kind in (0, 1, 3):
                ship(kind, kb - blocks).wait_recv()

        wait_recv(2, kb)
        wait_recv(3, kb)
        under = [face_recv[2, kb, pl.ds(c * ROWS, cj), :] for c in range(comps)]
        prev = [jnp.zeros((cj, LANES), jnp.float32)] * comps
        upper = [jnp.zeros((cj, LANES), jnp.float32)] * comps
        for s in reversed(range(steps)):
            coef_e = cpl_flat[cell_rows(kb, s, 2), :]
            coef_f = cpl_flat[cell_rows(kb, s, 3), :]
            down = prev
            if s >= ci - 1:
                down = [
                    jnp.where(sub == cj + ci - 2 - s, under[c], prev[c]) for c in range(comps)
                ]
            right = [pltpu.roll(p, 1, 0) for p in prev]
            if s >= cj - 1:
                right = [
                    jnp.where(
                        sub == 0,
                        jnp.broadcast_to(
                            face_recv[3, kb, pl.ds(c * ROWS + s - cj + 1, 1), :], (cj, LANES)
                        ),
                        right[c],
                    )
                    for c in range(comps)
                ]
            vec = [coef_e * down[c] + coef_f * right[c] for c in range(comps)]
            prev = product(lambda e: entry(inv_flat, kb, s, entries, e), vec)
            prev = [star_v[kb, s, c] + prev[c] for c in range(comps)]
            for c in range(comps):
                field_flat[cell_rows(kb, s, c), :] = prev[c]
                if s < cj:
                    upper[c] = jnp.where(sub == cj - 1 - s, prev[c], upper[c])
                if s < ci:
                    face_send[3, kb, pl.ds(c * ROWS + s, 1), :] = prev[c][cj - 1 : cj, :]
        for c in range(comps):
            face_send[2, kb, pl.ds(c * ROWS, cj), :] = upper[c]
        start_send(2, kb)
        start_send(3, kb)

        @pl.when(kb >= blocks)
        def _():
            ship(4, kb - blocks).start()

    middle = 2 * blocks + 1
    last = 4 * blocks + 2
    begin = jnp.where(ahead == reach, 1, middle + 1)
    early = (ahead * 3 <= reach) | (first_core & beyond)
    asks_first = far | (second_core & (ahead * 2 >= reach))

    def ship_inputs():
        for kb in range(blocks):
            ship(0, kb).start()
            ship(1, kb).start()

            @pl.when(far)
            def _():
                ship(2, kb).start()

    @pl.loop(0, last + 1)
    def _(n):
        @pl.when((n == 0) & wave_first)
        def _():
            enter()

        @pl.when(first_core & beyond & (n == 0))
        def _():
            ship_inputs()

        @pl.when((n == 0) & wave_first)
        def _():
            wave_on()

        @pl.when(((n == 0) & idle_first) | ((n == middle) & jnp.logical_not(idle_first)))
        def _():
            plan()

        @pl.when(((n == 0) & asks_first) | ((n == middle) & jnp.logical_not(asks_first)))
        def _():
            send_asks()

        ahead_chunk = n - 1
        own = (ahead_chunk >= 0) & (ahead_chunk < blocks) & own_forward
        taken = (ahead_chunk >= blocks) & (ahead_chunk < 2 * blocks) & taken_forward

        @pl.when(own | taken)
        def _():
            forward(ahead_chunk)

        back_chunk = n - begin
        own = (back_chunk >= 0) & (back_chunk < blocks) & own_backward
        taken = (back_chunk >= blocks) & (back_chunk < 2 * blocks) & taken_backward

        @pl.when(own | taken)
        def _():
            backward(back_chunk)

        @pl.when(((n == middle) & early) | ((n == last) & jnp.logical_not(early)))
        def _():
            prepare()

    @pl.when(first_core & beyond)
    def _():
        for kb in range(blocks):
            ship(4, kb).wait_recv()

    lane8 = lax.broadcasted_iota(jnp.int32, (ROWS, LANES), 1)

    def gather(q, slot):
        acc = jnp.zeros((ROWS, LANES), jnp.float32)
        for s in range(slot_count):
            parts = [
                field_flat[pl.ds(rows_s[slot, d, s], ROWS), :] * spread[d, pl.ds(q * slot_count + s, 1), :]
                for d in range(many)
            ]
            while len(parts) > 1:
                parts = [parts[i] + parts[i + 1] for i in range(0, len(parts), 2)]
            total = jnp.sum(parts[0], axis=1, keepdims=True)
            acc = jnp.where(lane8 == s, total, acc)
        reply_send[q] = acc
        reply(q).start()

    @pl.loop(0, owner_count // FETCHES)
    def _(turn):
        for slot in range(FETCHES):
            t = turn * FETCHES + slot
            following = t + FETCHES - 1

            @pl.when(following < owner_count)
            def _():
                fetch_rows(turn_of(following), (slot + FETCHES - 1) % FETCHES).start()

            fetch_rows(turn_of(t), slot).wait()
            gather(turn_of(t), slot)

    @pl.loop(0, owner_count)
    def _(q):
        ask(q).wait_send()
        reply(q).wait_send()

    for chunk in range(2 * blocks):
        own = chunk < blocks
        for kind in range(4):
            if kind < 2:
                done = own_forward if own else taken_forward
            else:
                done = own_backward if own else taken_backward

            @pl.when(puts[kind] & done)
            def _():
                send(kind, chunk).wait_send()

    for kb in range(blocks):
        for kind in range(5):
            sent = (
                first_core & beyond,
                first_core & beyond,
                first_core & far,
                first_core & beyond & jnp.logical_not(far),
                taken_backward,
            )[kind]

            @pl.when(sent)
            def _():
                ship(kind, kb).wait_send()

    @pl.loop(0, owner_count)
    def _(q):
        replied(q).wait_recv()
        reply_out[q] = reply_recv[q]


def run_sweeps(residual, inverses, couplings, owners, donors, weights, receptors):
    inputs = (residual, inverses, couplings, owners, donors, weights, receptors)
    ci, comps, cj, length = residual.shape
    many, count = donors.shape
    blocks = length // LANES
    steps = ci + cj - 1
    tall = 2 * blocks * (ci + cj - 1) + cj - 1
    rows, cols = lax.axis_size("px"), lax.axis_size("py")
    owner_count = rows * cols
    slot_count = max(2, 2 * count // owner_count)
    slots = owner_count * slot_count
    assert owner_count % FETCHES == 0 and cj == ROWS and ci <= ROWS and many == ROWS and 2 * slot_count <= LANES
    assert ci * cj * length <= 2 ** (2 * LOW)
    dims = (ci, cj, comps, blocks, rows, cols, slot_count)
    face = comps * ROWS
    dma = pltpu.SemaphoreType.DMA
    hbm = pl.BlockSpec(memory_space=pltpu.HBM)
    vmem = pl.BlockSpec(memory_space=pltpu.VMEM)
    return pl.pallas_call(
        functools.partial(sweep_kernel, dims),
        out_shape=(
            pltpu.VMEM((tall, cj, ROWS, LANES), jnp.float32),
            pltpu.VMEM((1, slots), jnp.int32),
            pltpu.VMEM((owner_count, ROWS, LANES), jnp.float32),
        ),
        in_specs=[hbm] * 7,
        out_specs=(vmem, vmem, vmem),
        scratch_shapes=[
            pltpu.VMEM(owners.shape, owners.dtype),
            pltpu.VMEM(donors.shape, donors.dtype),
            pltpu.VMEM(weights.shape, weights.dtype),
            pltpu.VMEM(receptors.shape, receptors.dtype),
            pltpu.VMEM((tall, comps * comps, cj, LANES), jnp.float32),
            pltpu.VMEM((tall, comps, cj, LANES), jnp.float32),
            pltpu.VMEM((tall, cj, ROWS, LANES), jnp.float32),
            pltpu.VMEM((2 * blocks, steps, comps, cj, LANES), jnp.float32),
            pltpu.VMEM((4, 2 * blocks, face, LANES), jnp.float32),
            pltpu.VMEM((4, 2 * blocks, face, LANES), jnp.float32),
            pltpu.VMEM((owner_count, ROWS, LANES), jnp.float32),
            pltpu.VMEM((owner_count, ROWS, LANES), jnp.float32),
            pltpu.VMEM((owner_count * ROWS, LANES), jnp.int32),
            pltpu.SMEM((FETCHES, ROWS, LANES), jnp.int32),
            pltpu.VMEM((many, slots, LANES), jnp.float32),
            pltpu.VMEM((owner_count, ROWS, LANES), jnp.float32),
            pltpu.VMEM((owner_count, ROWS, LANES), jnp.float32),
            dma((3, blocks)),
            dma((4,)),
            dma((4, 2 * blocks)),
            dma((4, 2 * blocks)),
            dma((5, blocks)),
            dma((5, blocks)),
            dma((owner_count,)),
            dma((owner_count,)),
            dma((owner_count,)),
            dma((owner_count,)),
            dma((FETCHES,)),
            pltpu.SemaphoreType.REGULAR((4,)),
        ],
        compiler_params=pltpu.CompilerParams(
            collective_id=0, has_side_effects=True, vmem_limit_bytes=53 * 1024 * 1024
        ),
    )(*(pltpu.with_memory_space_constraint(x, pltpu.HBM) for x in inputs))


def place_kernel(dims, code, reply, field, out_hbm, work, out, out_sem):
    ci, cj, comps, slot_count = dims
    owner_count = reply.shape[0]
    blocks = out.shape[3] // LANES
    pitch = ci + cj - 1
    lane = lax.broadcasted_iota(jnp.int32, (ROWS, LANES), 1)
    lines = work.reshape(work.shape[0] * cj * ROWS, LANES)

    for q in range(owner_count):
        tile = reply[q]
        for s in range(slot_count):
            line, spot = divmod_const(code[0, q * slot_count + s], 2 * LANES)
            rows = pl.ds(pl.multiple_of(line, ROWS), ROWS)
            value = jnp.broadcast_to(tile[:, s : s + 1], (ROWS, LANES))
            pltpu.store(lines.at[rows], value, mask=lane == spot)

    stack = work.reshape(work.shape[0], cj * ROWS, LANES)

    def out_copy(i):
        return pltpu.make_async_copy(out.at[i], out_hbm.at[i], out_sem.at[i])

    @pl.loop(0, ci)
    def _(i):
        for kb in range(blocks):
            for c in range(comps):
                out[i, c, :, kb * LANES : (kb + 1) * LANES] = stack[
                    kb * pitch + cj - 1 + i, pl.ds(c, cj, stride=ROWS), :
                ]
        out_copy(i).start()

    @pl.loop(0, ci)
    def _(i):
        out_copy(i).wait()


def run_place(code, reply, field, length, dims):
    ci, cj, comps, slot_count = dims
    vmem = pl.BlockSpec(memory_space=pltpu.VMEM)
    return pl.pallas_call(
        functools.partial(place_kernel, dims),
        out_shape=(
            jax.ShapeDtypeStruct((ci, comps, cj, length), jnp.float32),
            jax.ShapeDtypeStruct(field.shape, jnp.float32),
        ),
        in_specs=[pl.BlockSpec(memory_space=pltpu.SMEM), vmem, vmem],
        out_specs=(pl.BlockSpec(memory_space=pltpu.HBM), vmem),
        scratch_shapes=[
            pltpu.VMEM((ci, comps, cj, length), jnp.float32),
            pltpu.SemaphoreType.DMA((ci,)),
        ],
        input_output_aliases={2: 1},
        compiler_params=pltpu.CompilerParams(vmem_limit_bytes=16 * 1024 * 1024),
    )(code, reply, field)[0]


def local(residual, inverses, couplings, receptors, owners, donors, weights):
    ci, cj, comps = residual.shape[1:4]
    many = donors.shape[-1]
    count = donors.shape[-2]
    field, code, reply = run_sweeps(
        residual[0].transpose(0, 2, 1, 3),
        inverses[0].transpose(0, 2, 1, 3),
        couplings[0],
        owners.reshape(1, count),
        donors.reshape(count, many).T,
        weights.reshape(count, many).T,
        receptors.reshape(1, count),
    )
    slot_count = code.shape[1] // reply.shape[0]
    update = run_place(code, reply, field, residual.shape[4], (ci, cj, comps, slot_count))
    return update.transpose(0, 2, 1, 3)[None]


def solution(mesh):
    placed = (
        P("grid", "px", "py", None, None),
        P("grid", "px", "py", None, None),
        P("grid", "px", "py", None, None),
        P("grid", "px", "py", None),
        P("grid", "px", "py", None, None),
        P("grid", "px", "py", None, None),
        P("grid", "px", "py", None, None),
    )
    return jax.shard_map(
        local,
        mesh=mesh,
        in_specs=placed,
        out_specs=P("grid", "px", "py", None, None),
        check_vma=False,
    )
```

```python
import functools

import jax
import jax.numpy as jnp
from jax import lax
from jax.experimental import pallas as pl
from jax.experimental.pallas import tpu as pltpu
from jax.sharding import PartitionSpec as P

MESH = pl.DeviceIdType.MESH
LANES = 128
ROWS = 8
LOW = 8
EMPTY = LANES
FETCHES = 4


def divmod_const(value, by):
    if by & (by - 1) == 0:
        return value >> (by.bit_length() - 1), value & (by - 1)
    return value // by, value % by


def sweep_kernel(
    dims,
    res_hbm,
    inv_hbm,
    cpl_hbm,
    owners_hbm,
    donors_hbm,
    weights_hbm,
    receptors_hbm,
    field_v,
    code_out,
    reply_out,
    owners,
    donors,
    weights,
    receptors,
    inv_v,
    res_v,
    cpl_v,
    star_v,
    face_send,
    face_recv,
    ask_send,
    ask_recv,
    rows_v,
    rows_s,
    spread,
    reply_send,
    reply_recv,
    in_sem,
    small_sem,
    send_sem,
    recv_sem,
    ship_send_sem,
    ship_recv_sem,
    ask_send_sem,
    ask_recv_sem,
    reply_send_sem,
    reply_recv_sem,
    rows_sem,
    wave_sem,
):
    ci, cj, comps, blocks, count_rows, count_cols, slot_count = dims
    length = blocks * LANES
    entries = comps * comps
    steps = ci + cj - 1
    pitch = ci + cj - 1
    many, count = donors.shape
    owner_count = count_rows * count_cols
    slots = owner_count * slot_count
    grid = lax.axis_index("grid")
    px = lax.axis_index("px")
    py = lax.axis_index("py")
    me = px * count_cols + py
    ahead = px + py
    reach = count_rows + count_cols - 2

    first_core = grid == 0
    second_core = grid == 1

    def is_far(at):
        return at * 3 >= reach * 2

    def is_beyond(at):
        return at >= 1

    far = is_far(ahead)
    beyond = is_beyond(ahead)
    own_forward = second_core | jnp.logical_not(far)
    own_backward = second_core | jnp.logical_not(beyond)
    taken_forward = second_core & far
    taken_backward = second_core & beyond

    def rows_of(chunk):
        return pl.ds(chunk * pitch + cj - 1, ci)

    def inputs_of(kb, chunk):
        lanes = pl.ds(pl.multiple_of(kb * LANES, LANES), LANES)
        rows = rows_of(chunk)
        return (
            (inv_hbm.at[:, :, :, lanes], inv_v.at[rows]),
            (cpl_hbm.at[:, :, :, lanes], cpl_v.at[rows, :, pl.ds(0, 4), :]),
            (res_hbm.at[:, :, :, lanes], res_v.at[rows]),
        )

    def input_copies(kb):
        return [
            pltpu.make_async_copy(source, target, in_sem.at[t, kb])
            for t, (source, target) in enumerate(inputs_of(kb, kb))
        ]

    def ship(kind, kb):
        if kind < 3:
            source, target = inputs_of(kb, blocks + kb)[kind]
        elif kind == 3:
            source, target = star_v.at[kb], star_v.at[blocks + kb]
        else:
            source, target = field_v.at[rows_of(blocks + kb)], field_v.at[rows_of(kb)]
        return pltpu.make_async_remote_copy(
            src_ref=source,
            dst_ref=target,
            send_sem=ship_send_sem.at[kind, kb],
            recv_sem=ship_recv_sem.at[kind, kb],
            device_id={"grid": 1 - grid},
            device_id_type=MESH,
        )

    small_copies = [
        pltpu.make_async_copy(source, target, small_sem.at[t])
        for t, (source, target) in enumerate(
            (
                (owners_hbm, owners),
                (donors_hbm, donors),
                (weights_hbm, weights),
                (receptors_hbm, receptors),
            )
        )
    ]
    eager = min(2, blocks)

    @pl.when(own_forward)
    def _():
        for kb in range(eager):
            for copy in input_copies(kb):
                copy.start()

    for copy in small_copies:
        copy.start()

    has_prev_row = px > 0
    has_next_row = px < count_rows - 1
    has_prev_col = py > 0
    has_next_col = py < count_cols - 1
    prev_row = {"px": px - 1}
    next_row = {"px": px + 1}
    prev_col = {"py": py - 1}
    next_col = {"py": py + 1}
    sides = (
        (has_prev_row, prev_row),
        (has_next_row, next_row),
        (has_prev_col, prev_col),
        (has_next_col, next_col),
    )

    def other(q):
        return {"grid": 1 - grid, "px": q // count_cols, "py": q % count_cols}

    barrier = pltpu.get_barrier_semaphore()
    for there, device in sides:

        @pl.when(there)
        def _():
            for core in range(2):
                pl.semaphore_signal(
                    barrier, inc=1, device_id=dict(device, grid=core), device_id_type=MESH
                )

    pl.semaphore_signal(
        barrier, inc=1, device_id={"grid": 1 - grid}, device_id_type=MESH
    )

    def enter():
        near = sum(there.astype(jnp.int32) for there, _ in sides)
        pl.semaphore_wait(barrier, 2 * near + 1)

    def wave(came_from, goes_to):
        for kind, there, _ in came_from:

            @pl.when(there)
            def _():
                pl.semaphore_wait(wave_sem.at[kind], 1)

        for kind, there, device in goes_to:

            @pl.when(there)
            def _():
                pl.semaphore_signal(
                    wave_sem.at[kind], inc=1, device_id=device, device_id_type=MESH
                )

    def wave_on():
        wave(
            ((0, has_prev_row, prev_row), (1, has_prev_col, prev_col)),
            ((0, has_next_row, next_row), (1, has_next_col, next_col)),
        )

    def wave_back():
        wave(
            ((2, has_next_row, next_row), (3, has_next_col, next_col)),
            ((2, has_prev_row, prev_row), (3, has_prev_col, prev_col)),
        )

    def ask(q):
        return pltpu.make_async_remote_copy(
            src_ref=ask_send.at[q],
            dst_ref=ask_recv.at[me],
            send_sem=ask_send_sem.at[q],
            recv_sem=ask_recv_sem.at[me],
            device_id=other(q),
            device_id_type=MESH,
        )

    def asked(q):
        return pltpu.make_async_remote_copy(
            src_ref=ask_send.at[q],
            dst_ref=ask_recv.at[q],
            send_sem=ask_send_sem.at[q],
            recv_sem=ask_recv_sem.at[q],
            device_id=other(q),
            device_id_type=MESH,
        )

    def reply(q):
        return pltpu.make_async_remote_copy(
            src_ref=reply_send.at[q],
            dst_ref=reply_recv.at[me],
            send_sem=reply_send_sem.at[q],
            recv_sem=reply_recv_sem.at[me],
            device_id=other(q),
            device_id_type=MESH,
        )

    def replied(q):
        return pltpu.make_async_remote_copy(
            src_ref=reply_send.at[q],
            dst_ref=reply_recv.at[q],
            send_sem=reply_send_sem.at[q],
            recv_sem=reply_recv_sem.at[q],
            device_id=other(q),
            device_id_type=MESH,
        )

    def digits(value):
        return [(value >> LOW).astype(jnp.float32), (value & (2**LOW - 1)).astype(jnp.float32)]

    def plan():
        for copy in small_copies:
            copy.wait()
        owner = owners[...]
        ones = jnp.where(
            owner == lax.broadcasted_iota(jnp.int32, (owner_count, count), 0), 1.0, 0.0
        )
        before = jnp.where(
            lax.broadcasted_iota(jnp.int32, (count, count), 0)
            < lax.broadcasted_iota(jnp.int32, (count, count), 1),
            1.0,
            0.0,
        ).astype(jnp.bfloat16)
        seen = jnp.dot(ones.astype(jnp.bfloat16), before, preferred_element_type=jnp.float32)
        rank = jnp.sum(seen * ones, axis=0, keepdims=True).astype(jnp.int32)
        place = owner * slot_count + rank
        weight = weights[...]
        high = weight.astype(jnp.bfloat16).astype(jnp.float32)
        mid = (weight - high).astype(jnp.bfloat16).astype(jnp.float32)
        low = weight - high - mid
        cell = receptors[...]
        marks = jnp.concatenate(
            digits(cell) + [jnp.ones((1, count), jnp.float32), jnp.zeros((ROWS - 3, count), jnp.float32)],
            axis=0,
        )
        table = jnp.concatenate(digits(donors[...]) + [high, mid, low, marks], axis=0).astype(
            jnp.bfloat16
        )
        wide = min(2 * LANES, slots)
        lane = lax.broadcasted_iota(jnp.int32, (many, LANES), 1)
        for base in range(0, slots, wide):
            slot = lax.broadcasted_iota(jnp.int32, (wide, count), 0) + base
            pick = jnp.where(slot == place, 1.0, 0.0).astype(jnp.bfloat16)
            got = lax.dot_general(
                table, pick, (((1,), (1,)), ((), ())), preferred_element_type=jnp.float32
            )
            cells = got[:many] * float(2**LOW) + got[many : 2 * many]
            share = got[2 * many : 3 * many] + got[3 * many : 4 * many] + got[4 * many : 5 * many]
            mark = got[5 * many : 5 * many + 3]
            target = (mark[0:1] * float(2**LOW) + mark[1:2]).astype(jnp.int32)
            pencil, k = divmod_const(target, length)
            kb, spot = divmod_const(k, LANES)
            line = kb * (pitch * cj) + (cj - 1) * cj + pencil
            code_out[:, base : base + wide] = jnp.where(
                mark[2:3] > 0.5, line * (ROWS * 2 * LANES) + spot, EMPTY
            )
            for q in range(base // slot_count, (base + wide) // slot_count):
                at = q * slot_count - base
                tile = at // LANES * LANES
                shift = at - tile
                left = cells[:, tile : tile + LANES]
                right = share[:, tile : tile + LANES]
                if shift:
                    left = pltpu.roll(left, LANES - shift, 1)
                if (slot_count - shift) % LANES:
                    right = pltpu.roll(right, (slot_count - shift) % LANES, 1)
                ask_send[q] = jnp.where(lane < slot_count, left, right)

    def send_asks():
        wave_back()

        @pl.loop(0, owner_count)
        def _(q):
            ask(q).start()

    def prepare():
        line = lax.broadcasted_iota(jnp.int32, (slot_count, LANES), 1)

        @pl.loop(0, owner_count)
        def _(q):
            asked(q).wait_recv()
            tile = ask_recv[q]
            cell = tile.astype(jnp.int32)
            pencil, k = divmod_const(cell, length)
            kb, _ = divmod_const(k, LANES)
            i, j = divmod_const(pencil, cj)
            row = kb * (pitch * cj) + (i + (cj - 1)) * cj + j
            rows_v[pl.ds(pl.multiple_of(q * ROWS, ROWS), ROWS), :] = jnp.clip(
                row, 0, field_v.shape[0] * cj - 1
            ) * ROWS
            turned = tile.T
            first = pl.multiple_of(q * slot_count, slot_count)
            for d in range(many):
                spot = turned[:slot_count, d : d + 1].astype(jnp.int32) & (LANES - 1)
                share = turned[slot_count : 2 * slot_count, d : d + 1]
                spread[d, pl.ds(first, slot_count), :] = jnp.where(line == spot, share, 0.0)

        for slot in range(FETCHES - 1):
            fetch_rows(turn_of(slot), slot).start()

    def turn_of(t):
        return (me + (owner_count - 1) - t) % owner_count

    def fetch_rows(q, slot):
        return pltpu.make_async_copy(
            rows_v.at[pl.ds(pl.multiple_of(q * ROWS, ROWS), ROWS)],
            rows_s.at[slot],
            rows_sem.at[slot],
        )

    def send(kind, chunk):
        device = (next_row, next_col, prev_row, prev_col)[kind]
        taken = chunk >= blocks
        moves = (first_core | taken) & (is_far(ahead + 1) if kind < 2 else is_beyond(ahead - 1))
        target = chunk - jnp.where(taken, blocks, 0) + jnp.where(moves, blocks, 0)
        return pltpu.make_async_remote_copy(
            src_ref=face_send.at[kind, chunk],
            dst_ref=face_recv.at[kind, target],
            send_sem=send_sem.at[kind, chunk],
            recv_sem=recv_sem.at[kind, target],
            device_id=dict(device, grid=jnp.where(moves, 1, jnp.where(taken, 0, grid))),
            device_id_type=MESH,
        )

    def arrival(kind, chunk):
        return pltpu.make_async_remote_copy(
            src_ref=face_send.at[kind, chunk],
            dst_ref=face_recv.at[kind, chunk],
            send_sem=send_sem.at[kind, chunk],
            recv_sem=recv_sem.at[kind, chunk],
            device_id={"grid": 1 - grid},
            device_id_type=MESH,
        )

    wave_first = ahead >= 1
    idle_first = ahead >= 2
    gets = (has_prev_row, has_prev_col, has_next_row, has_next_col)
    puts = (has_next_row, has_next_col, has_prev_row, has_prev_col)

    for kind in range(4):

        @pl.when(jnp.logical_not(gets[kind]))
        def _():
            face_recv[kind] = jnp.zeros(face_recv.shape[1:], jnp.float32)

    sub = lax.broadcasted_iota(jnp.int32, (cj, LANES), 0)

    def product(mat, vec):
        out = []
        for r in range(comps):
            terms = [mat(r * comps + c) * vec[c] for c in range(comps)]
            while len(terms) > 1:
                terms = [
                    terms[t] + terms[t + 1] if t + 1 < len(terms) else terms[t]
                    for t in range(0, len(terms), 2)
                ]
            out.append(terms[0])
        return out

    def wait_recv(kind, kb):
        @pl.when(gets[kind])
        def _():
            arrival(kind, kb).wait_recv()

    def start_send(kind, kb):
        @pl.when(puts[kind])
        def _():
            send(kind, kb).start()

    inv_flat = inv_v.reshape(inv_v.shape[0] * entries * cj, LANES)
    res_flat = res_v.reshape(res_v.shape[0] * comps * cj, LANES)
    cpl_flat = cpl_v.reshape(cpl_v.shape[0] * cj * ROWS, LANES)
    field_flat = field_v.reshape(field_v.shape[0] * cj * ROWS, LANES)

    def entry(ref, kb, s, height, e):
        base = pl.multiple_of(kb * (pitch * height * cj), ROWS)
        start = base + (s * height * cj + e * cj + cj - 1)
        return ref[pl.ds(start, cj, stride=height * cj - 1), :]

    def cell_rows(kb, s, c):
        base = pl.multiple_of(kb * (pitch * cj * ROWS), ROWS)
        return pl.ds(base + ((s * cj + cj - 1) * ROWS + c), cj, stride=(cj - 1) * ROWS)

    def forward(kb):
        @pl.when(kb < blocks)
        def _():
            for copy in input_copies(kb):
                copy.wait()

        @pl.when(kb >= blocks)
        def _():
            for kind in range(3):
                ship(kind, kb - blocks).wait_recv()

        @pl.when(kb == 0)
        def _():
            for later in range(eager, blocks):
                for copy in input_copies(later):
                    copy.start()

        wait_recv(0, kb)
        wait_recv(1, kb)
        upper = [face_recv[0, kb, pl.ds(c * ROWS, cj), :] for c in range(comps)]
        prev = [jnp.zeros((cj, LANES), jnp.float32)] * comps
        lower = [jnp.zeros((cj, LANES), jnp.float32)] * comps
        for s in range(steps):
            coef_a = cpl_flat[cell_rows(kb, s, 0), :]
            coef_b = cpl_flat[cell_rows(kb, s, 1), :]
            up = prev
            if s < cj:
                up = [jnp.where(sub == cj - 1 - s, upper[c], prev[c]) for c in range(comps)]
            left = [pltpu.roll(p, cj - 1, 0) for p in prev]
            if s < ci:
                left = [
                    jnp.where(
                        sub == cj - 1,
                        jnp.broadcast_to(
                            face_recv[1, kb, pl.ds(c * ROWS + s, 1), :], (cj, LANES)
                        ),
                        left[c],
                    )
                    for c in range(comps)
                ]
            vec = [
                entry(res_flat, kb, s, comps, c) + coef_a * up[c] + coef_b * left[c]
                for c in range(comps)
            ]
            prev = product(lambda e: entry(inv_flat, kb, s, entries, e), vec)
            for c in range(comps):
                star_v[kb, s, c] = prev[c]
                if s >= cj - 1:
                    face_send[1, kb, pl.ds(c * ROWS + s - cj + 1, 1), :] = prev[c][0:1, :]
                if s >= ci - 1:
                    lower[c] = jnp.where(sub == cj + ci - 2 - s, prev[c], lower[c])
        for c in range(comps):
            face_send[0, kb, pl.ds(c * ROWS, cj), :] = lower[c]

        @pl.when((kb == 0) & jnp.logical_not(wave_first))
        def _():
            enter()

        start_send(0, kb)
        start_send(1, kb)

        @pl.when((kb == 0) & jnp.logical_not(wave_first))
        def _():
            wave_on()

        @pl.when(first_core & beyond)
        def _():
            ship(3, kb).start()

    def backward(kb):
        @pl.when((kb >= blocks) & jnp.logical_not(far))
        def _():
            for kind in (0, 1, 3):
                ship(kind, kb - blocks).wait_recv()

        wait_recv(2, kb)
        wait_recv(3, kb)
        under = [face_recv[2, kb, pl.ds(c * ROWS, cj), :] for c in range(comps)]
        prev = [jnp.zeros((cj, LANES), jnp.float32)] * comps
        upper = [jnp.zeros((cj, LANES), jnp.float32)] * comps
        for s in reversed(range(steps)):
            coef_e = cpl_flat[cell_rows(kb, s, 2), :]
            coef_f = cpl_flat[cell_rows(kb, s, 3), :]
            down = prev
            if s >= ci - 1:
                down = [
                    jnp.where(sub == cj + ci - 2 - s, under[c], prev[c]) for c in range(comps)
                ]
            right = [pltpu.roll(p, 1, 0) for p in prev]
            if s >= cj - 1:
                right = [
                    jnp.where(
                        sub == 0,
                        jnp.broadcast_to(
                            face_recv[3, kb, pl.ds(c * ROWS + s - cj + 1, 1), :], (cj, LANES)
                        ),
                        right[c],
                    )
                    for c in range(comps)
                ]
            vec = [coef_e * down[c] + coef_f * right[c] for c in range(comps)]
            prev = product(lambda e: entry(inv_flat, kb, s, entries, e), vec)
            prev = [star_v[kb, s, c] + prev[c] for c in range(comps)]
            for c in range(comps):
                field_flat[cell_rows(kb, s, c), :] = prev[c]
                if s < cj:
                    upper[c] = jnp.where(sub == cj - 1 - s, prev[c], upper[c])
                if s < ci:
                    face_send[3, kb, pl.ds(c * ROWS + s, 1), :] = prev[c][cj - 1 : cj, :]
        for c in range(comps):
            face_send[2, kb, pl.ds(c * ROWS, cj), :] = upper[c]
        start_send(2, kb)
        start_send(3, kb)

        @pl.when(kb >= blocks)
        def _():
            ship(4, kb - blocks).start()

    middle = 2 * blocks + 1
    last = 4 * blocks + 2
    begin = jnp.where(ahead == reach, 1, middle + 1)
    early = (ahead * 3 <= reach) | (first_core & beyond)
    asks_first = far | (second_core & (ahead * 2 >= reach))

    def ship_inputs():
        for kb in range(blocks):
            ship(0, kb).start()
            ship(1, kb).start()

            @pl.when(far)
            def _():
                ship(2, kb).start()

    @pl.loop(0, last + 1)
    def _(n):
        @pl.when((n == 0) & wave_first)
        def _():
            enter()

        @pl.when(first_core & beyond & (n == 0))
        def _():
            ship_inputs()

        @pl.when((n == 0) & wave_first)
        def _():
            wave_on()

        @pl.when(((n == 0) & idle_first) | ((n == middle) & jnp.logical_not(idle_first)))
        def _():
            plan()

        @pl.when(((n == 0) & asks_first) | ((n == middle) & jnp.logical_not(asks_first)))
        def _():
            send_asks()

        ahead_chunk = n - 1
        own = (ahead_chunk >= 0) & (ahead_chunk < blocks) & own_forward
        taken = (ahead_chunk >= blocks) & (ahead_chunk < 2 * blocks) & taken_forward

        @pl.when(own | taken)
        def _():
            forward(ahead_chunk)

        back_chunk = n - begin
        own = (back_chunk >= 0) & (back_chunk < blocks) & own_backward
        taken = (back_chunk >= blocks) & (back_chunk < 2 * blocks) & taken_backward

        @pl.when(own | taken)
        def _():
            backward(back_chunk)

        @pl.when(((n == middle) & early) | ((n == last) & jnp.logical_not(early)))
        def _():
            prepare()

    @pl.when(first_core & beyond)
    def _():
        for kb in range(blocks):
            ship(4, kb).wait_recv()

    lane8 = lax.broadcasted_iota(jnp.int32, (ROWS, LANES), 1)

    def gather(q, slot):
        acc = jnp.zeros((ROWS, LANES), jnp.float32)
        for s in range(slot_count):
            parts = [
                field_flat[pl.ds(rows_s[slot, d, s], ROWS), :] * spread[d, pl.ds(q * slot_count + s, 1), :]
                for d in range(many)
            ]
            while len(parts) > 1:
                parts = [parts[i] + parts[i + 1] for i in range(0, len(parts), 2)]
            total = jnp.sum(parts[0], axis=1, keepdims=True)
            acc = jnp.where(lane8 == s, total, acc)
        reply_send[q] = acc
        reply(q).start()

    @pl.loop(0, owner_count // FETCHES)
    def _(turn):
        for slot in range(FETCHES):
            t = turn * FETCHES + slot
            following = t + FETCHES - 1

            @pl.when(following < owner_count)
            def _():
                fetch_rows(turn_of(following), (slot + FETCHES - 1) % FETCHES).start()

            fetch_rows(turn_of(t), slot).wait()
            gather(turn_of(t), slot)

    @pl.loop(0, owner_count)
    def _(q):
        ask(q).wait_send()
        reply(q).wait_send()

    for chunk in range(2 * blocks):
        own = chunk < blocks
        for kind in range(4):
            if kind < 2:
                done = own_forward if own else taken_forward
            else:
                done = own_backward if own else taken_backward

            @pl.when(puts[kind] & done)
            def _():
                send(kind, chunk).wait_send()

    for kb in range(blocks):
        for kind in range(5):
            sent = (
                first_core & beyond,
                first_core & beyond,
                first_core & far,
                first_core & beyond & jnp.logical_not(far),
                taken_backward,
            )[kind]

            @pl.when(sent)
            def _():
                ship(kind, kb).wait_send()

    @pl.loop(0, owner_count)
    def _(q):
        replied(q).wait_recv()
        reply_out[q] = reply_recv[q]


def run_sweeps(residual, inverses, couplings, owners, donors, weights, receptors):
    inputs = (residual, inverses, couplings, owners, donors, weights, receptors)
    ci, comps, cj, length = residual.shape
    many, count = donors.shape
    blocks = length // LANES
    steps = ci + cj - 1
    tall = 2 * blocks * (ci + cj - 1) + cj - 1
    rows, cols = lax.axis_size("px"), lax.axis_size("py")
    owner_count = rows * cols
    slot_count = max(2, 2 * count // owner_count)
    slots = owner_count * slot_count
    assert owner_count % FETCHES == 0 and cj == ROWS and ci <= ROWS and many == ROWS and 2 * slot_count <= LANES
    assert ci * cj * length <= 2 ** (2 * LOW)
    dims = (ci, cj, comps, blocks, rows, cols, slot_count)
    face = comps * ROWS
    dma = pltpu.SemaphoreType.DMA
    hbm = pl.BlockSpec(memory_space=pltpu.HBM)
    vmem = pl.BlockSpec(memory_space=pltpu.VMEM)
    return pl.pallas_call(
        functools.partial(sweep_kernel, dims),
        out_shape=(
            pltpu.VMEM((tall, cj, ROWS, LANES), jnp.float32),
            pltpu.VMEM((1, slots), jnp.int32),
            pltpu.VMEM((owner_count, ROWS, LANES), jnp.float32),
        ),
        in_specs=[hbm] * 7,
        out_specs=(vmem, vmem, vmem),
        scratch_shapes=[
            pltpu.VMEM(owners.shape, owners.dtype),
            pltpu.VMEM(donors.shape, donors.dtype),
            pltpu.VMEM(weights.shape, weights.dtype),
            pltpu.VMEM(receptors.shape, receptors.dtype),
            pltpu.VMEM((tall, comps * comps, cj, LANES), jnp.float32),
            pltpu.VMEM((tall, comps, cj, LANES), jnp.float32),
            pltpu.VMEM((tall, cj, ROWS, LANES), jnp.float32),
            pltpu.VMEM((2 * blocks, steps, comps, cj, LANES), jnp.float32),
            pltpu.VMEM((4, 2 * blocks, face, LANES), jnp.float32),
            pltpu.VMEM((4, 2 * blocks, face, LANES), jnp.float32),
            pltpu.VMEM((owner_count, ROWS, LANES), jnp.float32),
            pltpu.VMEM((owner_count, ROWS, LANES), jnp.float32),
            pltpu.VMEM((owner_count * ROWS, LANES), jnp.int32),
            pltpu.SMEM((FETCHES, ROWS, LANES), jnp.int32),
            pltpu.VMEM((many, slots, LANES), jnp.float32),
            pltpu.VMEM((owner_count, ROWS, LANES), jnp.float32),
            pltpu.VMEM((owner_count, ROWS, LANES), jnp.float32),
            dma((3, blocks)),
            dma((4,)),
            dma((4, 2 * blocks)),
            dma((4, 2 * blocks)),
            dma((5, blocks)),
            dma((5, blocks)),
            dma((owner_count,)),
            dma((owner_count,)),
            dma((owner_count,)),
            dma((owner_count,)),
            dma((FETCHES,)),
            pltpu.SemaphoreType.REGULAR((4,)),
        ],
        compiler_params=pltpu.CompilerParams(
            collective_id=0, has_side_effects=True, vmem_limit_bytes=53 * 1024 * 1024
        ),
    )(*(pltpu.with_memory_space_constraint(x, pltpu.HBM) for x in inputs))


def place_kernel(dims, code, reply, field, out_hbm, work, out, out_sem):
    ci, cj, comps, slot_count = dims
    owner_count = reply.shape[0]
    blocks = out.shape[3] // LANES
    pitch = ci + cj - 1
    lane = lax.broadcasted_iota(jnp.int32, (ROWS, LANES), 1)
    lines = work.reshape(work.shape[0] * cj * ROWS, LANES)

    for s in range(slot_count):
        for q in range(owner_count):
            tile = reply[q]
            line, spot = divmod_const(code[0, q * slot_count + s], 2 * LANES)
            rows = pl.ds(pl.multiple_of(line, ROWS), ROWS)
            value = jnp.broadcast_to(tile[:, s : s + 1], (ROWS, LANES))
            pltpu.store(lines.at[rows], value, mask=lane == spot)

    stack = work.reshape(work.shape[0], cj * ROWS, LANES)

    def out_copy(i):
        return pltpu.make_async_copy(out.at[i], out_hbm.at[i], out_sem.at[i])

    @pl.loop(0, ci)
    def _(i):
        for kb in range(blocks):
            for c in range(comps):
                out[i, c, :, kb * LANES : (kb + 1) * LANES] = stack[
                    kb * pitch + cj - 1 + i, pl.ds(c, cj, stride=ROWS), :
                ]
        out_copy(i).start()

    @pl.loop(0, ci)
    def _(i):
        out_copy(i).wait()


def run_place(code, reply, field, length, dims):
    ci, cj, comps, slot_count = dims
    vmem = pl.BlockSpec(memory_space=pltpu.VMEM)
    return pl.pallas_call(
        functools.partial(place_kernel, dims),
        out_shape=(
            jax.ShapeDtypeStruct((ci, comps, cj, length), jnp.float32),
            jax.ShapeDtypeStruct(field.shape, jnp.float32),
        ),
        in_specs=[pl.BlockSpec(memory_space=pltpu.SMEM), vmem, vmem],
        out_specs=(pl.BlockSpec(memory_space=pltpu.HBM), vmem),
        scratch_shapes=[
            pltpu.VMEM((ci, comps, cj, length), jnp.float32),
            pltpu.SemaphoreType.DMA((ci,)),
        ],
        input_output_aliases={2: 1},
        compiler_params=pltpu.CompilerParams(vmem_limit_bytes=16 * 1024 * 1024),
    )(code, reply, field)[0]


def local(residual, inverses, couplings, receptors, owners, donors, weights):
    ci, cj, comps = residual.shape[1:4]
    many = donors.shape[-1]
    count = donors.shape[-2]
    field, code, reply = run_sweeps(
        residual[0].transpose(0, 2, 1, 3),
        inverses[0].transpose(0, 2, 1, 3),
        couplings[0],
        owners.reshape(1, count),
        donors.reshape(count, many).T,
        weights.reshape(count, many).T,
        receptors.reshape(1, count),
    )
    slot_count = code.shape[1] // reply.shape[0]
    update = run_place(code, reply, field, residual.shape[4], (ci, cj, comps, slot_count))
    return update.transpose(0, 2, 1, 3)[None]


def solution(mesh):
    placed = (
        P("grid", "px", "py", None, None),
        P("grid", "px", "py", None, None),
        P("grid", "px", "py", None, None),
        P("grid", "px", "py", None),
        P("grid", "px", "py", None, None),
        P("grid", "px", "py", None, None),
        P("grid", "px", "py", None, None),
    )
    return jax.shard_map(
        local,
        mesh=mesh,
        in_specs=placed,
        out_specs=P("grid", "px", "py", None, None),
        check_vma=False,
    )
```
